32 devices in a mesh: fsdp: 4 (over x, core), seq: 8 (over z, y).
Axes of the slice: x: 2, y: 2, z: 4, core: 2. Of those that a mesh axis runs over, the one named last changes fastest.
Arguments:
- layer_in: bfloat16 [12288, 1024], P(('fsdp', 'seq'))
- cotangent: bfloat16 [12288, 1024], P(('fsdp', 'seq')), may hold values from -6 to 6
- doc_ids: int32 [4, 3072], P('fsdp'), may hold values from 0 to 5, never falling along the last dimension, each value on 1 to 1024 neighbouring positions
- valid_len: int32 [4], P('fsdp'), may hold values from 1536 to 3072
- attn_weights: bfloat16 [4096, 1024], P(('fsdp', 'seq'))
- mlp_weights: bfloat16 [8192, 1024], P(('fsdp', 'seq'))
- param_vector: bfloat16 [12288], P(('fsdp', 'seq'))
Outputs:
- layer_out: bfloat16 [12288, 1024], P(('fsdp', 'seq'))
- input_grad: float32 [12288, 1024], P(('fsdp', 'seq'))
- attn_grad: float32 [4096, 1024], P(('fsdp', 'seq'))
- mlp_grad: float32 [8192, 1024], P(('fsdp', 'seq'))
- vector_grad: float32 [12288], P(('fsdp', 'seq'))
- rms_values: float32 [4], replicated
The draws below stay inside these ranges and needn't reach their ends.
Inputs may be any that keep to these rules, and one draw needn't show every extreme that they name: `doc_ids`: in each row the numbers never fall and every number is used; a document is a run of 1 to 1024 tokens, and one run in each row has exactly 1024.
All inputs are finite; a program needn't handle non-finite values.
Results may differ from the reference program's by a relative error of at most 0.012.
The reference program's roundings to bfloat16 on the way count: a program that leaves them out, or rounds other values in their place, can miss the bound.
Values may be sent and summed in bfloat16 or wider, within the bound.
A program may use at most 192 MiB of HBM per device.

```python
import math
import jax
import jax.numpy as jnp
import numpy as np
from jax import lax

D = 1024
H = 16
FF = 4096
DOC_MAX = 1024
SEG = 3072
DOCS = 6
TOKENS = 12288
N_FSDP = 4


def draw_layer_in(key, part):
    row_index = jnp.arange(TOKENS, dtype=jnp.float32)[:, None]
    rising = jnp.exp(0.5 * math.log(3.0) * row_index / TOKENS)
    drawn = jnp.clip(jax.random.normal(key, (TOKENS, D), jnp.float32), -6.0, 6.0) * rising
    return drawn.astype(jnp.bfloat16)


def draw_attn_weights(key, part):
    row_index = jnp.arange(4 * D)[:, None]
    row_scale = jnp.where(row_index >= 3 * D, 4.0, 1.0) * D ** (-0.5)
    base_values = jnp.clip(jax.random.normal(key, (4 * D, D), jnp.float32), -6.0, 6.0)
    return (base_values * row_scale).astype(jnp.bfloat16)


def draw_mlp_weights(key, part):
    row_index = jnp.arange(2 * FF)[:, None]
    row_scale = jnp.where(row_index < FF, D ** (-0.5), FF ** (-0.5))
    base_values = jnp.clip(jax.random.normal(key, (2 * FF, D), jnp.float32), -6.0, 6.0)
    return (base_values * row_scale).astype(jnp.bfloat16)


def draw_param_vector(key, part):
    entry_index = jnp.arange(8 * D + FF)
    slot_number = entry_index // D
    is_gain = (slot_number == 3) | (slot_number == 6)
    base_values = jnp.clip(jax.random.normal(key, (8 * D + FF,), jnp.float32), -6.0, 6.0)
    drawn = jnp.where(is_gain, jnp.exp(0.2 * base_values), 0.3 * base_values)
    return drawn.astype(jnp.bfloat16)


def set_ends(values, key, low, top_value):
    extent = values.shape
    index_at = [jax.random.randint(jax.random.fold_in(key, axis), (), 0, extent[axis]) for axis in range(len(extent))]
    values = values.at[tuple(index_at)].set(low)
    longest = extent.index(max(extent))
    index_at[longest] = (index_at[longest] + 1) % extent[longest]
    return values.at[tuple(index_at)].set(top_value)


def block_levels(key, dims, cuts, least, largest):
    def one(dim, parts):
        heights = jax.random.uniform(jax.random.fold_in(jax.random.fold_in(key, 6), dim), (parts,), jnp.float32, least / len(cuts), largest / len(cuts))
        return jnp.repeat(jnp.exp(heights), dims[dim] // parts).reshape((-1,) + (1,) * (len(dims) - dim - 1))

    factor_of = one(*cuts[0])
    for cut in cuts[1:]:
        factor_of = factor_of * one(*cut)
    return factor_of


def profile(count, total, most, slope):
    loads = [(1 << 20) // math.isqrt(grade ** slope) + 1 for grade in range(2, count + 1)]
    surplus, holding = total - most - (count - 1), [1] * (count - 1)
    while surplus > 0:
        candidates = [i for i in range(count - 1) if holding[i] < most]
        mass, budget = sum([loads[i] for i in candidates]), surplus
        for i in candidates:
            addition = min(most - holding[i], max(1, budget * loads[i] // mass), surplus)
            holding[i] = holding[i] + addition
            surplus = surplus - addition
    return np.array([most] + holding)


def ragged(stream_key, amount, total, reach, skew):
    if amount == 2:
        one = jax.random.randint(stream_key, (), max(1, total - reach), min(reach, total - 1) + 1)
        return jnp.stack([one, total - one])
    tallies = jnp.asarray(profile(amount, total, reach, skew), jnp.int32)
    twos = (amount - 1) // 2
    source_of, taker = tallies[1:1 + 2 * twos:2], tallies[2:2 + 2 * twos:2]
    room = jnp.minimum(source_of - 1, reach - taker)
    shifted = jax.random.randint(jax.random.fold_in(stream_key, 1), (twos,), 0, 1 << 20) % (room + 1)
    tallies = tallies.at[1:1 + 2 * twos:2].set(source_of - shifted).at[2:2 + 2 * twos:2].set(taker + shifted)
    return tallies[jax.random.permutation(jax.random.fold_in(stream_key, 2), amount)]


def bell_draw(key, dims, scale, limit, cuts=(), kind=jnp.bfloat16):
    entries = scale * jax.random.normal(key, dims, jnp.float32)
    if cuts:
        entries = entries * block_levels(key, dims, cuts, -0.22, 0.18)
    return jnp.clip(entries, -limit, limit).astype(kind)


def setup_inputs(seed: int = 0) -> dict:
    seeds = jax.random.split(jax.random.key(seed), 8)
    return {
        "layer_in": draw_layer_in(jax.random.fold_in(seeds[7], 71), 0),
        "cotangent": bell_draw(seeds[1], (TOKENS, D), 1.0, 6.0, ((0, 32),)),
        "doc_ids": jax.vmap(lambda own: jnp.searchsorted(jnp.cumsum(ragged(own, DOCS, SEG, DOC_MAX, 1)), jnp.arange(SEG), side="right"))(jax.random.split(seeds[2], N_FSDP)).reshape((N_FSDP, SEG)).astype(jnp.int32),
        "valid_len": set_ends(jax.random.randint(seeds[3], (N_FSDP,), SEG // 2, SEG + 1), jax.random.fold_in(seeds[3], 1), SEG // 2, SEG).astype(jnp.int32),
        "attn_weights": draw_attn_weights(jax.random.fold_in(seeds[7], 71), 0),
        "mlp_weights": draw_mlp_weights(jax.random.fold_in(seeds[7], 71), 0),
        "param_vector": draw_param_vector(jax.random.fold_in(seeds[7], 71), 0),
    }


@jax.custom_vjp
def low(v):
    return lax.optimization_barrier(v.astype(jnp.bfloat16)).astype(jnp.float32)

@jax.custom_vjp
def low_back(v):
    return v

def low_keep(v):
    return (low(v), None)

def low_pass(kept, grad):
    return (grad,)

def back_keep(v):
    return (v, None)

def back_low(kept, grad):
    return (low(grad),)
low.defvjp(low_keep, low_pass)
low_back.defvjp(back_keep, back_low)
EPSILON = 1e-05

def matmul(left, right):
    return jnp.dot(left, right, precision=lax.Precision.HIGHEST, preferred_element_type=jnp.float32)

def layer_norm(values, norm_gain, norm_shift):
    row_mean = lax.optimization_barrier(jnp.mean(values, axis=1, keepdims=True))
    centered = values - row_mean
    row_var = lax.optimization_barrier(jnp.mean(centered * centered, axis=1, keepdims=True))
    return centered * lax.rsqrt(row_var + EPSILON) * norm_gain + norm_shift

def attention(queries, key_rows, value_rows, segment_doc):
    seg_len = queries.shape[0]
    head_size = queries.shape[2]
    block_rows = min(512, seg_len)
    block_count = seg_len // block_rows
    score_scale = head_size ** (-0.5)
    query_blocks = queries.reshape(block_count, block_rows, H, head_size)
    doc_blocks = segment_doc.reshape(block_count, block_rows)

    def one_block(block_pair):
        query_part, doc_part = block_pair
        scores = jnp.einsum('qhd,khd->hqk', query_part, key_rows, precision=lax.Precision.HIGHEST)
        scores = low_back(scores * score_scale)
        same_doc = doc_part[:, None] == segment_doc[None, :]
        scores = jnp.where(same_doc[None], scores, -1e+30)
        weights_low = low(jax.nn.softmax(scores, axis=-1))
        return jnp.einsum('hqk,khd->qhd', weights_low, value_rows, precision=lax.Precision.HIGHEST)
    mixed_rows = lax.map(jax.checkpoint(one_block), (query_blocks, doc_blocks))
    return mixed_rows.reshape(seg_len, H * head_size)

def forward(inputs, attn_params, mlp_params, vector_params, segment_doc):
    seg_len, model_width = inputs.shape
    hidden = mlp_params.shape[0] // 2
    head_size = model_width // H
    pieces = [vector_params[slot_index * model_width:(slot_index + 1) * model_width] for slot_index in range(8)]
    bias_q, bias_v, bias_o, gain_one, shift_one, bias_two, gain_two, shift_two = pieces
    bias_up = vector_params[8 * model_width:]
    weight_q = attn_params[0:model_width]
    weight_k = attn_params[model_width:2 * model_width]
    weight_v = attn_params[2 * model_width:3 * model_width]
    weight_o = attn_params[3 * model_width:]
    queries = low_back(low(matmul(inputs, weight_q) + bias_q))
    key_rows = low_back(low(matmul(inputs, weight_k)))
    value_rows = low_back(low(matmul(inputs, weight_v) + bias_v))
    mixed_rows = attention(queries.reshape(seg_len, H, head_size), key_rows.reshape(seg_len, H, head_size), value_rows.reshape(seg_len, H, head_size), segment_doc)
    mixed_rows = low_back(low(mixed_rows))
    branch = low_back(matmul(mixed_rows, weight_o) + bias_o)
    resid_one = inputs + branch
    normed = layer_norm(resid_one, gain_one, shift_one)
    upper = lax.dot_general(low(normed), mlp_params[:hidden], (((1,), (1,)), ((), ())), precision=lax.Precision.HIGHEST, preferred_element_type=jnp.float32)
    upper = low_back(upper + bias_up)
    active = low(jax.nn.gelu(upper, approximate=False))
    mlp_branch = low_back(matmul(active, mlp_params[hidden:]) + bias_two)
    resid_two = normed + mlp_branch
    layer_values = layer_norm(resid_two, gain_two, shift_two)
    return (layer_values, (resid_one, branch, resid_two, mlp_branch))

def reference(layer_in, cotangent, doc_ids, valid_len, attn_weights, mlp_weights, param_vector):
    attn_params = attn_weights.astype(jnp.float32)
    mlp_params = mlp_weights.astype(jnp.float32)
    vector_params = param_vector.astype(jnp.float32)
    model_width = layer_in.shape[1]
    segments = doc_ids.shape[0]
    seg_len = doc_ids.shape[1]
    inputs_all = layer_in.astype(jnp.float32).reshape(segments, seg_len, model_width)
    cotan_all = cotangent.astype(jnp.float32).reshape(segments, seg_len, model_width)
    positions = lax.iota(jnp.int32, seg_len)

    def one_segment(carried, segment):
        grad_attn, grad_mlp, grad_vector, square_sums = carried
        inputs, cotan_rows, segment_doc, segment_valid = segment

        def segment_layer(layer_inputs, attn_part, mlp_part, vector_part):
            return forward(layer_inputs, attn_part, mlp_part, vector_part, segment_doc)
        layer_values, pullback, kept_values = jax.vjp(segment_layer, inputs, attn_params, mlp_params, vector_params, has_aux=True)
        grad_inputs, part_attn, part_mlp, part_vector = pullback(cotan_rows)
        valid_rows = (positions < segment_valid).astype(jnp.float32)[:, None]
        squares = jnp.stack([jnp.sum(valid_rows * kept_term * kept_term) for kept_term in kept_values])
        carried = (grad_attn + part_attn, grad_mlp + part_mlp, grad_vector + part_vector, square_sums + squares)
        return (carried, (layer_values.astype(jnp.bfloat16), grad_inputs))
    start = (jnp.zeros(attn_params.shape, jnp.float32), jnp.zeros(mlp_params.shape, jnp.float32), jnp.zeros(vector_params.shape, jnp.float32), jnp.zeros((4,), jnp.float32))
    finals, outputs = lax.scan(one_segment, start, (inputs_all, cotan_all, doc_ids, valid_len))
    grad_attn, grad_mlp, grad_vector, square_sums = finals
    layer_out = outputs[0].reshape(segments * seg_len, model_width)
    input_grad = outputs[1].reshape(segments * seg_len, model_width)
    valid_total = jnp.sum(valid_len).astype(jnp.float32)
    rms_values = jnp.sqrt(square_sums / (valid_total * model_width))
    return (layer_out, input_grad, grad_attn, grad_mlp, grad_vector, rms_values)
```

```python
import jax
import jax.numpy as jnp
from jax import lax
from jax.sharding import PartitionSpec as P


H = 16


EPSILON = 1e-05
ROOT_HALF = 0.7071067811865476
INV_ROOT_TWO_PI = 0.3989422804014327


def norm_forward(values, norm_gain, norm_shift):
    row_mean = jnp.mean(values, axis=1, keepdims=True)
    centered = values - row_mean
    inverse = lax.rsqrt(jnp.mean(centered * centered, axis=1, keepdims=True) + EPSILON)
    scaled = centered * inverse
    return (scaled * norm_gain + norm_shift, scaled, inverse)


def norm_backward(gradient, scaled, inverse, norm_gain):
    grad_scaled = gradient * norm_gain
    grad_mean = jnp.mean(grad_scaled, axis=1, keepdims=True)
    grad_along = jnp.mean(grad_scaled * scaled, axis=1, keepdims=True)
    grad_rows = inverse * (grad_scaled - grad_mean - scaled * grad_along)
    return (grad_rows, jnp.sum(gradient * scaled, axis=0), jnp.sum(gradient, axis=0))


def gelu_slope(entries):
    return 0.5 * (1.0 + lax.erf(entries * ROOT_HALF)) + entries * INV_ROOT_TWO_PI * jnp.exp(
        -0.5 * entries * entries
    )


def attend_block(queries, key_rows, query_doc, key_doc, score_scale):
    scores = (
        jnp.einsum("qhd,khd->hqk", queries, key_rows, preferred_element_type=jnp.float32)
        * score_scale
    )
    same_doc = query_doc[:, None] == key_doc[None, :]
    return jnp.where(same_doc[None], scores, -1e30)


def scatter_sum(values):
    partial = lax.psum_scatter(values, "fsdp", scatter_dimension=0, tiled=True)
    return lax.psum_scatter(partial, "seq", scatter_dimension=0, tiled=True)


def contract_rows(left, right):
    return lax.dot_general(
        left, right, (((0,), (0,)), ((), ())), preferred_element_type=jnp.float32
    )


def contract_cols(left, right):
    return lax.dot_general(
        left, right, (((1,), (1,)), ((), ())), preferred_element_type=jnp.float32
    )


def layer_body(layer_in, cotangent, doc_ids, valid_len, attn_weights, mlp_weights, param_vector):
    seq_count = lax.axis_size("seq")
    seq_index = lax.axis_index("seq")
    tokens, model_width = layer_in.shape
    head_size = model_width // H
    local_heads = H // seq_count
    score_scale = head_size ** (-0.5)
    attn_full, mlp_full, vector_full = (
        lax.all_gather(attn_weights, ("fsdp", "seq"), axis=0, tiled=True),
        lax.all_gather(mlp_weights, ("fsdp", "seq"), axis=0, tiled=True),
        lax.all_gather(param_vector, ("fsdp", "seq"), axis=0, tiled=True),
    )
    hidden = mlp_full.shape[0] // 2
    vector_wide = vector_full.astype(jnp.float32)
    pieces = [
        vector_wide[slot_index * model_width : (slot_index + 1) * model_width]
        for slot_index in range(8)
    ]
    bias_q, bias_v, bias_o, gain_one, shift_one, bias_two, gain_two, shift_two = pieces
    bias_up = vector_wide[8 * model_width :]
    qkv_weights = attn_full[: 3 * model_width].reshape(3, model_width, model_width)
    out_weights = attn_full[3 * model_width :]
    in_weights = mlp_full[:hidden]
    down_weights = mlp_full[hidden:]
    segment_doc = doc_ids[0]
    seg_len = segment_doc.shape[0]
    block_rows = min(512, seg_len)
    block_count = seg_len // block_rows
    doc_blocks = segment_doc.reshape(block_count, block_rows)
    positions = seq_index * tokens + lax.iota(jnp.int32, tokens)
    valid_rows = (positions < valid_len[0]).astype(jnp.float32)[:, None]
    zero_row = jnp.zeros((1, model_width), jnp.float32)
    qkv_bias = jnp.concatenate([bias_q[None], zero_row, bias_v[None]], axis=0)
    projected = (
        jnp.einsum("td,ide->tie", layer_in, qkv_weights, preferred_element_type=jnp.float32)
        + qkv_bias[None]
    )
    qkv_split = projected.astype(jnp.bfloat16).reshape(tokens, 3, seq_count, local_heads, head_size)
    head_piece = lax.all_to_all(qkv_split, "seq", split_axis=2, concat_axis=0, tiled=True)
    queries = head_piece[:, 0, 0]
    attend_key_rows = head_piece[:, 1, 0]
    attend_value_rows = head_piece[:, 2, 0]
    head_count = queries.shape[1]
    query_blocks = queries.reshape(block_count, block_rows, head_count, head_size)

    def one_block(block_pair):
        query_part, doc_part = block_pair
        scores = attend_block(query_part, attend_key_rows, doc_part, segment_doc, score_scale)
        top_score = jnp.max(scores, axis=-1, keepdims=True)
        exponent = jnp.exp(scores - top_score)
        row_total = jnp.sum(exponent, axis=-1, keepdims=True)
        weights_low = (exponent / row_total).astype(jnp.bfloat16)
        mixed_part = jnp.einsum(
            "hqk,khd->qhd", weights_low, attend_value_rows, preferred_element_type=jnp.float32
        )
        return (mixed_part, (top_score + jnp.log(row_total))[..., 0])

    mixed_rows, log_total = lax.map(one_block, (query_blocks, doc_blocks))
    mixed_rows = mixed_rows.reshape(seg_len, 1, head_count, head_size).astype(jnp.bfloat16)
    log_total = jnp.transpose(log_total, (0, 2, 1)).reshape(seg_len, 1, head_count)
    token_mixed = lax.all_to_all(mixed_rows, "seq", split_axis=0, concat_axis=1, tiled=True)
    attn_mixed = token_mixed.reshape(tokens, model_width)
    branch = jnp.dot(attn_mixed, out_weights, preferred_element_type=jnp.float32) + bias_o
    resid_one = layer_in.astype(jnp.float32) + branch
    normed, scaled_one, inverse_one = norm_forward(resid_one, gain_one, shift_one)
    normed_low = normed.astype(jnp.bfloat16)
    upper = contract_cols(normed_low, in_weights) + bias_up
    active_low = jax.nn.gelu(upper, approximate=False).astype(jnp.bfloat16)
    mlp_branch = jnp.dot(active_low, down_weights, preferred_element_type=jnp.float32) + bias_two
    resid_two = normed + mlp_branch
    layer_values, scaled_two, inverse_two = norm_forward(resid_two, gain_two, shift_two)
    squares = jnp.stack(
        [
            jnp.sum(valid_rows * resid_one * resid_one),
            jnp.sum(valid_rows * branch * branch),
            jnp.sum(valid_rows * resid_two * resid_two),
            jnp.sum(valid_rows * mlp_branch * mlp_branch),
        ]
    )
    square_sums, valid_total = lax.psum((squares, jnp.sum(valid_rows)), ("fsdp", "seq"))
    rms_values = jnp.sqrt(square_sums / (valid_total * model_width))
    grad_out = cotangent.astype(jnp.float32)
    grad_resid_two, grad_gain_two, grad_shift_two = norm_backward(
        grad_out, scaled_two, inverse_two, gain_two
    )
    grad_mlp_low = grad_resid_two.astype(jnp.bfloat16)
    grad_bias_two = jnp.sum(grad_mlp_low.astype(jnp.float32), axis=0)
    grad_down = contract_rows(active_low, grad_mlp_low)
    grad_active = contract_cols(grad_mlp_low, down_weights)
    grad_upper_low = (grad_active * gelu_slope(upper)).astype(jnp.bfloat16)
    grad_bias_up = jnp.sum(grad_upper_low.astype(jnp.float32), axis=0)
    grad_in = contract_rows(grad_upper_low, normed_low)
    grad_normed = grad_resid_two + jnp.dot(
        grad_upper_low, in_weights, preferred_element_type=jnp.float32
    )
    grad_mlp_full = jnp.concatenate([grad_in, grad_down], axis=0)
    mlp_shard = scatter_sum(grad_mlp_full)
    grad_resid_one, grad_gain_one, grad_shift_one = norm_backward(
        grad_normed, scaled_one, inverse_one, gain_one
    )
    grad_branch_low = grad_resid_one.astype(jnp.bfloat16)
    grad_bias_o = jnp.sum(grad_branch_low.astype(jnp.float32), axis=0)
    grad_out_weights = contract_rows(attn_mixed, grad_branch_low)
    grad_mixed_low = contract_cols(grad_branch_low, out_weights).astype(jnp.bfloat16)
    grad_split = grad_mixed_low.reshape(tokens, 1, seq_count, local_heads, head_size)
    grad_heads = lax.all_to_all(grad_split, "seq", split_axis=2, concat_axis=0, tiled=True)
    head_inputs = head_piece[:, :, 0]
    head_grad = grad_heads[:, 0, 0]
    queries = head_inputs[:, 0]
    key_rows = head_inputs[:, 1]
    value_rows = head_inputs[:, 2]
    query_blocks = queries.reshape(block_count, block_rows, local_heads, head_size)
    grad_blocks = head_grad.reshape(block_count, block_rows, local_heads, head_size)
    log_blocks = log_total.reshape(block_count, block_rows, local_heads)

    def back_block(running, block_inputs):
        grad_keys, grad_values = running
        query_part, grad_part, log_part, doc_part = block_inputs
        scores = attend_block(query_part, key_rows, doc_part, segment_doc, score_scale)
        probs = jnp.exp(scores - jnp.transpose(log_part)[:, :, None])
        grad_probs = jnp.einsum(
            "qhd,khd->hqk", grad_part, value_rows, preferred_element_type=jnp.float32
        )
        row_inner = jnp.sum(grad_probs * probs, axis=-1, keepdims=True)
        grad_scores = (probs * (grad_probs - row_inner)).astype(jnp.bfloat16)
        grad_query = (
            jnp.einsum("hqk,khd->qhd", grad_scores, key_rows, preferred_element_type=jnp.float32)
            * score_scale
        )
        grad_keys = (
            grad_keys
            + jnp.einsum(
                "hqk,qhd->khd", grad_scores, query_part, preferred_element_type=jnp.float32
            )
            * score_scale
        )
        grad_values = grad_values + jnp.einsum(
            "hqk,qhd->khd",
            probs.astype(jnp.bfloat16),
            grad_part,
            preferred_element_type=jnp.float32,
        )
        return ((grad_keys, grad_values), grad_query)

    zeros_head = jnp.zeros((seg_len, local_heads, head_size), jnp.float32)
    (grad_keys, grad_values), grad_queries = lax.scan(
        back_block, (zeros_head, zeros_head), (query_blocks, grad_blocks, log_blocks, doc_blocks)
    )
    grad_queries = grad_queries.reshape(seg_len, local_heads, head_size)
    head_grads = jnp.stack([grad_queries, grad_keys, grad_values], axis=1).astype(jnp.bfloat16)[
        :, :, None
    ]
    token_grads = lax.all_to_all(head_grads, "seq", split_axis=0, concat_axis=2, tiled=True)
    grad_qkv = token_grads.reshape(tokens, 3, model_width)
    input_grad = grad_resid_one + jnp.einsum(
        "tie,ide->td", grad_qkv, qkv_weights, preferred_element_type=jnp.float32
    )
    grad_qkv_weights = jnp.einsum(
        "td,tie->ide", layer_in, grad_qkv, preferred_element_type=jnp.float32
    )
    grad_bias_qkv = jnp.sum(grad_qkv.astype(jnp.float32), axis=0)
    grad_vector = jnp.concatenate(
        [
            grad_bias_qkv[0],
            grad_bias_qkv[2],
            grad_bias_o,
            grad_gain_one,
            grad_shift_one,
            grad_bias_two,
            grad_gain_two,
            grad_shift_two,
            grad_bias_up,
        ]
    )
    grad_attn_full = jnp.concatenate(
        [grad_qkv_weights.reshape(3 * model_width, model_width), grad_out_weights], axis=0
    )
    attn_shard, mlp_shard, vector_shard = (
        scatter_sum(grad_attn_full), mlp_shard, scatter_sum(grad_vector)
    )
    return (
        layer_values.astype(jnp.bfloat16),
        input_grad,
        attn_shard,
        mlp_shard,
        vector_shard,
        rms_values,
    )


def solution(mesh):
    in_specs = (
        P(("fsdp", "seq"), None),
        P(("fsdp", "seq"), None),
        P("fsdp", None),
        P("fsdp"),
        P(("fsdp", "seq"), None),
        P(("fsdp", "seq"), None),
        P(("fsdp", "seq")),
    )
    out_specs = (
        P(("fsdp", "seq"), None),
        P(("fsdp", "seq"), None),
        P(("fsdp", "seq"), None),
        P(("fsdp", "seq"), None),
        P(("fsdp", "seq")),
        P(),
    )
    return jax.shard_map(
        layer_body, mesh=mesh, in_specs=in_specs, out_specs=out_specs, check_vma=False
    )
```

```python
import jax
import jax.numpy as jnp
from jax import lax
from jax.sharding import PartitionSpec as P


H = 16


EPSILON = 1e-05
ROOT_HALF = 0.7071067811865476
INV_ROOT_TWO_PI = 0.3989422804014327


def norm_forward(values, norm_gain, norm_shift):
    row_mean = jnp.mean(values, axis=1, keepdims=True)
    centered = values - row_mean
    inverse = lax.rsqrt(jnp.mean(centered * centered, axis=1, keepdims=True) + EPSILON)
    scaled = centered * inverse
    return (scaled * norm_gain + norm_shift, scaled, inverse)


def norm_backward(gradient, scaled, inverse, norm_gain):
    grad_scaled = gradient * norm_gain
    grad_mean = jnp.mean(grad_scaled, axis=1, keepdims=True)
    grad_along = jnp.mean(grad_scaled * scaled, axis=1, keepdims=True)
    grad_rows = inverse * (grad_scaled - grad_mean - scaled * grad_along)
    return (grad_rows, jnp.sum(gradient * scaled, axis=0), jnp.sum(gradient, axis=0))


def gelu_slope(entries):
    return 0.5 * (1.0 + lax.erf(entries * ROOT_HALF)) + entries * INV_ROOT_TWO_PI * jnp.exp(
        -0.5 * entries * entries
    )


def attend_block(queries, key_rows, query_doc, key_doc, score_scale):
    scores = (
        jnp.einsum("qhd,khd->hqk", queries, key_rows, preferred_element_type=jnp.float32)
        * score_scale
    )
    same_doc = query_doc[:, None] == key_doc[None, :]
    return jnp.where(same_doc[None], scores, -1e30)


def scatter_sum(values):
    partial = lax.psum_scatter(values, "fsdp", scatter_dimension=0, tiled=True)
    return lax.psum_scatter(partial, "seq", scatter_dimension=0, tiled=True)


def attn_sum(values):
    return lax.psum_scatter(values, "fsdp", scatter_dimension=0, tiled=True)[0]


def contract_rows(left, right):
    return lax.dot_general(
        left, right, (((0,), (0,)), ((), ())), preferred_element_type=jnp.float32
    )


def contract_cols(left, right):
    return lax.dot_general(
        left, right, (((1,), (1,)), ((), ())), preferred_element_type=jnp.float32
    )


def layer_body(layer_in, cotangent, doc_ids, valid_len, attn_weights, mlp_weights, param_vector):
    seq_count = lax.axis_size("seq")
    seq_index = lax.axis_index("seq")
    tokens, model_width = layer_in.shape
    head_size = model_width // H
    local_heads = H // seq_count
    score_scale = head_size ** (-0.5)
    attn_full, mlp_full, vector_full = (
        lax.all_gather(attn_weights, ("fsdp", "seq"), axis=0, tiled=True),
        lax.all_gather(mlp_weights, ("fsdp", "seq"), axis=0, tiled=True),
        lax.all_gather(param_vector, ("fsdp", "seq"), axis=0, tiled=True),
    )
    hidden = mlp_full.shape[0] // 2
    vector_wide = vector_full.astype(jnp.float32)
    pieces = [
        vector_wide[slot_index * model_width : (slot_index + 1) * model_width]
        for slot_index in range(8)
    ]
    bias_q, bias_v, bias_o, gain_one, shift_one, bias_two, gain_two, shift_two = pieces
    bias_up = vector_wide[8 * model_width :]
    qkv_weights = attn_full[: 3 * model_width].reshape(3, model_width, model_width)
    out_weights = attn_full[3 * model_width :]
    in_weights = mlp_full[:hidden]
    down_weights = mlp_full[hidden:]
    segment_in = lax.all_gather(layer_in, "seq", axis=0, tiled=True)
    segment_doc = doc_ids[0]
    seg_len = segment_doc.shape[0]
    block_rows = min(512, seg_len)
    block_count = seg_len // block_rows
    doc_blocks = segment_doc.reshape(block_count, block_rows)
    positions = seq_index * tokens + lax.iota(jnp.int32, tokens)
    valid_rows = (positions < valid_len[0]).astype(jnp.float32)[:, None]
    zero_row = jnp.zeros((1, model_width), jnp.float32)
    qkv_bias = jnp.concatenate([bias_q[None], zero_row, bias_v[None]], axis=0)
    projected = (
        jnp.einsum("td,ide->tie", layer_in, qkv_weights, preferred_element_type=jnp.float32)
        + qkv_bias[None]
    )
    qkv_split = projected.astype(jnp.bfloat16).reshape(tokens, 3, seq_count, local_heads, head_size)
    head_piece = lax.all_to_all(qkv_split, "seq", split_axis=2, concat_axis=0, tiled=True)
    queries = head_piece[:, 0, 0]
    attend_key_rows = head_piece[:, 1, 0]
    attend_value_rows = head_piece[:, 2, 0]
    head_count = queries.shape[1]
    query_blocks = queries.reshape(block_count, block_rows, head_count, head_size)

    def one_block(block_pair):
        query_part, doc_part = block_pair
        scores = attend_block(query_part, attend_key_rows, doc_part, segment_doc, score_scale)
        top_score = jnp.max(scores, axis=-1, keepdims=True)
        exponent = jnp.exp(scores - top_score)
        row_total = jnp.sum(exponent, axis=-1, keepdims=True)
        weights_low = (exponent / row_total).astype(jnp.bfloat16)
        mixed_part = jnp.einsum(
            "hqk,khd->qhd", weights_low, attend_value_rows, preferred_element_type=jnp.float32
        )
        return (mixed_part, (top_score + jnp.log(row_total))[..., 0])

    mixed_rows, log_total = lax.map(one_block, (query_blocks, doc_blocks))
    mixed_rows = mixed_rows.reshape(seg_len, 1, head_count, head_size).astype(jnp.bfloat16)
    log_total = jnp.transpose(log_total, (0, 2, 1)).reshape(seg_len, 1, head_count)
    token_mixed = lax.all_to_all(mixed_rows, "seq", split_axis=0, concat_axis=1, tiled=True)
    attn_mixed = token_mixed.reshape(tokens, model_width)
    branch = jnp.dot(attn_mixed, out_weights, preferred_element_type=jnp.float32) + bias_o
    resid_one = layer_in.astype(jnp.float32) + branch
    normed, scaled_one, inverse_one = norm_forward(resid_one, gain_one, shift_one)
    normed_low = normed.astype(jnp.bfloat16)
    upper = contract_cols(normed_low, in_weights) + bias_up
    active_low = jax.nn.gelu(upper, approximate=False).astype(jnp.bfloat16)
    mlp_branch = jnp.dot(active_low, down_weights, preferred_element_type=jnp.float32) + bias_two
    resid_two = normed + mlp_branch
    layer_values, scaled_two, inverse_two = norm_forward(resid_two, gain_two, shift_two)
    squares = jnp.stack(
        [
            jnp.sum(valid_rows * resid_one * resid_one),
            jnp.sum(valid_rows * branch * branch),
            jnp.sum(valid_rows * resid_two * resid_two),
            jnp.sum(valid_rows * mlp_branch * mlp_branch),
        ]
    )
    square_sums, valid_total = lax.psum((squares, jnp.sum(valid_rows)), ("fsdp", "seq"))
    rms_values = jnp.sqrt(square_sums / (valid_total * model_width))
    grad_out = cotangent.astype(jnp.float32)
    grad_resid_two, grad_gain_two, grad_shift_two = norm_backward(
        grad_out, scaled_two, inverse_two, gain_two
    )
    grad_mlp_low = grad_resid_two.astype(jnp.bfloat16)
    grad_bias_two = jnp.sum(grad_mlp_low.astype(jnp.float32), axis=0)
    grad_down = contract_rows(active_low, grad_mlp_low)
    grad_active = contract_cols(grad_mlp_low, down_weights)
    grad_upper_low = (grad_active * gelu_slope(upper)).astype(jnp.bfloat16)
    grad_bias_up = jnp.sum(grad_upper_low.astype(jnp.float32), axis=0)
    grad_in = contract_rows(grad_upper_low, normed_low)
    grad_normed = grad_resid_two + jnp.dot(
        grad_upper_low, in_weights, preferred_element_type=jnp.float32
    )
    grad_mlp_full = jnp.concatenate([grad_in, grad_down], axis=0)
    mlp_shard = scatter_sum(grad_mlp_full)
    grad_resid_one, grad_gain_one, grad_shift_one = norm_backward(
        grad_normed, scaled_one, inverse_one, gain_one
    )
    grad_branch_low = grad_resid_one.astype(jnp.bfloat16)
    grad_bias_o = jnp.sum(grad_branch_low.astype(jnp.float32), axis=0)
    fsdp_count = lax.axis_size("fsdp")
    block_height = 4 * model_width // (fsdp_count * seq_count)
    out_blocks = model_width // (seq_count * block_height)
    out_rows = lax.psum_scatter(
        contract_rows(attn_mixed, grad_branch_low).reshape(
            out_blocks, seq_count, block_height, model_width
        ),
        "seq",
        scatter_dimension=1,
        tiled=True,
    )[:, 0]
    grad_mixed_low = contract_cols(grad_branch_low, out_weights).astype(jnp.bfloat16)
    grad_split = grad_mixed_low.reshape(tokens, 1, seq_count, local_heads, head_size)
    grad_heads = lax.all_to_all(grad_split, "seq", split_axis=2, concat_axis=0, tiled=True)
    head_inputs = head_piece[:, :, 0]
    head_grad = grad_heads[:, 0, 0]
    queries = head_inputs[:, 0]
    key_rows = head_inputs[:, 1]
    value_rows = head_inputs[:, 2]
    query_blocks = queries.reshape(block_count, block_rows, local_heads, head_size)
    grad_blocks = head_grad.reshape(block_count, block_rows, local_heads, head_size)
    log_blocks = log_total.reshape(block_count, block_rows, local_heads)

    def back_block(running, block_inputs):
        grad_keys, grad_values = running
        query_part, grad_part, log_part, doc_part = block_inputs
        scores = attend_block(query_part, key_rows, doc_part, segment_doc, score_scale)
        probs = jnp.exp(scores - jnp.transpose(log_part)[:, :, None])
        grad_probs = jnp.einsum(
            "qhd,khd->hqk", grad_part, value_rows, preferred_element_type=jnp.float32
        )
        row_inner = jnp.sum(grad_probs * probs, axis=-1, keepdims=True)
        grad_scores = (probs * (grad_probs - row_inner)).astype(jnp.bfloat16)
        grad_query = (
            jnp.einsum("hqk,khd->qhd", grad_scores, key_rows, preferred_element_type=jnp.float32)
            * score_scale
        )
        grad_keys = (
            grad_keys
            + jnp.einsum(
                "hqk,qhd->khd", grad_scores, query_part, preferred_element_type=jnp.float32
            )
            * score_scale
        )
        grad_values = grad_values + jnp.einsum(
            "hqk,qhd->khd",
            probs.astype(jnp.bfloat16),
            grad_part,
            preferred_element_type=jnp.float32,
        )
        return ((grad_keys, grad_values), grad_query)

    zeros_head = jnp.zeros((seg_len, local_heads, head_size), jnp.float32)
    (grad_keys, grad_values), grad_queries = lax.scan(
        back_block, (zeros_head, zeros_head), (query_blocks, grad_blocks, log_blocks, doc_blocks)
    )
    grad_queries = grad_queries.reshape(seg_len, local_heads, head_size)
    head_grads = jnp.stack([grad_queries, grad_keys, grad_values], axis=1).astype(jnp.bfloat16)
    head_weight_grads = jnp.einsum(
        "td,tihe->dihe", segment_in, head_grads, preferred_element_type=jnp.float32
    )
    qkv_blocks = 3 * out_blocks
    head_width = local_heads * head_size
    by_row = jnp.transpose(head_weight_grads.reshape(model_width, 3, head_width), (1, 0, 2))
    row_blocks = lax.all_to_all(
        by_row.reshape(qkv_blocks, seq_count, block_height, head_width),
        "seq", split_axis=1, concat_axis=1, tiled=True,
    )
    qkv_rows = jnp.transpose(row_blocks, (0, 2, 1, 3)).reshape(qkv_blocks, block_height, model_width)
    head_grads = head_grads[:, :, None]
    token_grads = lax.all_to_all(head_grads, "seq", split_axis=0, concat_axis=2, tiled=True)
    grad_qkv = token_grads.reshape(tokens, 3, model_width)
    input_grad = grad_resid_one + jnp.einsum(
        "tie,ide->td", grad_qkv, qkv_weights, preferred_element_type=jnp.float32
    )
    grad_bias_qkv = jnp.sum(grad_qkv.astype(jnp.float32), axis=0)
    grad_vector = jnp.concatenate(
        [
            grad_bias_qkv[0],
            grad_bias_qkv[2],
            grad_bias_o,
            grad_gain_one,
            grad_shift_one,
            grad_bias_two,
            grad_gain_two,
            grad_shift_two,
            grad_bias_up,
        ]
    )
    grad_attn_rows = jnp.concatenate([qkv_rows, out_rows], axis=0)
    attn_shard, mlp_shard, vector_shard = (
        attn_sum(grad_attn_rows),
        mlp_shard,
        scatter_sum(grad_vector),
    )
    return (
        layer_values.astype(jnp.bfloat16),
        input_grad,
        attn_shard,
        mlp_shard,
        vector_shard,
        rms_values,
    )


def solution(mesh):
    in_specs = (
        P(("fsdp", "seq"), None),
        P(("fsdp", "seq"), None),
        P("fsdp", None),
        P("fsdp"),
        P(("fsdp", "seq"), None),
        P(("fsdp", "seq"), None),
        P(("fsdp", "seq")),
    )
    out_specs = (
        P(("fsdp", "seq"), None),
        P(("fsdp", "seq"), None),
        P(("fsdp", "seq"), None),
        P(("fsdp", "seq"), None),
        P(("fsdp", "seq")),
        P(),
    )
    return jax.shard_map(
        layer_body, mesh=mesh, in_specs=in_specs, out_specs=out_specs, check_vma=False
    )
```

```python
import jax
import jax.numpy as jnp
from jax import lax
from jax.sharding import PartitionSpec as P


H = 16


EPSILON = 1e-05
ROOT_HALF = 0.7071067811865476
INV_ROOT_TWO_PI = 0.3989422804014327


def norm_forward(values, norm_gain, norm_shift):
    row_mean = jnp.mean(values, axis=1, keepdims=True)
    centered = values - row_mean
    inverse = lax.rsqrt(jnp.mean(centered * centered, axis=1, keepdims=True) + EPSILON)
    scaled = centered * inverse
    return (scaled * norm_gain + norm_shift, scaled, inverse)


def norm_backward(gradient, scaled, inverse, norm_gain):
    grad_scaled = gradient * norm_gain
    grad_mean = jnp.mean(grad_scaled, axis=1, keepdims=True)
    grad_along = jnp.mean(grad_scaled * scaled, axis=1, keepdims=True)
    grad_rows = inverse * (grad_scaled - grad_mean - scaled * grad_along)
    return (grad_rows, jnp.sum(gradient * scaled, axis=0), jnp.sum(gradient, axis=0))


def gelu_slope(entries):
    return 0.5 * (1.0 + lax.erf(entries * ROOT_HALF)) + entries * INV_ROOT_TWO_PI * jnp.exp(
        -0.5 * entries * entries
    )


def attend_block(queries, key_rows, query_doc, key_doc, score_scale):
    scores = (
        jnp.einsum("qhd,khd->hqk", queries, key_rows, preferred_element_type=jnp.float32)
        * score_scale
    )
    same_doc = query_doc[:, None] == key_doc[None, :]
    return jnp.where(same_doc[None], scores, -1e30)


def scatter_sum(values):
    partial = lax.psum_scatter(values, "fsdp", scatter_dimension=0, tiled=True)
    return lax.psum_scatter(partial, "seq", scatter_dimension=0, tiled=True)


def attn_sum(values):
    return lax.psum_scatter(values, "fsdp", scatter_dimension=0, tiled=True)[0]


def contract_rows(left, right):
    return lax.dot_general(
        left, right, (((0,), (0,)), ((), ())), preferred_element_type=jnp.float32
    )


def contract_cols(left, right):
    return lax.dot_general(
        left, right, (((1,), (1,)), ((), ())), preferred_element_type=jnp.float32
    )


def layer_body(layer_in, cotangent, doc_ids, valid_len, attn_weights, mlp_weights, param_vector):
    seq_count = lax.axis_size("seq")
    seq_index = lax.axis_index("seq")
    tokens, model_width = layer_in.shape
    head_size = model_width // H
    local_heads = H // seq_count
    score_scale = head_size ** (-0.5)
    attn_full, mlp_full, vector_full = (
        lax.all_gather(attn_weights, ("fsdp", "seq"), axis=0, tiled=True),
        lax.all_gather(mlp_weights, ("fsdp", "seq"), axis=0, tiled=True),
        lax.all_gather(param_vector, ("fsdp", "seq"), axis=0, tiled=True),
    )
    hidden = mlp_full.shape[0] // 2
    vector_wide = vector_full.astype(jnp.float32)
    pieces = [
        vector_wide[slot_index * model_width : (slot_index + 1) * model_width]
        for slot_index in range(8)
    ]
    bias_q, bias_v, bias_o, gain_one, shift_one, bias_two, gain_two, shift_two = pieces
    bias_up = vector_wide[8 * model_width :]
    qkv_weights = attn_full[: 3 * model_width].reshape(3, model_width, model_width)
    out_weights = attn_full[3 * model_width :]
    in_weights = mlp_full[:hidden]
    down_weights = mlp_full[hidden:]
    segment_in = lax.all_gather(layer_in, "seq", axis=0, tiled=True)
    segment_doc = doc_ids[0]
    seg_len = segment_doc.shape[0]
    block_rows = min(512, seg_len)
    block_count = seg_len // block_rows
    doc_blocks = segment_doc.reshape(block_count, block_rows)
    positions = seq_index * tokens + lax.iota(jnp.int32, tokens)
    valid_rows = (positions < valid_len[0]).astype(jnp.float32)[:, None]
    zero_row = jnp.zeros((1, model_width), jnp.float32)
    qkv_bias = jnp.concatenate([bias_q[None], zero_row, bias_v[None]], axis=0)
    projected = (
        jnp.einsum("td,ide->tie", layer_in, qkv_weights, preferred_element_type=jnp.float32)
        + qkv_bias[None]
    )
    qkv_split = projected.astype(jnp.bfloat16).reshape(tokens, 3, seq_count, local_heads, head_size)
    head_piece = lax.all_to_all(qkv_split, "seq", split_axis=2, concat_axis=0, tiled=True)
    queries = head_piece[:, 0, 0]
    attend_key_rows = head_piece[:, 1, 0]
    attend_value_rows = head_piece[:, 2, 0]
    head_count = queries.shape[1]
    query_blocks = queries.reshape(block_count, block_rows, head_count, head_size)

    def one_block(block_pair):
        query_part, doc_part = block_pair
        scores = attend_block(query_part, attend_key_rows, doc_part, segment_doc, score_scale)
        top_score = jnp.max(scores, axis=-1, keepdims=True)
        exponent = jnp.exp(scores - top_score)
        row_total = jnp.sum(exponent, axis=-1, keepdims=True)
        weights_low = (exponent / row_total).astype(jnp.bfloat16)
        mixed_part = jnp.einsum(
            "hqk,khd->qhd", weights_low, attend_value_rows, preferred_element_type=jnp.float32
        )
        return (mixed_part, (top_score + jnp.log(row_total))[..., 0])

    mixed_rows, log_total = lax.map(one_block, (query_blocks, doc_blocks))
    mixed_rows = mixed_rows.reshape(seg_len, 1, head_count, head_size).astype(jnp.bfloat16)
    log_total = jnp.transpose(log_total, (0, 2, 1)).reshape(seg_len, 1, head_count)
    token_mixed = lax.all_to_all(mixed_rows, "seq", split_axis=0, concat_axis=1, tiled=True)
    attn_mixed = token_mixed.reshape(tokens, model_width)
    branch = jnp.dot(attn_mixed, out_weights, preferred_element_type=jnp.float32) + bias_o
    resid_one = layer_in.astype(jnp.float32) + branch
    normed, scaled_one, inverse_one = norm_forward(resid_one, gain_one, shift_one)
    normed_low = normed.astype(jnp.bfloat16)
    normed_seg = lax.all_gather(normed_low, "seq", axis=0, tiled=True)
    upper = contract_cols(normed_low, in_weights) + bias_up
    active_low = jax.nn.gelu(upper, approximate=False).astype(jnp.bfloat16)
    mlp_branch = jnp.dot(active_low, down_weights, preferred_element_type=jnp.float32) + bias_two
    resid_two = normed + mlp_branch
    layer_values, scaled_two, inverse_two = norm_forward(resid_two, gain_two, shift_two)
    squares = jnp.stack(
        [
            jnp.sum(valid_rows * resid_one * resid_one),
            jnp.sum(valid_rows * branch * branch),
            jnp.sum(valid_rows * resid_two * resid_two),
            jnp.sum(valid_rows * mlp_branch * mlp_branch),
        ]
    )
    square_sums, valid_total = lax.psum((squares, jnp.sum(valid_rows)), ("fsdp", "seq"))
    rms_values = jnp.sqrt(square_sums / (valid_total * model_width))
    grad_out = cotangent.astype(jnp.float32)
    grad_resid_two, grad_gain_two, grad_shift_two = norm_backward(
        grad_out, scaled_two, inverse_two, gain_two
    )
    grad_mlp_low = grad_resid_two.astype(jnp.bfloat16)
    grad_bias_two = jnp.sum(grad_mlp_low.astype(jnp.float32), axis=0)
    grad_active = contract_cols(grad_mlp_low, down_weights)
    grad_upper_low = (grad_active * gelu_slope(upper)).astype(jnp.bfloat16)
    grad_bias_up = jnp.sum(grad_upper_low.astype(jnp.float32), axis=0)
    grad_normed = grad_resid_two + jnp.dot(
        grad_upper_low, in_weights, preferred_element_type=jnp.float32
    )
    fsdp_count = lax.axis_size("fsdp")
    mlp_height = 2 * hidden // (fsdp_count * seq_count)
    mlp_groups = hidden // (seq_count * mlp_height)

    def own_rows(rows):
        blocks = rows.reshape((mlp_groups, seq_count, mlp_height) + rows.shape[1:])
        picked = lax.dynamic_index_in_dim(blocks, seq_index, axis=1, keepdims=False)
        return picked.reshape((mlp_groups * mlp_height,) + rows.shape[1:])

    grad_mlp_seg = lax.all_gather(grad_mlp_low, "seq", axis=0, tiled=True)
    upper_own = contract_cols(normed_seg, own_rows(in_weights)) + own_rows(bias_up)
    active_own = jax.nn.gelu(upper_own, approximate=False).astype(jnp.bfloat16)
    grad_active_own = contract_cols(grad_mlp_seg, own_rows(down_weights))
    grad_upper_own = (grad_active_own * gelu_slope(upper_own)).astype(jnp.bfloat16)
    grad_in_own = contract_rows(grad_upper_own, normed_seg)
    grad_down_own = contract_rows(active_own, grad_mlp_seg)
    mlp_stack = jnp.concatenate(
        [
            grad_in_own.reshape(mlp_groups, mlp_height, model_width),
            grad_down_own.reshape(mlp_groups, mlp_height, model_width),
        ],
        axis=0,
    )
    mlp_shard = lax.psum_scatter(mlp_stack, "fsdp", scatter_dimension=0, tiled=True)[0]
    grad_resid_one, grad_gain_one, grad_shift_one = norm_backward(
        grad_normed, scaled_one, inverse_one, gain_one
    )
    grad_branch_low = grad_resid_one.astype(jnp.bfloat16)
    grad_bias_o = jnp.sum(grad_branch_low.astype(jnp.float32), axis=0)
    block_height = 4 * model_width // (fsdp_count * seq_count)
    out_blocks = model_width // (seq_count * block_height)
    out_rows = lax.psum_scatter(
        contract_rows(attn_mixed, grad_branch_low).reshape(
            out_blocks, seq_count, block_height, model_width
        ),
        "seq",
        scatter_dimension=1,
        tiled=True,
    )[:, 0]
    grad_mixed_low = contract_cols(grad_branch_low, out_weights).astype(jnp.bfloat16)
    grad_split = grad_mixed_low.reshape(tokens, 1, seq_count, local_heads, head_size)
    grad_heads = lax.all_to_all(grad_split, "seq", split_axis=2, concat_axis=0, tiled=True)
    head_inputs = head_piece[:, :, 0]
    head_grad = grad_heads[:, 0, 0]
    queries = head_inputs[:, 0]
    key_rows = head_inputs[:, 1]
    value_rows = head_inputs[:, 2]
    query_blocks = queries.reshape(block_count, block_rows, local_heads, head_size)
    grad_blocks = head_grad.reshape(block_count, block_rows, local_heads, head_size)
    log_blocks = log_total.reshape(block_count, block_rows, local_heads)

    def back_block(running, block_inputs):
        grad_keys, grad_values = running
        query_part, grad_part, log_part, doc_part = block_inputs
        scores = attend_block(query_part, key_rows, doc_part, segment_doc, score_scale)
        probs = jnp.exp(scores - jnp.transpose(log_part)[:, :, None])
        grad_probs = jnp.einsum(
            "qhd,khd->hqk", grad_part, value_rows, preferred_element_type=jnp.float32
        )
        row_inner = jnp.sum(grad_probs * probs, axis=-1, keepdims=True)
        grad_scores = (probs * (grad_probs - row_inner)).astype(jnp.bfloat16)
        grad_query = (
            jnp.einsum("hqk,khd->qhd", grad_scores, key_rows, preferred_element_type=jnp.float32)
            * score_scale
        )
        grad_keys = (
            grad_keys
            + jnp.einsum(
                "hqk,qhd->khd", grad_scores, query_part, preferred_element_type=jnp.float32
            )
            * score_scale
        )
        grad_values = grad_values + jnp.einsum(
            "hqk,qhd->khd",
            probs.astype(jnp.bfloat16),
            grad_part,
            preferred_element_type=jnp.float32,
        )
        return ((grad_keys, grad_values), grad_query)

    zeros_head = jnp.zeros((seg_len, local_heads, head_size), jnp.float32)
    (grad_keys, grad_values), grad_queries = lax.scan(
        back_block, (zeros_head, zeros_head), (query_blocks, grad_blocks, log_blocks, doc_blocks)
    )
    grad_queries = grad_queries.reshape(seg_len, local_heads, head_size)
    head_grads = jnp.stack([grad_queries, grad_keys, grad_values], axis=1).astype(jnp.bfloat16)
    head_weight_grads = jnp.einsum(
        "td,tihe->dihe", segment_in, head_grads, preferred_element_type=jnp.float32
    )
    qkv_blocks = 3 * out_blocks
    head_width = local_heads * head_size
    by_row = jnp.transpose(head_weight_grads.reshape(model_width, 3, head_width), (1, 0, 2))
    row_blocks = lax.all_to_all(
        by_row.reshape(qkv_blocks, seq_count, block_height, head_width),
        "seq", split_axis=1, concat_axis=1, tiled=True,
    )
    qkv_rows = jnp.transpose(row_blocks, (0, 2, 1, 3)).reshape(qkv_blocks, block_height, model_width)
    head_grads = head_grads[:, :, None]
    token_grads = lax.all_to_all(head_grads, "seq", split_axis=0, concat_axis=2, tiled=True)
    grad_qkv = token_grads.reshape(tokens, 3, model_width)
    input_grad = grad_resid_one + jnp.einsum(
        "tie,ide->td", grad_qkv, qkv_weights, preferred_element_type=jnp.float32
    )
    grad_bias_qkv = jnp.sum(grad_qkv.astype(jnp.float32), axis=0)
    grad_vector = jnp.concatenate(
        [
            grad_bias_qkv[0],
            grad_bias_qkv[2],
            grad_bias_o,
            grad_gain_one,
            grad_shift_one,
            grad_bias_two,
            grad_gain_two,
            grad_shift_two,
            grad_bias_up,
        ]
    )
    grad_attn_rows = jnp.concatenate([qkv_rows, out_rows], axis=0)
    attn_shard, mlp_shard, vector_shard = (
        attn_sum(grad_attn_rows),
        mlp_shard,
        scatter_sum(grad_vector),
    )
    return (
        layer_values.astype(jnp.bfloat16),
        input_grad,
        attn_shard,
        mlp_shard,
        vector_shard,
        rms_values,
    )


def solution(mesh):
    in_specs = (
        P(("fsdp", "seq"), None),
        P(("fsdp", "seq"), None),
        P("fsdp", None),
        P("fsdp"),
        P(("fsdp", "seq"), None),
        P(("fsdp", "seq"), None),
        P(("fsdp", "seq")),
    )
    out_specs = (
        P(("fsdp", "seq"), None),
        P(("fsdp", "seq"), None),
        P(("fsdp", "seq"), None),
        P(("fsdp", "seq"), None),
        P(("fsdp", "seq")),
        P(),
    )
    return jax.shard_map(
        layer_body, mesh=mesh, in_specs=in_specs, out_specs=out_specs, check_vma=False
    )
```

```python
import jax
import jax.numpy as jnp
from jax import lax
from jax.sharding import PartitionSpec as P


H = 16


EPSILON = 1e-05
ROOT_HALF = 0.7071067811865476
INV_ROOT_TWO_PI = 0.3989422804014327


def norm_forward(values, norm_gain, norm_shift):
    row_mean = jnp.mean(values, axis=1, keepdims=True)
    centered = values - row_mean
    inverse = lax.rsqrt(jnp.mean(centered * centered, axis=1, keepdims=True) + EPSILON)
    scaled = centered * inverse
    return (scaled * norm_gain + norm_shift, scaled, inverse)


def norm_backward(gradient, scaled, inverse, norm_gain):
    grad_scaled = gradient * norm_gain
    grad_mean = jnp.mean(grad_scaled, axis=1, keepdims=True)
    grad_along = jnp.mean(grad_scaled * scaled, axis=1, keepdims=True)
    grad_rows = inverse * (grad_scaled - grad_mean - scaled * grad_along)
    return (grad_rows, jnp.sum(gradient * scaled, axis=0), jnp.sum(gradient, axis=0))


def gelu_slope(entries):
    return 0.5 * (1.0 + lax.erf(entries * ROOT_HALF)) + entries * INV_ROOT_TWO_PI * jnp.exp(
        -0.5 * entries * entries
    )


def attend_block(queries, key_rows, query_doc, key_doc, score_scale):
    scores = (
        jnp.einsum("qhd,khd->hqk", queries, key_rows, preferred_element_type=jnp.float32)
        * score_scale
    )
    same_doc = query_doc[:, None] == key_doc[None, :]
    return jnp.where(same_doc[None], scores, -1e30)


def attn_sum(values):
    return lax.psum_scatter(values, "fsdp", scatter_dimension=0, tiled=True)[0]


def contract_rows(left, right):
    return lax.dot_general(
        left, right, (((0,), (0,)), ((), ())), preferred_element_type=jnp.float32
    )


def contract_cols(left, right):
    return lax.dot_general(
        left, right, (((1,), (1,)), ((), ())), preferred_element_type=jnp.float32
    )


def layer_body(layer_in, cotangent, doc_ids, valid_len, attn_weights, mlp_weights, param_vector):
    seq_count = lax.axis_size("seq")
    seq_index = lax.axis_index("seq")
    tokens, model_width = layer_in.shape
    head_size = model_width // H
    local_heads = H // seq_count
    score_scale = head_size ** (-0.5)
    attn_full, mlp_full, vector_full = (
        lax.all_gather(attn_weights, ("fsdp", "seq"), axis=0, tiled=True),
        lax.all_gather(mlp_weights, ("fsdp", "seq"), axis=0, tiled=True),
        lax.all_gather(param_vector, ("fsdp", "seq"), axis=0, tiled=True),
    )
    hidden = mlp_full.shape[0] // 2
    vector_wide = vector_full.astype(jnp.float32)
    pieces = [
        vector_wide[slot_index * model_width : (slot_index + 1) * model_width]
        for slot_index in range(8)
    ]
    bias_q, bias_v, bias_o, gain_one, shift_one, bias_two, gain_two, shift_two = pieces
    bias_up = vector_wide[8 * model_width :]
    qkv_weights = attn_full[: 3 * model_width].reshape(3, model_width, model_width)
    out_weights = attn_full[3 * model_width :]
    in_weights = mlp_full[:hidden]
    down_weights = mlp_full[hidden:]
    segment_in = lax.all_gather(layer_in, "seq", axis=0, tiled=True)
    segment_doc = doc_ids[0]
    seg_len = segment_doc.shape[0]
    block_rows = min(512, seg_len)
    block_count = seg_len // block_rows
    doc_blocks = segment_doc.reshape(block_count, block_rows)
    positions = seq_index * tokens + lax.iota(jnp.int32, tokens)
    valid_rows = (positions < valid_len[0]).astype(jnp.float32)[:, None]
    zero_row = jnp.zeros((1, model_width), jnp.float32)
    qkv_bias = jnp.concatenate([bias_q[None], zero_row, bias_v[None]], axis=0)
    projected = (
        jnp.einsum("td,ide->tie", layer_in, qkv_weights, preferred_element_type=jnp.float32)
        + qkv_bias[None]
    )
    qkv_split = projected.astype(jnp.bfloat16).reshape(tokens, 3, seq_count, local_heads, head_size)
    head_piece = lax.all_to_all(qkv_split, "seq", split_axis=2, concat_axis=0, tiled=True)
    queries = head_piece[:, 0, 0]
    attend_key_rows = head_piece[:, 1, 0]
    attend_value_rows = head_piece[:, 2, 0]
    head_count = queries.shape[1]
    query_blocks = queries.reshape(block_count, block_rows, head_count, head_size)

    def one_block(block_pair):
        query_part, doc_part = block_pair
        scores = attend_block(query_part, attend_key_rows, doc_part, segment_doc, score_scale)
        top_score = jnp.max(scores, axis=-1, keepdims=True)
        exponent = jnp.exp(scores - top_score)
        row_total = jnp.sum(exponent, axis=-1, keepdims=True)
        weights_low = (exponent / row_total).astype(jnp.bfloat16)
        mixed_part = jnp.einsum(
            "hqk,khd->qhd", weights_low, attend_value_rows, preferred_element_type=jnp.float32
        )
        return (mixed_part, (top_score + jnp.log(row_total))[..., 0])

    mixed_rows, log_total = lax.map(one_block, (query_blocks, doc_blocks))
    mixed_rows = mixed_rows.reshape(seg_len, 1, head_count, head_size).astype(jnp.bfloat16)
    log_total = jnp.transpose(log_total, (0, 2, 1)).reshape(seg_len, 1, head_count)
    token_mixed = lax.all_to_all(mixed_rows, "seq", split_axis=0, concat_axis=1, tiled=True)
    attn_mixed = token_mixed.reshape(tokens, model_width)
    branch = jnp.dot(attn_mixed, out_weights, preferred_element_type=jnp.float32) + bias_o
    resid_one = layer_in.astype(jnp.float32) + branch
    normed, scaled_one, inverse_one = norm_forward(resid_one, gain_one, shift_one)
    normed_low = normed.astype(jnp.bfloat16)
    normed_seg = lax.all_gather(normed_low, "seq", axis=0, tiled=True)
    upper = contract_cols(normed_low, in_weights) + bias_up
    active_low = jax.nn.gelu(upper, approximate=False).astype(jnp.bfloat16)
    mlp_branch = jnp.dot(active_low, down_weights, preferred_element_type=jnp.float32) + bias_two
    resid_two = normed + mlp_branch
    layer_values, scaled_two, inverse_two = norm_forward(resid_two, gain_two, shift_two)
    squares = jnp.stack(
        [
            jnp.sum(valid_rows * resid_one * resid_one),
            jnp.sum(valid_rows * branch * branch),
            jnp.sum(valid_rows * resid_two * resid_two),
            jnp.sum(valid_rows * mlp_branch * mlp_branch),
        ]
    )
    square_sums, valid_total = lax.psum((squares, jnp.sum(valid_rows)), ("fsdp", "seq"))
    square_sums, valid_total, cotangent = lax.optimization_barrier(
        (square_sums, valid_total, cotangent)
    )
    grad_out = cotangent.astype(jnp.float32)
    grad_resid_two, grad_gain_two, grad_shift_two = norm_backward(
        grad_out, scaled_two, inverse_two, gain_two
    )
    grad_mlp_low = grad_resid_two.astype(jnp.bfloat16)
    grad_bias_two = jnp.sum(grad_mlp_low.astype(jnp.float32), axis=0)
    grad_active = contract_cols(grad_mlp_low, down_weights)
    grad_upper_low = (grad_active * gelu_slope(upper)).astype(jnp.bfloat16)
    grad_bias_up = jnp.sum(grad_upper_low.astype(jnp.float32), axis=0)
    grad_normed = grad_resid_two + jnp.dot(
        grad_upper_low, in_weights, preferred_element_type=jnp.float32
    )
    fsdp_count = lax.axis_size("fsdp")
    mlp_height = 2 * hidden // (fsdp_count * seq_count)
    mlp_groups = hidden // (seq_count * mlp_height)

    def own_rows(rows):
        blocks = rows.reshape((mlp_groups, seq_count, mlp_height) + rows.shape[1:])
        picked = lax.dynamic_index_in_dim(blocks, seq_index, axis=1, keepdims=False)
        return picked.reshape((mlp_groups * mlp_height,) + rows.shape[1:])

    grad_mlp_seg = lax.all_gather(grad_mlp_low, "seq", axis=0, tiled=True)
    upper_own = contract_cols(normed_seg, own_rows(in_weights)) + own_rows(bias_up)
    active_own = jax.nn.gelu(upper_own, approximate=False).astype(jnp.bfloat16)
    grad_active_own = contract_cols(grad_mlp_seg, own_rows(down_weights))
    grad_upper_own = (grad_active_own * gelu_slope(upper_own)).astype(jnp.bfloat16)
    grad_in_own = contract_rows(grad_upper_own, normed_seg)
    grad_down_own = contract_rows(active_own, grad_mlp_seg)
    mlp_stack = jnp.concatenate(
        [
            grad_in_own.reshape(mlp_groups, mlp_height, model_width),
            grad_down_own.reshape(mlp_groups, mlp_height, model_width),
        ],
        axis=0,
    )
    mlp_shard = lax.psum_scatter(mlp_stack, "fsdp", scatter_dimension=0, tiled=True)[0]
    grad_resid_one, grad_gain_one, grad_shift_one = norm_backward(
        grad_normed, scaled_one, inverse_one, gain_one
    )
    grad_branch_low = grad_resid_one.astype(jnp.bfloat16)
    grad_bias_o = jnp.sum(grad_branch_low.astype(jnp.float32), axis=0)
    block_height = 4 * model_width // (fsdp_count * seq_count)
    out_blocks = model_width // (seq_count * block_height)
    out_rows = lax.psum_scatter(
        contract_rows(attn_mixed, grad_branch_low).reshape(
            out_blocks, seq_count, block_height, model_width
        ),
        "seq",
        scatter_dimension=1,
        tiled=True,
    )[:, 0]
    grad_mixed_low = contract_cols(grad_branch_low, out_weights).astype(jnp.bfloat16)
    grad_split = grad_mixed_low.reshape(tokens, 1, seq_count, local_heads, head_size)
    grad_heads = lax.all_to_all(grad_split, "seq", split_axis=2, concat_axis=0, tiled=True)
    head_inputs = head_piece[:, :, 0]
    head_grad = grad_heads[:, 0, 0]
    queries = head_inputs[:, 0]
    key_rows = head_inputs[:, 1]
    value_rows = head_inputs[:, 2]
    query_blocks = queries.reshape(block_count, block_rows, local_heads, head_size)
    grad_blocks = head_grad.reshape(block_count, block_rows, local_heads, head_size)
    log_blocks = log_total.reshape(block_count, block_rows, local_heads)

    def back_block(running, block_inputs):
        grad_keys, grad_values = running
        query_part, grad_part, log_part, doc_part = block_inputs
        scores = attend_block(query_part, key_rows, doc_part, segment_doc, score_scale)
        probs = jnp.exp(scores - jnp.transpose(log_part)[:, :, None])
        grad_probs = jnp.einsum(
            "qhd,khd->hqk", grad_part, value_rows, preferred_element_type=jnp.float32
        )
        row_inner = jnp.sum(grad_probs * probs, axis=-1, keepdims=True)
        grad_scores = (probs * (grad_probs - row_inner)).astype(jnp.bfloat16)
        grad_query = (
            jnp.einsum("hqk,khd->qhd", grad_scores, key_rows, preferred_element_type=jnp.float32)
            * score_scale
        )
        grad_keys = (
            grad_keys
            + jnp.einsum(
                "hqk,qhd->khd", grad_scores, query_part, preferred_element_type=jnp.float32
            )
            * score_scale
        )
        grad_values = grad_values + jnp.einsum(
            "hqk,qhd->khd",
            probs.astype(jnp.bfloat16),
            grad_part,
            preferred_element_type=jnp.float32,
        )
        return ((grad_keys, grad_values), grad_query)

    zeros_head = jnp.zeros((seg_len, local_heads, head_size), jnp.float32)
    (grad_keys, grad_values), grad_queries = lax.scan(
        back_block, (zeros_head, zeros_head), (query_blocks, grad_blocks, log_blocks, doc_blocks)
    )
    grad_queries = grad_queries.reshape(seg_len, local_heads, head_size)
    head_grads = jnp.stack([grad_queries, grad_keys, grad_values], axis=1).astype(jnp.bfloat16)
    head_weight_grads = jnp.einsum(
        "td,tihe->dihe", segment_in, head_grads, preferred_element_type=jnp.float32
    )
    qkv_blocks = 3 * out_blocks
    head_width = local_heads * head_size
    head_bias_sums = jnp.sum(head_grads.astype(jnp.float32), axis=0).reshape(3, head_width)
    bias_qv = lax.dynamic_update_slice(
        jnp.zeros((2, model_width), jnp.float32),
        head_bias_sums[::2],
        (0, seq_index * head_width),
    )
    grad_vector = jnp.concatenate(
        [
            bias_qv.reshape(-1),
            grad_bias_o,
            grad_gain_one,
            grad_shift_one,
            grad_bias_two,
            grad_gain_two,
            grad_shift_two,
            grad_bias_up,
        ]
    )
    slot = grad_vector.shape[0] // (fsdp_count * seq_count)
    vector_part = jnp.transpose(grad_vector.reshape(fsdp_count, seq_count, slot), (1, 0, 2))
    by_row = jnp.transpose(head_weight_grads.reshape(model_width, 3, head_width), (1, 0, 2))
    row_part = jnp.transpose(
        by_row.reshape(qkv_blocks, seq_count, block_height, head_width), (1, 0, 2, 3)
    )
    row_size = qkv_blocks * block_height * head_width
    exchanged = lax.all_to_all(
        jnp.concatenate(
            [row_part.reshape(seq_count, -1), vector_part.reshape(seq_count, -1)], axis=1
        ),
        "seq", split_axis=0, concat_axis=0, tiled=True,
    )
    row_blocks = exchanged[:, :row_size].reshape(seq_count, qkv_blocks, block_height, head_width)
    qkv_rows = jnp.transpose(row_blocks, (1, 2, 0, 3)).reshape(qkv_blocks, block_height, model_width)
    vector_rows = jnp.sum(exchanged[:, row_size:].reshape(seq_count, fsdp_count, slot), axis=0)
    vector_rows = jnp.pad(vector_rows, ((0, 0), (0, model_width - slot)))[:, None]
    head_grads = head_grads[:, :, None]
    token_grads = lax.all_to_all(head_grads, "seq", split_axis=0, concat_axis=2, tiled=True)
    grad_qkv = token_grads.reshape(tokens, 3, model_width)
    input_grad = grad_resid_one + jnp.einsum(
        "tie,ide->td", grad_qkv, qkv_weights, preferred_element_type=jnp.float32
    )
    grad_attn_rows = jnp.concatenate([qkv_rows, out_rows], axis=0)
    summed = attn_sum(jnp.concatenate([grad_attn_rows, vector_rows], axis=1))
    attn_shard = summed[:block_height]
    vector_shard = summed[block_height, :slot]
    rms_values = jnp.sqrt(square_sums / (valid_total * model_width))
    return (
        layer_values.astype(jnp.bfloat16),
        input_grad,
        attn_shard,
        mlp_shard,
        vector_shard,
        rms_values,
    )


def solution(mesh):
    in_specs = (
        P(("fsdp", "seq"), None),
        P(("fsdp", "seq"), None),
        P("fsdp", None),
        P("fsdp"),
        P(("fsdp", "seq"), None),
        P(("fsdp", "seq"), None),
        P(("fsdp", "seq")),
    )
    out_specs = (
        P(("fsdp", "seq"), None),
        P(("fsdp", "seq"), None),
        P(("fsdp", "seq"), None),
        P(("fsdp", "seq"), None),
        P(("fsdp", "seq")),
        P(),
    )
    return jax.shard_map(
        layer_body, mesh=mesh, in_specs=in_specs, out_specs=out_specs, check_vma=False
    )
```

```python
import functools
import jax
import jax.numpy as jnp
from jax import lax
from jax.sharding import PartitionSpec as P

from jax.experimental import pallas as pl
from jax.experimental.pallas import tpu as pltpu


H = 16

BLOCK = 256
NEG = -1e30


def key_ranges(segment_doc, block):
    firsts = segment_doc[::block]
    lasts = segment_doc[block - 1 :: block]
    starts = jnp.sum(segment_doc[None, :] < firsts[:, None], axis=1).astype(jnp.int32)
    ends = jnp.sum(segment_doc[None, :] <= lasts[:, None], axis=1).astype(jnp.int32)
    return starts // block, (ends + block - 1) // block


def _scores(q, k, doc_q, doc_k, scale):
    s = lax.dot_general(q, k, (((1,), (1,)), ((), ())), preferred_element_type=jnp.float32) * scale
    return jnp.where(doc_q == doc_k, s, NEG)


def _fwd_kernel(lo_ref, hi_ref, q_ref, k_ref, v_ref, dq_ref, dk_ref, out_ref, lse_ref, *, scale, block):
    i = pl.program_id(1)
    lo = lo_ref[i]
    hi = hi_ref[i]
    q = q_ref[...]
    doc_q = dq_ref[...]

    def pass_one(kb, carry):
        m, l = carry
        start = pl.multiple_of(kb * block, block)
        s = _scores(q, k_ref[pl.ds(start, block), :], doc_q, dk_ref[:, pl.ds(start, block)], scale)
        m_new = jnp.maximum(m, jnp.max(s, axis=1, keepdims=True))
        l = l * jnp.exp(m - m_new) + jnp.sum(jnp.exp(s - m_new), axis=1, keepdims=True)
        return m_new, l

    rows = q.shape[0]
    m, l = lax.fori_loop(
        lo, hi, pass_one,
        (jnp.full((rows, 1), NEG, jnp.float32), jnp.zeros((rows, 1), jnp.float32)),
    )

    def pass_two(kb, acc):
        start = pl.multiple_of(kb * block, block)
        s = _scores(q, k_ref[pl.ds(start, block), :], doc_q, dk_ref[:, pl.ds(start, block)], scale)
        p = (jnp.exp(s - m) / l).astype(jnp.bfloat16)
        return acc + jnp.dot(p, v_ref[pl.ds(start, block), :], preferred_element_type=jnp.float32)

    acc = lax.fori_loop(lo, hi, pass_two, jnp.zeros(out_ref.shape, jnp.float32))
    out_ref[...] = acc.astype(out_ref.dtype)
    lse_ref[...] = m + jnp.log(l)


def attn_forward(q, k, v, segment_doc, scale, block=BLOCK):
    heads, seg_len, d = q.shape
    lo, hi = key_ranges(segment_doc, block)
    doc_col = segment_doc.reshape(seg_len, 1)
    doc_row = segment_doc.reshape(1, seg_len)
    grid = (heads, seg_len // block)
    spec_q = pl.BlockSpec((None, block, d), lambda h, i, lo, hi: (h, i, 0))
    spec_kv = pl.BlockSpec((None, seg_len, d), lambda h, i, lo, hi: (h, 0, 0))
    spec_dq = pl.BlockSpec((block, 1), lambda h, i, lo, hi: (i, 0))
    spec_dk = pl.BlockSpec((1, seg_len), lambda h, i, lo, hi: (0, 0))
    spec_lse = pl.BlockSpec((None, block, 1), lambda h, i, lo, hi: (h, i, 0))
    return pl.pallas_call(
        functools.partial(_fwd_kernel, scale=scale, block=block),
        grid_spec=pltpu.PrefetchScalarGridSpec(
            num_scalar_prefetch=2,
            grid=grid,
            in_specs=[spec_q, spec_kv, spec_kv, spec_dq, spec_dk],
            out_specs=[spec_q, spec_lse],
        ),
        out_shape=[
            jax.ShapeDtypeStruct((heads, seg_len, d), jnp.bfloat16),
            jax.ShapeDtypeStruct((heads, seg_len, 1), jnp.float32),
        ],
        compiler_params=pltpu.CompilerParams(dimension_semantics=("arbitrary", "arbitrary")),
    )(lo, hi, q, k, v, doc_col, doc_row)


def _bwd_kernel(lo_ref, hi_ref, q_ref, k_ref, v_ref, da_ref, lse_ref, dq_ref, dk_ref,
                gq_ref, gk_ref, gv_ref, *, scale, block):
    i = pl.program_id(1)
    lo = lo_ref[i]
    hi = hi_ref[i]

    @pl.when(i == 0)
    def _():
        gk_ref[...] = jnp.zeros(gk_ref.shape, gk_ref.dtype)
        gv_ref[...] = jnp.zeros(gv_ref.shape, gv_ref.dtype)

    q = q_ref[...]
    da = da_ref[...]
    lse = lse_ref[...]
    doc_q = dq_ref[...]

    def probs(start):
        s = _scores(q, k_ref[pl.ds(start, block), :], doc_q, dk_ref[:, pl.ds(start, block)], scale)
        p = jnp.exp(s - lse)
        dp = lax.dot_general(da, v_ref[pl.ds(start, block), :], (((1,), (1,)), ((), ())),
                             preferred_element_type=jnp.float32)
        return p, dp

    def pass_one(kb, delta):
        start = pl.multiple_of(kb * block, block)
        p, dp = probs(start)
        return delta + jnp.sum(dp * p, axis=1, keepdims=True)

    rows = q.shape[0]
    delta = lax.fori_loop(lo, hi, pass_one, jnp.zeros((rows, 1), jnp.float32))

    def pass_two(kb, gq):
        start = pl.multiple_of(kb * block, block)
        p, dp = probs(start)
        ds = (p * (dp - delta)).astype(jnp.bfloat16)
        pb = p.astype(jnp.bfloat16)
        k_blk = k_ref[pl.ds(start, block), :]
        gq = gq + jnp.dot(ds, k_blk, preferred_element_type=jnp.float32)
        gk_ref[pl.ds(start, block), :] += lax.dot_general(
            ds, q, (((0,), (0,)), ((), ())), preferred_element_type=jnp.float32)
        gv_ref[pl.ds(start, block), :] += lax.dot_general(
            pb, da, (((0,), (0,)), ((), ())), preferred_element_type=jnp.float32)
        return gq

    gq = lax.fori_loop(lo, hi, pass_two, jnp.zeros(gq_ref.shape, jnp.float32))
    gq_ref[...] = gq * scale

    @pl.when(i == pl.num_programs(1) - 1)
    def _():
        gk_ref[...] = gk_ref[...] * scale


def attn_backward(q, k, v, da, lse, segment_doc, scale, block=BLOCK):
    heads, seg_len, d = q.shape
    lo, hi = key_ranges(segment_doc, block)
    doc_col = segment_doc.reshape(seg_len, 1)
    doc_row = segment_doc.reshape(1, seg_len)
    grid = (heads, seg_len // block)
    spec_q = pl.BlockSpec((None, block, d), lambda h, i, lo, hi: (h, i, 0))
    spec_kv = pl.BlockSpec((None, seg_len, d), lambda h, i, lo, hi: (h, 0, 0))
    spec_dq = pl.BlockSpec((block, 1), lambda h, i, lo, hi: (i, 0))
    spec_dk = pl.BlockSpec((1, seg_len), lambda h, i, lo, hi: (0, 0))
    spec_lse = pl.BlockSpec((None, block, 1), lambda h, i, lo, hi: (h, i, 0))
    return pl.pallas_call(
        functools.partial(_bwd_kernel, scale=scale, block=block),
        grid_spec=pltpu.PrefetchScalarGridSpec(
            num_scalar_prefetch=2,
            grid=grid,
            in_specs=[spec_q, spec_kv, spec_kv, spec_q, spec_lse, spec_dq, spec_dk],
            out_specs=[spec_q, spec_kv, spec_kv],
        ),
        out_shape=[jax.ShapeDtypeStruct((heads, seg_len, d), jnp.float32)] * 3,
        compiler_params=pltpu.CompilerParams(dimension_semantics=("arbitrary", "arbitrary")),
    )(lo, hi, q, k, v, da, lse, doc_col, doc_row)


EPSILON = 1e-05
ROOT_HALF = 0.7071067811865476
INV_ROOT_TWO_PI = 0.3989422804014327


def norm_forward(values, norm_gain, norm_shift):
    row_mean = jnp.mean(values, axis=1, keepdims=True)
    centered = values - row_mean
    inverse = lax.rsqrt(jnp.mean(centered * centered, axis=1, keepdims=True) + EPSILON)
    scaled = centered * inverse
    return (scaled * norm_gain + norm_shift, scaled, inverse)


def norm_backward(gradient, scaled, inverse, norm_gain):
    grad_scaled = gradient * norm_gain
    grad_mean = jnp.mean(grad_scaled, axis=1, keepdims=True)
    grad_along = jnp.mean(grad_scaled * scaled, axis=1, keepdims=True)
    grad_rows = inverse * (grad_scaled - grad_mean - scaled * grad_along)
    return (grad_rows, jnp.sum(gradient * scaled, axis=0), jnp.sum(gradient, axis=0))


def gelu_slope(entries):
    return 0.5 * (1.0 + lax.erf(entries * ROOT_HALF)) + entries * INV_ROOT_TWO_PI * jnp.exp(
        -0.5 * entries * entries
    )


def attn_sum(values):
    return lax.psum_scatter(values, "fsdp", scatter_dimension=0, tiled=True)[0]


def contract_rows(left, right):
    return lax.dot_general(
        left, right, (((0,), (0,)), ((), ())), preferred_element_type=jnp.float32
    )


def contract_cols(left, right):
    return lax.dot_general(
        left, right, (((1,), (1,)), ((), ())), preferred_element_type=jnp.float32
    )


def layer_body(layer_in, cotangent, doc_ids, valid_len, attn_weights, mlp_weights, param_vector):
    seq_count = lax.axis_size("seq")
    seq_index = lax.axis_index("seq")
    tokens, model_width = layer_in.shape
    head_size = model_width // H
    local_heads = H // seq_count
    score_scale = head_size ** (-0.5)
    attn_full, mlp_full, vector_full = (
        lax.all_gather(attn_weights, ("fsdp", "seq"), axis=0, tiled=True),
        lax.all_gather(mlp_weights, ("fsdp", "seq"), axis=0, tiled=True),
        lax.all_gather(param_vector, ("fsdp", "seq"), axis=0, tiled=True),
    )
    hidden = mlp_full.shape[0] // 2
    vector_wide = vector_full.astype(jnp.float32)
    pieces = [
        vector_wide[slot_index * model_width : (slot_index + 1) * model_width]
        for slot_index in range(8)
    ]
    bias_q, bias_v, bias_o, gain_one, shift_one, bias_two, gain_two, shift_two = pieces
    bias_up = vector_wide[8 * model_width :]
    qkv_weights = attn_full[: 3 * model_width].reshape(3, model_width, model_width)
    out_weights = attn_full[3 * model_width :]
    in_weights = mlp_full[:hidden]
    down_weights = mlp_full[hidden:]
    segment_in = lax.all_gather(layer_in, "seq", axis=0, tiled=True)
    segment_doc = doc_ids[0]
    seg_len = segment_doc.shape[0]
    positions = seq_index * tokens + lax.iota(jnp.int32, tokens)
    valid_rows = (positions < valid_len[0]).astype(jnp.float32)[:, None]
    zero_row = jnp.zeros((1, model_width), jnp.float32)
    qkv_bias = jnp.concatenate([bias_q[None], zero_row, bias_v[None]], axis=0)
    projected = (
        jnp.einsum("td,ide->tie", layer_in, qkv_weights, preferred_element_type=jnp.float32)
        + qkv_bias[None]
    )
    qkv_split = projected.astype(jnp.bfloat16).reshape(tokens, 3, seq_count, local_heads, head_size)
    head_piece = lax.all_to_all(qkv_split, "seq", split_axis=2, concat_axis=0, tiled=True)
    queries = head_piece[:, 0, 0]
    attend_key_rows = head_piece[:, 1, 0]
    attend_value_rows = head_piece[:, 2, 0]
    head_count = queries.shape[1]
    by_head = lambda rows: jnp.transpose(rows, (1, 0, 2))
    head_q, head_k, head_v = by_head(queries), by_head(attend_key_rows), by_head(attend_value_rows)
    head_mixed, log_total = attn_forward(head_q, head_k, head_v, segment_doc, score_scale)
    mixed_rows = jnp.transpose(head_mixed, (1, 0, 2)).reshape(seg_len, 1, head_count, head_size)
    token_mixed = lax.all_to_all(mixed_rows, "seq", split_axis=0, concat_axis=1, tiled=True)
    attn_mixed = token_mixed.reshape(tokens, model_width)
    branch = jnp.dot(attn_mixed, out_weights, preferred_element_type=jnp.float32) + bias_o
    resid_one = layer_in.astype(jnp.float32) + branch
    normed, scaled_one, inverse_one = norm_forward(resid_one, gain_one, shift_one)
    normed_low = normed.astype(jnp.bfloat16)
    normed_seg = lax.all_gather(normed_low, "seq", axis=0, tiled=True)
    upper = contract_cols(normed_low, in_weights) + bias_up
    active_low = jax.nn.gelu(upper, approximate=False).astype(jnp.bfloat16)
    mlp_branch = jnp.dot(active_low, down_weights, preferred_element_type=jnp.float32) + bias_two
    resid_two = normed + mlp_branch
    layer_values, scaled_two, inverse_two = norm_forward(resid_two, gain_two, shift_two)
    squares = jnp.stack(
        [
            jnp.sum(valid_rows * resid_one * resid_one),
            jnp.sum(valid_rows * branch * branch),
            jnp.sum(valid_rows * resid_two * resid_two),
            jnp.sum(valid_rows * mlp_branch * mlp_branch),
        ]
    )
    square_sums, valid_total = lax.psum((squares, jnp.sum(valid_rows)), ("fsdp", "seq"))
    square_sums, valid_total, cotangent = lax.optimization_barrier(
        (square_sums, valid_total, cotangent)
    )
    grad_out = cotangent.astype(jnp.float32)
    grad_resid_two, grad_gain_two, grad_shift_two = norm_backward(
        grad_out, scaled_two, inverse_two, gain_two
    )
    grad_mlp_low = grad_resid_two.astype(jnp.bfloat16)
    grad_bias_two = jnp.sum(grad_mlp_low.astype(jnp.float32), axis=0)
    grad_active = contract_cols(grad_mlp_low, down_weights)
    grad_upper_low = (grad_active * gelu_slope(upper)).astype(jnp.bfloat16)
    grad_bias_up = jnp.sum(grad_upper_low.astype(jnp.float32), axis=0)
    grad_normed = grad_resid_two + jnp.dot(
        grad_upper_low, in_weights, preferred_element_type=jnp.float32
    )
    fsdp_count = lax.axis_size("fsdp")
    mlp_height = 2 * hidden // (fsdp_count * seq_count)
    mlp_groups = hidden // (seq_count * mlp_height)

    def own_rows(rows):
        blocks = rows.reshape((mlp_groups, seq_count, mlp_height) + rows.shape[1:])
        picked = lax.dynamic_index_in_dim(blocks, seq_index, axis=1, keepdims=False)
        return picked.reshape((mlp_groups * mlp_height,) + rows.shape[1:])

    grad_mlp_seg = lax.all_gather(grad_mlp_low, "seq", axis=0, tiled=True)
    upper_own = contract_cols(normed_seg, own_rows(in_weights)) + own_rows(bias_up)
    active_own = jax.nn.gelu(upper_own, approximate=False).astype(jnp.bfloat16)
    grad_active_own = contract_cols(grad_mlp_seg, own_rows(down_weights))
    grad_upper_own = (grad_active_own * gelu_slope(upper_own)).astype(jnp.bfloat16)
    grad_in_own = contract_rows(grad_upper_own, normed_seg)
    grad_down_own = contract_rows(active_own, grad_mlp_seg)
    mlp_stack = jnp.concatenate(
        [
            grad_in_own.reshape(mlp_groups, mlp_height, model_width),
            grad_down_own.reshape(mlp_groups, mlp_height, model_width),
        ],
        axis=0,
    )
    mlp_shard = lax.psum_scatter(mlp_stack, "fsdp", scatter_dimension=0, tiled=True)[0]
    grad_resid_one, grad_gain_one, grad_shift_one = norm_backward(
        grad_normed, scaled_one, inverse_one, gain_one
    )
    grad_branch_low = grad_resid_one.astype(jnp.bfloat16)
    grad_bias_o = jnp.sum(grad_branch_low.astype(jnp.float32), axis=0)
    block_height = 4 * model_width // (fsdp_count * seq_count)
    out_blocks = model_width // (seq_count * block_height)
    out_rows = lax.psum_scatter(
        contract_rows(attn_mixed, grad_branch_low).reshape(
            out_blocks, seq_count, block_height, model_width
        ),
        "seq",
        scatter_dimension=1,
        tiled=True,
    )[:, 0]
    grad_mixed_low = contract_cols(grad_branch_low, out_weights).astype(jnp.bfloat16)
    grad_split = grad_mixed_low.reshape(tokens, 1, seq_count, local_heads, head_size)
    grad_heads = lax.all_to_all(grad_split, "seq", split_axis=2, concat_axis=0, tiled=True)
    head_grad = by_head(grad_heads[:, 0, 0])

    grad_queries, grad_keys, grad_values = attn_backward(
        head_q, head_k, head_v, head_grad, log_total, segment_doc, score_scale
    )
    head_grads = jnp.transpose(
        jnp.stack([grad_queries, grad_keys, grad_values], axis=0), (2, 0, 1, 3)
    ).astype(jnp.bfloat16)
    head_weight_grads = jnp.einsum(
        "td,tihe->dihe", segment_in, head_grads, preferred_element_type=jnp.float32
    )
    qkv_blocks = 3 * out_blocks
    head_width = local_heads * head_size
    head_bias_sums = jnp.sum(head_grads.astype(jnp.float32), axis=0).reshape(3, head_width)
    bias_qv = lax.dynamic_update_slice(
        jnp.zeros((2, model_width), jnp.float32),
        head_bias_sums[::2],
        (0, seq_index * head_width),
    )
    grad_vector = jnp.concatenate(
        [
            bias_qv.reshape(-1),
            grad_bias_o,
            grad_gain_one,
            grad_shift_one,
            grad_bias_two,
            grad_gain_two,
            grad_shift_two,
            grad_bias_up,
        ]
    )
    slot = grad_vector.shape[0] // (fsdp_count * seq_count)
    vector_part = jnp.transpose(grad_vector.reshape(fsdp_count, seq_count, slot), (1, 0, 2))
    by_row = jnp.transpose(head_weight_grads.reshape(model_width, 3, head_width), (1, 0, 2))
    row_part = jnp.transpose(
        by_row.reshape(qkv_blocks, seq_count, block_height, head_width), (1, 0, 2, 3)
    )
    row_size = qkv_blocks * block_height * head_width
    exchanged = lax.all_to_all(
        jnp.concatenate(
            [row_part.reshape(seq_count, -1), vector_part.reshape(seq_count, -1)], axis=1
        ),
        "seq", split_axis=0, concat_axis=0, tiled=True,
    )
    row_blocks = exchanged[:, :row_size].reshape(seq_count, qkv_blocks, block_height, head_width)
    qkv_rows = jnp.transpose(row_blocks, (1, 2, 0, 3)).reshape(qkv_blocks, block_height, model_width)
    vector_rows = jnp.sum(exchanged[:, row_size:].reshape(seq_count, fsdp_count, slot), axis=0)
    vector_rows = jnp.pad(vector_rows, ((0, 0), (0, model_width - slot)))[:, None]
    head_grads = head_grads[:, :, None]
    token_grads = lax.all_to_all(head_grads, "seq", split_axis=0, concat_axis=2, tiled=True)
    grad_qkv = token_grads.reshape(tokens, 3, model_width)
    input_grad = grad_resid_one + jnp.einsum(
        "tie,ide->td", grad_qkv, qkv_weights, preferred_element_type=jnp.float32
    )
    grad_attn_rows = jnp.concatenate([qkv_rows, out_rows], axis=0)
    summed = attn_sum(jnp.concatenate([grad_attn_rows, vector_rows], axis=1))
    attn_shard = summed[:block_height]
    vector_shard = summed[block_height, :slot]
    rms_values = jnp.sqrt(square_sums / (valid_total * model_width))
    return (
        layer_values.astype(jnp.bfloat16),
        input_grad,
        attn_shard,
        mlp_shard,
        vector_shard,
        rms_values,
    )


def solution(mesh):
    in_specs = (
        P(("fsdp", "seq"), None),
        P(("fsdp", "seq"), None),
        P("fsdp", None),
        P("fsdp"),
        P(("fsdp", "seq"), None),
        P(("fsdp", "seq"), None),
        P(("fsdp", "seq")),
    )
    out_specs = (
        P(("fsdp", "seq"), None),
        P(("fsdp", "seq"), None),
        P(("fsdp", "seq"), None),
        P(("fsdp", "seq"), None),
        P(("fsdp", "seq")),
        P(),
    )
    return jax.shard_map(
        layer_body, mesh=mesh, in_specs=in_specs, out_specs=out_specs, check_vma=False
    )
```

```python
import functools
import jax
import jax.numpy as jnp
from jax import lax
from jax.sharding import PartitionSpec as P

from jax.experimental import pallas as pl
from jax.experimental.pallas import tpu as pltpu


H = 16

BLOCK = 256
NEG = -1e30


def key_ranges(segment_doc, block):
    firsts = segment_doc[::block]
    lasts = segment_doc[block - 1 :: block]
    starts = jnp.sum(segment_doc[None, :] < firsts[:, None], axis=1).astype(jnp.int32)
    ends = jnp.sum(segment_doc[None, :] <= lasts[:, None], axis=1).astype(jnp.int32)
    return starts // block, (ends + block - 1) // block


def _scores(q, k, doc_q, doc_k, scale):
    s = lax.dot_general(q, k, (((1,), (1,)), ((), ())), preferred_element_type=jnp.float32) * scale
    return jnp.where(doc_q == doc_k, s, NEG)


def _fwd_kernel(lo_ref, hi_ref, q_ref, k_ref, v_ref, dq_ref, dk_ref, out_ref, lse_ref, *, scale, block):
    i = pl.program_id(1)
    lo = lo_ref[i]
    hi = hi_ref[i]
    q = q_ref[...]
    doc_q = dq_ref[...]

    def pass_one(kb, carry):
        m, l = carry
        start = pl.multiple_of(kb * block, block)
        s = _scores(q, k_ref[pl.ds(start, block), :], doc_q, dk_ref[:, pl.ds(start, block)], scale)
        m_new = jnp.maximum(m, jnp.max(s, axis=1, keepdims=True))
        l = l * jnp.exp(m - m_new) + jnp.sum(jnp.exp(s - m_new), axis=1, keepdims=True)
        return m_new, l

    rows = q.shape[0]
    m, l = lax.fori_loop(
        lo, hi, pass_one,
        (jnp.full((rows, 1), NEG, jnp.float32), jnp.zeros((rows, 1), jnp.float32)),
    )

    def pass_two(kb, acc):
        start = pl.multiple_of(kb * block, block)
        s = _scores(q, k_ref[pl.ds(start, block), :], doc_q, dk_ref[:, pl.ds(start, block)], scale)
        p = (jnp.exp(s - m) / l).astype(jnp.bfloat16)
        return acc + jnp.dot(p, v_ref[pl.ds(start, block), :], preferred_element_type=jnp.float32)

    acc = lax.fori_loop(lo, hi, pass_two, jnp.zeros(out_ref.shape, jnp.float32))
    out_ref[...] = acc.astype(out_ref.dtype)
    lse_ref[...] = m + jnp.log(l)


def attn_forward(q, k, v, segment_doc, scale, block=BLOCK):
    heads, seg_len, d = q.shape
    lo, hi = key_ranges(segment_doc, block)
    doc_col = segment_doc.reshape(seg_len, 1)
    doc_row = segment_doc.reshape(1, seg_len)
    grid = (heads, seg_len // block)
    spec_q = pl.BlockSpec((None, block, d), lambda h, i, lo, hi: (h, i, 0))
    spec_kv = pl.BlockSpec((None, seg_len, d), lambda h, i, lo, hi: (h, 0, 0))
    spec_dq = pl.BlockSpec((block, 1), lambda h, i, lo, hi: (i, 0))
    spec_dk = pl.BlockSpec((1, seg_len), lambda h, i, lo, hi: (0, 0))
    spec_lse = pl.BlockSpec((None, block, 1), lambda h, i, lo, hi: (h, i, 0))
    return pl.pallas_call(
        functools.partial(_fwd_kernel, scale=scale, block=block),
        grid_spec=pltpu.PrefetchScalarGridSpec(
            num_scalar_prefetch=2,
            grid=grid,
            in_specs=[spec_q, spec_kv, spec_kv, spec_dq, spec_dk],
            out_specs=[spec_q, spec_lse],
        ),
        out_shape=[
            jax.ShapeDtypeStruct((heads, seg_len, d), jnp.bfloat16),
            jax.ShapeDtypeStruct((heads, seg_len, 1), jnp.float32),
        ],
        compiler_params=pltpu.CompilerParams(dimension_semantics=("arbitrary", "arbitrary")),
    )(lo, hi, q, k, v, doc_col, doc_row)


def _bwd_kernel(lo_ref, hi_ref, q_ref, k_ref, v_ref, da_ref, lse_ref, dq_ref, dk_ref,
                gq_ref, gk_ref, gv_ref, *, scale, block):
    i = pl.program_id(1)
    lo = lo_ref[i]
    hi = hi_ref[i]

    @pl.when(i == 0)
    def _():
        gk_ref[...] = jnp.zeros(gk_ref.shape, gk_ref.dtype)
        gv_ref[...] = jnp.zeros(gv_ref.shape, gv_ref.dtype)

    q = q_ref[...]
    da = da_ref[...]
    lse = lse_ref[...]
    doc_q = dq_ref[...]

    def probs(start):
        s = _scores(q, k_ref[pl.ds(start, block), :], doc_q, dk_ref[:, pl.ds(start, block)], scale)
        p = jnp.exp(s - lse)
        dp = lax.dot_general(da, v_ref[pl.ds(start, block), :], (((1,), (1,)), ((), ())),
                             preferred_element_type=jnp.float32)
        return p, dp

    def pass_one(kb, delta):
        start = pl.multiple_of(kb * block, block)
        p, dp = probs(start)
        return delta + jnp.sum(dp * p, axis=1, keepdims=True)

    rows = q.shape[0]
    delta = lax.fori_loop(lo, hi, pass_one, jnp.zeros((rows, 1), jnp.float32))

    def pass_two(kb, gq):
        start = pl.multiple_of(kb * block, block)
        p, dp = probs(start)
        ds = (p * (dp - delta)).astype(jnp.bfloat16)
        pb = p.astype(jnp.bfloat16)
        k_blk = k_ref[pl.ds(start, block), :]
        gq = gq + jnp.dot(ds, k_blk, preferred_element_type=jnp.float32)
        gk_ref[pl.ds(start, block), :] += lax.dot_general(
            ds, q, (((0,), (0,)), ((), ())), preferred_element_type=jnp.float32)
        gv_ref[pl.ds(start, block), :] += lax.dot_general(
            pb, da, (((0,), (0,)), ((), ())), preferred_element_type=jnp.float32)
        return gq

    gq = lax.fori_loop(lo, hi, pass_two, jnp.zeros(gq_ref.shape, jnp.float32))
    gq_ref[...] = gq * scale

    @pl.when(i == pl.num_programs(1) - 1)
    def _():
        gk_ref[...] = gk_ref[...] * scale


def attn_backward(q, k, v, da, lse, segment_doc, scale, block=BLOCK):
    heads, seg_len, d = q.shape
    lo, hi = key_ranges(segment_doc, block)
    doc_col = segment_doc.reshape(seg_len, 1)
    doc_row = segment_doc.reshape(1, seg_len)
    grid = (heads, seg_len // block)
    spec_q = pl.BlockSpec((None, block, d), lambda h, i, lo, hi: (h, i, 0))
    spec_kv = pl.BlockSpec((None, seg_len, d), lambda h, i, lo, hi: (h, 0, 0))
    spec_dq = pl.BlockSpec((block, 1), lambda h, i, lo, hi: (i, 0))
    spec_dk = pl.BlockSpec((1, seg_len), lambda h, i, lo, hi: (0, 0))
    spec_lse = pl.BlockSpec((None, block, 1), lambda h, i, lo, hi: (h, i, 0))
    return pl.pallas_call(
        functools.partial(_bwd_kernel, scale=scale, block=block),
        grid_spec=pltpu.PrefetchScalarGridSpec(
            num_scalar_prefetch=2,
            grid=grid,
            in_specs=[spec_q, spec_kv, spec_kv, spec_q, spec_lse, spec_dq, spec_dk],
            out_specs=[spec_q, spec_kv, spec_kv],
        ),
        out_shape=[jax.ShapeDtypeStruct((heads, seg_len, d), jnp.float32)] * 3,
        compiler_params=pltpu.CompilerParams(dimension_semantics=("arbitrary", "arbitrary")),
    )(lo, hi, q, k, v, da, lse, doc_col, doc_row)


EPSILON = 1e-05
ROOT_HALF = 0.7071067811865476
INV_ROOT_TWO_PI = 0.3989422804014327


def norm_forward(values, norm_gain, norm_shift):
    row_mean = jnp.mean(values, axis=1, keepdims=True)
    centered = values - row_mean
    inverse = lax.rsqrt(jnp.mean(centered * centered, axis=1, keepdims=True) + EPSILON)
    scaled = centered * inverse
    return (scaled * norm_gain + norm_shift, scaled, inverse)


def norm_backward(gradient, scaled, inverse, norm_gain):
    grad_scaled = gradient * norm_gain
    grad_mean = jnp.mean(grad_scaled, axis=1, keepdims=True)
    grad_along = jnp.mean(grad_scaled * scaled, axis=1, keepdims=True)
    grad_rows = inverse * (grad_scaled - grad_mean - scaled * grad_along)
    return (grad_rows, jnp.sum(gradient * scaled, axis=0), jnp.sum(gradient, axis=0))


def gelu_slope(entries):
    return 0.5 * (1.0 + lax.erf(entries * ROOT_HALF)) + entries * INV_ROOT_TWO_PI * jnp.exp(
        -0.5 * entries * entries
    )


def attn_sum(values):
    return lax.psum_scatter(values, "fsdp", scatter_dimension=0, tiled=True)[0]


def contract_rows(left, right):
    return lax.dot_general(
        left, right, (((0,), (0,)), ((), ())), preferred_element_type=jnp.float32
    )


def contract_cols(left, right):
    return lax.dot_general(
        left, right, (((1,), (1,)), ((), ())), preferred_element_type=jnp.float32
    )


def layer_body(layer_in, cotangent, doc_ids, valid_len, attn_weights, mlp_weights, param_vector):
    seq_count = lax.axis_size("seq")
    seq_index = lax.axis_index("seq")
    tokens, model_width = layer_in.shape
    head_size = model_width // H
    local_heads = H // seq_count
    score_scale = head_size ** (-0.5)
    attn_full, mlp_full, vector_full = (
        lax.all_gather(attn_weights, ("fsdp", "seq"), axis=0, tiled=True),
        lax.all_gather(mlp_weights, ("fsdp", "seq"), axis=0, tiled=True),
        lax.all_gather(param_vector, ("fsdp", "seq"), axis=0, tiled=True),
    )
    hidden = mlp_full.shape[0] // 2
    vector_wide = vector_full.astype(jnp.float32)
    pieces = [
        vector_wide[slot_index * model_width : (slot_index + 1) * model_width]
        for slot_index in range(8)
    ]
    bias_q, bias_v, bias_o, gain_one, shift_one, bias_two, gain_two, shift_two = pieces
    bias_up = vector_wide[8 * model_width :]
    qkv_weights = attn_full[: 3 * model_width].reshape(3, model_width, model_width)
    out_weights = attn_full[3 * model_width :]
    in_weights = mlp_full[:hidden]
    down_weights = mlp_full[hidden:]
    segment_in = lax.all_gather(layer_in, "seq", axis=0, tiled=True)
    segment_doc = doc_ids[0]
    seg_len = segment_doc.shape[0]
    positions = seq_index * tokens + lax.iota(jnp.int32, tokens)
    valid_rows = (positions < valid_len[0]).astype(jnp.float32)[:, None]
    zero_row = jnp.zeros((1, model_width), jnp.float32)
    qkv_bias = jnp.concatenate([bias_q[None], zero_row, bias_v[None]], axis=0)
    projected = (
        jnp.einsum("td,ide->tie", layer_in, qkv_weights, preferred_element_type=jnp.float32)
        + qkv_bias[None]
    )
    head_width = local_heads * head_size
    qkv_send = jnp.transpose(
        projected.astype(jnp.bfloat16).reshape(tokens, 3, seq_count, head_width), (2, 0, 1, 3)
    ).reshape(seq_count, tokens, 3 * head_width)
    qkv_recv = lax.all_to_all(qkv_send, "seq", split_axis=0, concat_axis=0, tiled=True)
    head_all = jnp.transpose(
        qkv_recv.reshape(seg_len, 3, local_heads, head_size), (1, 2, 0, 3)
    )
    head_q, head_k, head_v = head_all[0], head_all[1], head_all[2]
    head_mixed, log_total = attn_forward(head_q, head_k, head_v, segment_doc, score_scale)
    mixed_rows = jnp.transpose(head_mixed, (1, 0, 2)).reshape(seq_count, tokens, head_width)
    token_mixed = lax.all_to_all(mixed_rows, "seq", split_axis=0, concat_axis=0, tiled=True)
    attn_mixed = jnp.transpose(token_mixed, (1, 0, 2)).reshape(tokens, model_width)
    branch = jnp.dot(attn_mixed, out_weights, preferred_element_type=jnp.float32) + bias_o
    resid_one = layer_in.astype(jnp.float32) + branch
    normed, scaled_one, inverse_one = norm_forward(resid_one, gain_one, shift_one)
    normed_low = normed.astype(jnp.bfloat16)
    normed_seg = lax.all_gather(normed_low, "seq", axis=0, tiled=True)
    upper = contract_cols(normed_low, in_weights) + bias_up
    active_low = jax.nn.gelu(upper, approximate=False).astype(jnp.bfloat16)
    mlp_branch = jnp.dot(active_low, down_weights, preferred_element_type=jnp.float32) + bias_two
    resid_two = normed + mlp_branch
    layer_values, scaled_two, inverse_two = norm_forward(resid_two, gain_two, shift_two)
    squares = jnp.stack(
        [
            jnp.sum(valid_rows * resid_one * resid_one),
            jnp.sum(valid_rows * branch * branch),
            jnp.sum(valid_rows * resid_two * resid_two),
            jnp.sum(valid_rows * mlp_branch * mlp_branch),
        ]
    )
    square_sums, valid_total = lax.psum((squares, jnp.sum(valid_rows)), ("fsdp", "seq"))
    square_sums, valid_total, cotangent = lax.optimization_barrier(
        (square_sums, valid_total, cotangent)
    )
    grad_out = cotangent.astype(jnp.float32)
    grad_resid_two, grad_gain_two, grad_shift_two = norm_backward(
        grad_out, scaled_two, inverse_two, gain_two
    )
    grad_mlp_low = grad_resid_two.astype(jnp.bfloat16)
    grad_bias_two = jnp.sum(grad_mlp_low.astype(jnp.float32), axis=0)
    grad_active = contract_cols(grad_mlp_low, down_weights)
    grad_upper_low = (grad_active * gelu_slope(upper)).astype(jnp.bfloat16)
    grad_bias_up = jnp.sum(grad_upper_low.astype(jnp.float32), axis=0)
    grad_normed = grad_resid_two + jnp.dot(
        grad_upper_low, in_weights, preferred_element_type=jnp.float32
    )
    fsdp_count = lax.axis_size("fsdp")
    mlp_height = 2 * hidden // (fsdp_count * seq_count)
    mlp_groups = hidden // (seq_count * mlp_height)

    def own_rows(rows):
        blocks = rows.reshape((mlp_groups, seq_count, mlp_height) + rows.shape[1:])
        picked = lax.dynamic_index_in_dim(blocks, seq_index, axis=1, keepdims=False)
        return picked.reshape((mlp_groups * mlp_height,) + rows.shape[1:])

    grad_mlp_seg = lax.all_gather(grad_mlp_low, "seq", axis=0, tiled=True)
    upper_own = contract_cols(normed_seg, own_rows(in_weights)) + own_rows(bias_up)
    active_own = jax.nn.gelu(upper_own, approximate=False).astype(jnp.bfloat16)
    grad_active_own = contract_cols(grad_mlp_seg, own_rows(down_weights))
    grad_upper_own = (grad_active_own * gelu_slope(upper_own)).astype(jnp.bfloat16)
    grad_in_own = contract_rows(grad_upper_own, normed_seg)
    grad_down_own = contract_rows(active_own, grad_mlp_seg)
    mlp_stack = jnp.concatenate(
        [
            grad_in_own.reshape(mlp_groups, mlp_height, model_width),
            grad_down_own.reshape(mlp_groups, mlp_height, model_width),
        ],
        axis=0,
    )
    mlp_shard = lax.psum_scatter(mlp_stack, "fsdp", scatter_dimension=0, tiled=True)[0]
    grad_resid_one, grad_gain_one, grad_shift_one = norm_backward(
        grad_normed, scaled_one, inverse_one, gain_one
    )
    grad_branch_low = grad_resid_one.astype(jnp.bfloat16)
    grad_bias_o = jnp.sum(grad_branch_low.astype(jnp.float32), axis=0)
    block_height = 4 * model_width // (fsdp_count * seq_count)
    out_blocks = model_width // (seq_count * block_height)
    out_rows = lax.psum_scatter(
        contract_rows(attn_mixed, grad_branch_low).reshape(
            out_blocks, seq_count, block_height, model_width
        ),
        "seq",
        scatter_dimension=1,
        tiled=True,
    )[:, 0]
    grad_mixed_low = contract_cols(grad_branch_low, out_weights).astype(jnp.bfloat16)
    grad_split = jnp.transpose(
        grad_mixed_low.reshape(tokens, seq_count, head_width), (1, 0, 2)
    )
    grad_heads = lax.all_to_all(grad_split, "seq", split_axis=0, concat_axis=0, tiled=True)
    head_grad = jnp.transpose(grad_heads.reshape(seg_len, local_heads, head_size), (1, 0, 2))

    grad_queries, grad_keys, grad_values = attn_backward(
        head_q, head_k, head_v, head_grad, log_total, segment_doc, score_scale
    )
    head_grads = jnp.transpose(
        jnp.stack([grad_queries, grad_keys, grad_values], axis=0), (2, 0, 1, 3)
    ).astype(jnp.bfloat16)
    head_weight_grads = jnp.einsum(
        "td,tihe->dihe", segment_in, head_grads, preferred_element_type=jnp.float32
    )
    qkv_blocks = 3 * out_blocks
    head_bias_sums = jnp.sum(head_grads.astype(jnp.float32), axis=0).reshape(3, head_width)
    bias_qv = lax.dynamic_update_slice(
        jnp.zeros((2, model_width), jnp.float32),
        head_bias_sums[::2],
        (0, seq_index * head_width),
    )
    grad_vector = jnp.concatenate(
        [
            bias_qv.reshape(-1),
            grad_bias_o,
            grad_gain_one,
            grad_shift_one,
            grad_bias_two,
            grad_gain_two,
            grad_shift_two,
            grad_bias_up,
        ]
    )
    slot = grad_vector.shape[0] // (fsdp_count * seq_count)
    vector_part = jnp.transpose(grad_vector.reshape(fsdp_count, seq_count, slot), (1, 0, 2))
    by_row = jnp.transpose(head_weight_grads.reshape(model_width, 3, head_width), (1, 0, 2))
    row_part = jnp.transpose(
        by_row.reshape(qkv_blocks, seq_count, block_height, head_width), (1, 0, 2, 3)
    )
    row_size = qkv_blocks * block_height * head_width
    exchanged = lax.all_to_all(
        jnp.concatenate(
            [row_part.reshape(seq_count, -1), vector_part.reshape(seq_count, -1)], axis=1
        ),
        "seq", split_axis=0, concat_axis=0, tiled=True,
    )
    row_blocks = exchanged[:, :row_size].reshape(seq_count, qkv_blocks, block_height, head_width)
    qkv_rows = jnp.transpose(row_blocks, (1, 2, 0, 3)).reshape(qkv_blocks, block_height, model_width)
    vector_rows = jnp.sum(exchanged[:, row_size:].reshape(seq_count, fsdp_count, slot), axis=0)
    vector_rows = jnp.pad(vector_rows, ((0, 0), (0, model_width - slot)))[:, None]
    token_grads = lax.all_to_all(
        head_grads.reshape(seq_count, tokens, 3 * head_width),
        "seq", split_axis=0, concat_axis=0, tiled=True,
    )
    grad_qkv = jnp.transpose(
        token_grads.reshape(seq_count, tokens, 3, head_width), (1, 2, 0, 3)
    ).reshape(tokens, 3, model_width)
    input_grad = grad_resid_one + jnp.einsum(
        "tie,ide->td", grad_qkv, qkv_weights, preferred_element_type=jnp.float32
    )
    grad_attn_rows = jnp.concatenate([qkv_rows, out_rows], axis=0)
    summed = attn_sum(jnp.concatenate([grad_attn_rows, vector_rows], axis=1))
    attn_shard = summed[:block_height]
    vector_shard = summed[block_height, :slot]
    rms_values = jnp.sqrt(square_sums / (valid_total * model_width))
    return (
        layer_values.astype(jnp.bfloat16),
        input_grad,
        attn_shard,
        mlp_shard,
        vector_shard,
        rms_values,
    )


def solution(mesh):
    in_specs = (
        P(("fsdp", "seq"), None),
        P(("fsdp", "seq"), None),
        P("fsdp", None),
        P("fsdp"),
        P(("fsdp", "seq"), None),
        P(("fsdp", "seq"), None),
        P(("fsdp", "seq")),
    )
    out_specs = (
        P(("fsdp", "seq"), None),
        P(("fsdp", "seq"), None),
        P(("fsdp", "seq"), None),
        P(("fsdp", "seq"), None),
        P(("fsdp", "seq")),
        P(),
    )
    return jax.shard_map(
        layer_body, mesh=mesh, in_specs=in_specs, out_specs=out_specs, check_vma=False
    )
```

```python
import functools
import jax
import jax.numpy as jnp
from jax import lax
from jax.sharding import PartitionSpec as P

from jax.experimental import pallas as pl
from jax.experimental.pallas import tpu as pltpu


H = 16

BLOCK = 256
NEG = -1e30


def key_ranges(segment_doc, block):
    firsts = segment_doc[::block]
    lasts = segment_doc[block - 1 :: block]
    starts = jnp.sum(segment_doc[None, :] < firsts[:, None], axis=1).astype(jnp.int32)
    ends = jnp.sum(segment_doc[None, :] <= lasts[:, None], axis=1).astype(jnp.int32)
    return starts // block, (ends + block - 1) // block


def _scores(q, k, doc_q, doc_k, scale):
    s = lax.dot_general(q, k, (((1,), (1,)), ((), ())), preferred_element_type=jnp.float32) * scale
    return jnp.where(doc_q == doc_k, s, NEG)


def _fwd_kernel(lo_ref, hi_ref, q_ref, k_ref, v_ref, dq_ref, dk_ref, out_ref, lse_ref, *, scale, block):
    i = pl.program_id(1)
    lo = lo_ref[i]
    hi = hi_ref[i]
    q = q_ref[...]
    doc_q = dq_ref[...]

    def pass_one(kb, carry):
        m, l = carry
        start = pl.multiple_of(kb * block, block)
        s = _scores(q, k_ref[pl.ds(start, block), :], doc_q, dk_ref[:, pl.ds(start, block)], scale)
        m_new = jnp.maximum(m, jnp.max(s, axis=1, keepdims=True))
        l = l * jnp.exp(m - m_new) + jnp.sum(jnp.exp(s - m_new), axis=1, keepdims=True)
        return m_new, l

    rows = q.shape[0]
    m, l = lax.fori_loop(
        lo, hi, pass_one,
        (jnp.full((rows, 1), NEG, jnp.float32), jnp.zeros((rows, 1), jnp.float32)),
    )

    def pass_two(kb, acc):
        start = pl.multiple_of(kb * block, block)
        s = _scores(q, k_ref[pl.ds(start, block), :], doc_q, dk_ref[:, pl.ds(start, block)], scale)
        p = (jnp.exp(s - m) / l).astype(jnp.bfloat16)
        return acc + jnp.dot(p, v_ref[pl.ds(start, block), :], preferred_element_type=jnp.float32)

    acc = lax.fori_loop(lo, hi, pass_two, jnp.zeros(out_ref.shape, jnp.float32))
    out_ref[...] = acc.astype(out_ref.dtype)
    lse_ref[...] = m + jnp.log(l)


def attn_forward(q, k, v, segment_doc, scale, block=BLOCK):
    heads, seg_len, d = q.shape
    lo, hi = key_ranges(segment_doc, block)
    doc_col = segment_doc.reshape(seg_len, 1)
    doc_row = segment_doc.reshape(1, seg_len)
    grid = (heads, seg_len // block)
    spec_q = pl.BlockSpec((None, block, d), lambda h, i, lo, hi: (h, i, 0))
    spec_kv = pl.BlockSpec((None, seg_len, d), lambda h, i, lo, hi: (h, 0, 0))
    spec_dq = pl.BlockSpec((block, 1), lambda h, i, lo, hi: (i, 0))
    spec_dk = pl.BlockSpec((1, seg_len), lambda h, i, lo, hi: (0, 0))
    spec_lse = pl.BlockSpec((None, block, 1), lambda h, i, lo, hi: (h, i, 0))
    return pl.pallas_call(
        functools.partial(_fwd_kernel, scale=scale, block=block),
        grid_spec=pltpu.PrefetchScalarGridSpec(
            num_scalar_prefetch=2,
            grid=grid,
            in_specs=[spec_q, spec_kv, spec_kv, spec_dq, spec_dk],
            out_specs=[spec_q, spec_lse],
        ),
        out_shape=[
            jax.ShapeDtypeStruct((heads, seg_len, d), jnp.bfloat16),
            jax.ShapeDtypeStruct((heads, seg_len, 1), jnp.float32),
        ],
        compiler_params=pltpu.CompilerParams(dimension_semantics=("arbitrary", "arbitrary")),
    )(lo, hi, q, k, v, doc_col, doc_row)


def _bwd_kernel(lo_ref, hi_ref, q_ref, k_ref, v_ref, da_ref, lse_ref, dq_ref, dk_ref,
                gq_ref, gk_ref, gv_ref, *, scale, block):
    i = pl.program_id(1)
    lo = lo_ref[i]
    hi = hi_ref[i]

    @pl.when(i == 0)
    def _():
        gk_ref[...] = jnp.zeros(gk_ref.shape, gk_ref.dtype)
        gv_ref[...] = jnp.zeros(gv_ref.shape, gv_ref.dtype)

    q = q_ref[...]
    da = da_ref[...]
    lse = lse_ref[...]
    doc_q = dq_ref[...]

    def probs(start):
        s = _scores(q, k_ref[pl.ds(start, block), :], doc_q, dk_ref[:, pl.ds(start, block)], scale)
        p = jnp.exp(s - lse)
        dp = lax.dot_general(da, v_ref[pl.ds(start, block), :], (((1,), (1,)), ((), ())),
                             preferred_element_type=jnp.float32)
        return p, dp

    def pass_one(kb, delta):
        start = pl.multiple_of(kb * block, block)
        p, dp = probs(start)
        return delta + jnp.sum(dp * p, axis=1, keepdims=True)

    rows = q.shape[0]
    delta = lax.fori_loop(lo, hi, pass_one, jnp.zeros((rows, 1), jnp.float32))

    def pass_two(kb, gq):
        start = pl.multiple_of(kb * block, block)
        p, dp = probs(start)
        ds = (p * (dp - delta)).astype(jnp.bfloat16)
        pb = p.astype(jnp.bfloat16)
        k_blk = k_ref[pl.ds(start, block), :]
        gq = gq + jnp.dot(ds, k_blk, preferred_element_type=jnp.float32)
        gk_ref[pl.ds(start, block), :] += lax.dot_general(
            ds, q, (((0,), (0,)), ((), ())), preferred_element_type=jnp.float32)
        gv_ref[pl.ds(start, block), :] += lax.dot_general(
            pb, da, (((0,), (0,)), ((), ())), preferred_element_type=jnp.float32)
        return gq

    gq = lax.fori_loop(lo, hi, pass_two, jnp.zeros(gq_ref.shape, jnp.float32))
    gq_ref[...] = gq * scale

    @pl.when(i == pl.num_programs(1) - 1)
    def _():
        gk_ref[...] = gk_ref[...] * scale


def attn_backward(q, k, v, da, lse, segment_doc, scale, block=BLOCK):
    heads, seg_len, d = q.shape
    lo, hi = key_ranges(segment_doc, block)
    doc_col = segment_doc.reshape(seg_len, 1)
    doc_row = segment_doc.reshape(1, seg_len)
    grid = (heads, seg_len // block)
    spec_q = pl.BlockSpec((None, block, d), lambda h, i, lo, hi: (h, i, 0))
    spec_kv = pl.BlockSpec((None, seg_len, d), lambda h, i, lo, hi: (h, 0, 0))
    spec_dq = pl.BlockSpec((block, 1), lambda h, i, lo, hi: (i, 0))
    spec_dk = pl.BlockSpec((1, seg_len), lambda h, i, lo, hi: (0, 0))
    spec_lse = pl.BlockSpec((None, block, 1), lambda h, i, lo, hi: (h, i, 0))
    return pl.pallas_call(
        functools.partial(_bwd_kernel, scale=scale, block=block),
        grid_spec=pltpu.PrefetchScalarGridSpec(
            num_scalar_prefetch=2,
            grid=grid,
            in_specs=[spec_q, spec_kv, spec_kv, spec_q, spec_lse, spec_dq, spec_dk],
            out_specs=[spec_q, spec_kv, spec_kv],
        ),
        out_shape=[jax.ShapeDtypeStruct((heads, seg_len, d), jnp.float32)] * 3,
        compiler_params=pltpu.CompilerParams(dimension_semantics=("arbitrary", "arbitrary")),
    )(lo, hi, q, k, v, da, lse, doc_col, doc_row)


EPSILON = 1e-05
ROOT_HALF = 0.7071067811865476
INV_ROOT_TWO_PI = 0.3989422804014327


def norm_forward(values, norm_gain, norm_shift):
    row_mean = jnp.mean(values, axis=1, keepdims=True)
    centered = values - row_mean
    inverse = lax.rsqrt(jnp.mean(centered * centered, axis=1, keepdims=True) + EPSILON)
    scaled = centered * inverse
    return (scaled * norm_gain + norm_shift, scaled, inverse)


def norm_backward(gradient, scaled, inverse, norm_gain):
    grad_scaled = gradient * norm_gain
    grad_mean = jnp.mean(grad_scaled, axis=1, keepdims=True)
    grad_along = jnp.mean(grad_scaled * scaled, axis=1, keepdims=True)
    grad_rows = inverse * (grad_scaled - grad_mean - scaled * grad_along)
    return (grad_rows, jnp.sum(gradient * scaled, axis=0), jnp.sum(gradient, axis=0))


def gelu_slope(entries):
    return 0.5 * (1.0 + lax.erf(entries * ROOT_HALF)) + entries * INV_ROOT_TWO_PI * jnp.exp(
        -0.5 * entries * entries
    )


def ring_gather(rows, count, index):
    half = count // 2
    order = [2 * a for a in range(half)] + [2 * a + 1 for a in reversed(range(half))]
    place = [order.index(s) for s in range(count)]
    forward_pairs = [(order[i], order[(i + 1) % count]) for i in range(count)]
    backward_pairs = [(b, a) for a, b in forward_pairs]
    by_offset = [None] * count
    by_offset[0] = rows
    moving = rows
    for step in range(1, count - count // 2):
        moving = lax.ppermute(moving, "seq", forward_pairs)
        by_offset[count - step] = moving
    moving = rows
    for step in range(1, count // 2 + 1):
        moving = lax.ppermute(moving, "seq", backward_pairs)
        by_offset[step] = moving
    position = jnp.asarray(place, jnp.int32)[index]
    pick = (jnp.asarray(place, jnp.int32) - position) % count
    stacked = jnp.stack(by_offset)
    return jnp.take(stacked, pick, axis=0).reshape((count * rows.shape[0],) + rows.shape[1:])


def attn_sum(values):
    return lax.psum_scatter(values, "fsdp", scatter_dimension=0, tiled=True)[0]


def contract_rows(left, right):
    return lax.dot_general(
        left, right, (((0,), (0,)), ((), ())), preferred_element_type=jnp.float32
    )


def contract_cols(left, right):
    return lax.dot_general(
        left, right, (((1,), (1,)), ((), ())), preferred_element_type=jnp.float32
    )


def layer_body(layer_in, cotangent, doc_ids, valid_len, attn_weights, mlp_weights, param_vector):
    seq_count = lax.axis_size("seq")
    seq_index = lax.axis_index("seq")
    tokens, model_width = layer_in.shape
    head_size = model_width // H
    local_heads = H // seq_count
    score_scale = head_size ** (-0.5)
    attn_rows, vector_slot = attn_weights.shape[0], param_vector.shape[0]
    packed = jnp.concatenate(
        [attn_weights, jnp.pad(param_vector, (0, model_width - vector_slot))[None]], axis=0
    )
    packed_full = lax.all_gather(packed, ("fsdp", "seq"), axis=0, tiled=False)
    attn_full = packed_full[:, :attn_rows].reshape(-1, model_width)
    vector_full = packed_full[:, attn_rows, :vector_slot].reshape(-1)
    mlp_full = lax.all_gather(mlp_weights, ("fsdp", "seq"), axis=0, tiled=True)
    hidden = mlp_full.shape[0] // 2
    vector_wide = vector_full.astype(jnp.float32)
    pieces = [
        vector_wide[slot_index * model_width : (slot_index + 1) * model_width]
        for slot_index in range(8)
    ]
    bias_q, bias_v, bias_o, gain_one, shift_one, bias_two, gain_two, shift_two = pieces
    bias_up = vector_wide[8 * model_width :]
    qkv_weights = attn_full[: 3 * model_width].reshape(3, model_width, model_width)
    out_weights = attn_full[3 * model_width :]
    in_weights = mlp_full[:hidden]
    down_weights = mlp_full[hidden:]
    segment_in = ring_gather(layer_in, seq_count, seq_index)
    segment_doc = doc_ids[0]
    seg_len = segment_doc.shape[0]
    positions = seq_index * tokens + lax.iota(jnp.int32, tokens)
    valid_rows = (positions < valid_len[0]).astype(jnp.float32)[:, None]
    zero_row = jnp.zeros((1, model_width), jnp.float32)
    qkv_bias = jnp.concatenate([bias_q[None], zero_row, bias_v[None]], axis=0)
    head_width = local_heads * head_size
    own_columns = seq_index * head_width
    own_weights = lax.dynamic_slice_in_dim(qkv_weights, own_columns, head_width, axis=2)
    own_bias = lax.dynamic_slice_in_dim(qkv_bias, own_columns, head_width, axis=1)
    projected = (
        jnp.einsum("td,ide->tie", segment_in, own_weights, preferred_element_type=jnp.float32)
        + own_bias[None]
    )
    head_all = jnp.transpose(
        projected.astype(jnp.bfloat16).reshape(seg_len, 3, local_heads, head_size), (1, 2, 0, 3)
    )
    head_q, head_k, head_v = head_all[0], head_all[1], head_all[2]
    head_mixed, log_total = attn_forward(head_q, head_k, head_v, segment_doc, score_scale)
    mixed_rows = jnp.transpose(head_mixed, (1, 0, 2)).reshape(seq_count, tokens, head_width)
    token_mixed = lax.all_to_all(mixed_rows, "seq", split_axis=0, concat_axis=0, tiled=True)
    attn_mixed = jnp.transpose(token_mixed, (1, 0, 2)).reshape(tokens, model_width)
    branch = jnp.dot(attn_mixed, out_weights, preferred_element_type=jnp.float32) + bias_o
    resid_one = layer_in.astype(jnp.float32) + branch
    normed, scaled_one, inverse_one = norm_forward(resid_one, gain_one, shift_one)
    normed_low = normed.astype(jnp.bfloat16)
    normed_seg = lax.all_gather(normed_low, "seq", axis=0, tiled=True)
    upper = contract_cols(normed_low, in_weights) + bias_up
    active_low = jax.nn.gelu(upper, approximate=False).astype(jnp.bfloat16)
    mlp_branch = jnp.dot(active_low, down_weights, preferred_element_type=jnp.float32) + bias_two
    resid_two = normed + mlp_branch
    layer_values, scaled_two, inverse_two = norm_forward(resid_two, gain_two, shift_two)
    squares = jnp.stack(
        [
            jnp.sum(valid_rows * resid_one * resid_one),
            jnp.sum(valid_rows * branch * branch),
            jnp.sum(valid_rows * resid_two * resid_two),
            jnp.sum(valid_rows * mlp_branch * mlp_branch),
        ]
    )
    square_sums, valid_total = lax.psum((squares, jnp.sum(valid_rows)), ("fsdp", "seq"))
    square_sums, valid_total, cotangent = lax.optimization_barrier(
        (square_sums, valid_total, cotangent)
    )
    grad_out = cotangent.astype(jnp.float32)
    grad_resid_two, grad_gain_two, grad_shift_two = norm_backward(
        grad_out, scaled_two, inverse_two, gain_two
    )
    grad_mlp_low = grad_resid_two.astype(jnp.bfloat16)
    grad_bias_two = jnp.sum(grad_mlp_low.astype(jnp.float32), axis=0)
    grad_active = contract_cols(grad_mlp_low, down_weights)
    grad_upper_low = (grad_active * gelu_slope(upper)).astype(jnp.bfloat16)
    grad_bias_up = jnp.sum(grad_upper_low.astype(jnp.float32), axis=0)
    grad_normed = grad_resid_two + jnp.dot(
        grad_upper_low, in_weights, preferred_element_type=jnp.float32
    )
    fsdp_count = lax.axis_size("fsdp")
    mlp_height = 2 * hidden // (fsdp_count * seq_count)
    mlp_groups = hidden // (seq_count * mlp_height)

    def own_rows(rows):
        blocks = rows.reshape((mlp_groups, seq_count, mlp_height) + rows.shape[1:])
        picked = lax.dynamic_index_in_dim(blocks, seq_index, axis=1, keepdims=False)
        return picked.reshape((mlp_groups * mlp_height,) + rows.shape[1:])

    grad_mlp_seg = lax.all_gather(grad_mlp_low, "seq", axis=0, tiled=True)
    upper_own = contract_cols(normed_seg, own_rows(in_weights)) + own_rows(bias_up)
    active_own = jax.nn.gelu(upper_own, approximate=False).astype(jnp.bfloat16)
    grad_active_own = contract_cols(grad_mlp_seg, own_rows(down_weights))
    grad_upper_own = (grad_active_own * gelu_slope(upper_own)).astype(jnp.bfloat16)
    grad_in_own = contract_rows(grad_upper_own, normed_seg)
    grad_down_own = contract_rows(active_own, grad_mlp_seg)
    mlp_stack = jnp.concatenate(
        [
            grad_in_own.reshape(mlp_groups, mlp_height, model_width),
            grad_down_own.reshape(mlp_groups, mlp_height, model_width),
        ],
        axis=0,
    )
    mlp_shard = lax.psum_scatter(mlp_stack, "fsdp", scatter_dimension=0, tiled=True)[0]
    grad_resid_one, grad_gain_one, grad_shift_one = norm_backward(
        grad_normed, scaled_one, inverse_one, gain_one
    )
    grad_branch_low = grad_resid_one.astype(jnp.bfloat16)
    grad_bias_o = jnp.sum(grad_branch_low.astype(jnp.float32), axis=0)
    block_height = 4 * model_width // (fsdp_count * seq_count)
    out_blocks = model_width // (seq_count * block_height)
    out_rows = lax.psum_scatter(
        contract_rows(attn_mixed, grad_branch_low).reshape(
            out_blocks, seq_count, block_height, model_width
        ),
        "seq",
        scatter_dimension=1,
        tiled=True,
    )[:, 0]
    grad_mixed_low = contract_cols(grad_branch_low, out_weights).astype(jnp.bfloat16)
    grad_split = jnp.transpose(
        grad_mixed_low.reshape(tokens, seq_count, head_width), (1, 0, 2)
    )
    grad_heads = lax.all_to_all(grad_split, "seq", split_axis=0, concat_axis=0, tiled=True)
    head_grad = jnp.transpose(grad_heads.reshape(seg_len, local_heads, head_size), (1, 0, 2))

    grad_queries, grad_keys, grad_values = attn_backward(
        head_q, head_k, head_v, head_grad, log_total, segment_doc, score_scale
    )
    head_grads = jnp.transpose(
        jnp.stack([grad_queries, grad_keys, grad_values], axis=0), (2, 0, 1, 3)
    ).astype(jnp.bfloat16)
    head_weight_grads = jnp.einsum(
        "td,tihe->dihe", segment_in, head_grads, preferred_element_type=jnp.float32
    )
    qkv_blocks = 3 * out_blocks
    head_bias_sums = jnp.sum(head_grads.astype(jnp.float32), axis=0).reshape(3, head_width)
    bias_qv = lax.dynamic_update_slice(
        jnp.zeros((2, model_width), jnp.float32),
        head_bias_sums[::2],
        (0, seq_index * head_width),
    )
    grad_vector = jnp.concatenate(
        [
            bias_qv.reshape(-1),
            grad_bias_o,
            grad_gain_one,
            grad_shift_one,
            grad_bias_two,
            grad_gain_two,
            grad_shift_two,
            grad_bias_up,
        ]
    )
    slot = grad_vector.shape[0] // (fsdp_count * seq_count)
    vector_part = jnp.transpose(grad_vector.reshape(fsdp_count, seq_count, slot), (1, 0, 2))
    by_row = jnp.transpose(head_weight_grads.reshape(model_width, 3, head_width), (1, 0, 2))
    row_part = jnp.transpose(
        by_row.reshape(qkv_blocks, seq_count, block_height, head_width), (1, 0, 2, 3)
    )
    row_size = qkv_blocks * block_height * head_width
    exchanged = lax.all_to_all(
        jnp.concatenate(
            [row_part.reshape(seq_count, -1), vector_part.reshape(seq_count, -1)], axis=1
        ),
        "seq", split_axis=0, concat_axis=0, tiled=True,
    )
    row_blocks = exchanged[:, :row_size].reshape(seq_count, qkv_blocks, block_height, head_width)
    qkv_rows = jnp.transpose(row_blocks, (1, 2, 0, 3)).reshape(qkv_blocks, block_height, model_width)
    vector_rows = jnp.sum(exchanged[:, row_size:].reshape(seq_count, fsdp_count, slot), axis=0)
    vector_rows = jnp.pad(vector_rows, ((0, 0), (0, model_width - slot)))[:, None]
    token_grads = lax.all_to_all(
        head_grads.reshape(seq_count, tokens, 3 * head_width),
        "seq", split_axis=0, concat_axis=0, tiled=True,
    )
    grad_qkv = jnp.transpose(
        token_grads.reshape(seq_count, tokens, 3, head_width), (1, 2, 0, 3)
    ).reshape(tokens, 3, model_width)
    input_grad = grad_resid_one + jnp.einsum(
        "tie,ide->td", grad_qkv, qkv_weights, preferred_element_type=jnp.float32
    )
    grad_attn_rows = jnp.concatenate([qkv_rows, out_rows], axis=0)
    summed = attn_sum(jnp.concatenate([grad_attn_rows, vector_rows], axis=1))
    attn_shard = summed[:block_height]
    vector_shard = summed[block_height, :slot]
    rms_values = jnp.sqrt(square_sums / (valid_total * model_width))
    return (
        layer_values.astype(jnp.bfloat16),
        input_grad,
        attn_shard,
        mlp_shard,
        vector_shard,
        rms_values,
    )


def solution(mesh):
    in_specs = (
        P(("fsdp", "seq"), None),
        P(("fsdp", "seq"), None),
        P("fsdp", None),
        P("fsdp"),
        P(("fsdp", "seq"), None),
        P(("fsdp", "seq"), None),
        P(("fsdp", "seq")),
    )
    out_specs = (
        P(("fsdp", "seq"), None),
        P(("fsdp", "seq"), None),
        P(("fsdp", "seq"), None),
        P(("fsdp", "seq"), None),
        P(("fsdp", "seq")),
        P(),
    )
    return jax.shard_map(
        layer_body, mesh=mesh, in_specs=in_specs, out_specs=out_specs, check_vma=False
    )
```

```python
import functools
import jax
import jax.numpy as jnp
from jax import lax
from jax.sharding import PartitionSpec as P

from jax.experimental import pallas as pl
from jax.experimental.pallas import tpu as pltpu


H = 16

BLOCK = 256
NEG = -1e30


def key_ranges(segment_doc, block):
    firsts = segment_doc[::block]
    lasts = segment_doc[block - 1 :: block]
    starts = jnp.sum(segment_doc[None, :] < firsts[:, None], axis=1).astype(jnp.int32)
    ends = jnp.sum(segment_doc[None, :] <= lasts[:, None], axis=1).astype(jnp.int32)
    return starts // block, (ends + block - 1) // block


def _scores(q, k, doc_q, doc_k, scale):
    s = lax.dot_general(q, k, (((1,), (1,)), ((), ())), preferred_element_type=jnp.float32) * scale
    return jnp.where(doc_q == doc_k, s, NEG)


def _fwd_kernel(lo_ref, hi_ref, q_ref, k_ref, v_ref, dq_ref, dk_ref, out_ref, lse_ref, *, scale, block):
    i = pl.program_id(1)
    lo = lo_ref[i]
    hi = hi_ref[i]
    q = q_ref[...]
    doc_q = dq_ref[...]

    def pass_one(kb, carry):
        m, l = carry
        start = pl.multiple_of(kb * block, block)
        s = _scores(q, k_ref[pl.ds(start, block), :], doc_q, dk_ref[:, pl.ds(start, block)], scale)
        m_new = jnp.maximum(m, jnp.max(s, axis=1, keepdims=True))
        l = l * jnp.exp(m - m_new) + jnp.sum(jnp.exp(s - m_new), axis=1, keepdims=True)
        return m_new, l

    rows = q.shape[0]
    m, l = lax.fori_loop(
        lo, hi, pass_one,
        (jnp.full((rows, 1), NEG, jnp.float32), jnp.zeros((rows, 1), jnp.float32)),
    )

    def pass_two(kb, acc):
        start = pl.multiple_of(kb * block, block)
        s = _scores(q, k_ref[pl.ds(start, block), :], doc_q, dk_ref[:, pl.ds(start, block)], scale)
        p = (jnp.exp(s - m) / l).astype(jnp.bfloat16)
        return acc + jnp.dot(p, v_ref[pl.ds(start, block), :], preferred_element_type=jnp.float32)

    acc = lax.fori_loop(lo, hi, pass_two, jnp.zeros(out_ref.shape, jnp.float32))
    out_ref[...] = acc.astype(out_ref.dtype)
    lse_ref[...] = m + jnp.log(l)


def attn_forward(q, k, v, segment_doc, scale, block=BLOCK):
    heads, seg_len, d = q.shape
    lo, hi = key_ranges(segment_doc, block)
    doc_col = segment_doc.reshape(seg_len, 1)
    doc_row = segment_doc.reshape(1, seg_len)
    grid = (heads, seg_len // block)
    spec_q = pl.BlockSpec((None, block, d), lambda h, i, lo, hi: (h, i, 0))
    spec_kv = pl.BlockSpec((None, seg_len, d), lambda h, i, lo, hi: (h, 0, 0))
    spec_dq = pl.BlockSpec((block, 1), lambda h, i, lo, hi: (i, 0))
    spec_dk = pl.BlockSpec((1, seg_len), lambda h, i, lo, hi: (0, 0))
    spec_lse = pl.BlockSpec((None, block, 1), lambda h, i, lo, hi: (h, i, 0))
    return pl.pallas_call(
        functools.partial(_fwd_kernel, scale=scale, block=block),
        grid_spec=pltpu.PrefetchScalarGridSpec(
            num_scalar_prefetch=2,
            grid=grid,
            in_specs=[spec_q, spec_kv, spec_kv, spec_dq, spec_dk],
            out_specs=[spec_q, spec_lse],
        ),
        out_shape=[
            jax.ShapeDtypeStruct((heads, seg_len, d), jnp.bfloat16),
            jax.ShapeDtypeStruct((heads, seg_len, 1), jnp.float32),
        ],
        compiler_params=pltpu.CompilerParams(dimension_semantics=("arbitrary", "arbitrary")),
    )(lo, hi, q, k, v, doc_col, doc_row)


def _bwd_kernel(lo_ref, hi_ref, q_ref, k_ref, v_ref, da_ref, lse_ref, dq_ref, dk_ref,
                gq_ref, gk_ref, gv_ref, *, scale, block):
    i = pl.program_id(1)
    lo = lo_ref[i]
    hi = hi_ref[i]

    @pl.when(i == 0)
    def _():
        gk_ref[...] = jnp.zeros(gk_ref.shape, gk_ref.dtype)
        gv_ref[...] = jnp.zeros(gv_ref.shape, gv_ref.dtype)

    q = q_ref[...]
    da = da_ref[...]
    lse = lse_ref[...]
    doc_q = dq_ref[...]

    def probs(start):
        s = _scores(q, k_ref[pl.ds(start, block), :], doc_q, dk_ref[:, pl.ds(start, block)], scale)
        p = jnp.exp(s - lse)
        dp = lax.dot_general(da, v_ref[pl.ds(start, block), :], (((1,), (1,)), ((), ())),
                             preferred_element_type=jnp.float32)
        return p, dp

    def pass_one(kb, delta):
        start = pl.multiple_of(kb * block, block)
        p, dp = probs(start)
        return delta + jnp.sum(dp * p, axis=1, keepdims=True)

    rows = q.shape[0]
    delta = lax.fori_loop(lo, hi, pass_one, jnp.zeros((rows, 1), jnp.float32))

    def pass_two(kb, gq):
        start = pl.multiple_of(kb * block, block)
        p, dp = probs(start)
        ds = (p * (dp - delta)).astype(jnp.bfloat16)
        pb = p.astype(jnp.bfloat16)
        k_blk = k_ref[pl.ds(start, block), :]
        gq = gq + jnp.dot(ds, k_blk, preferred_element_type=jnp.float32)
        gk_ref[pl.ds(start, block), :] += lax.dot_general(
            ds, q, (((0,), (0,)), ((), ())), preferred_element_type=jnp.float32)
        gv_ref[pl.ds(start, block), :] += lax.dot_general(
            pb, da, (((0,), (0,)), ((), ())), preferred_element_type=jnp.float32)
        return gq

    gq = lax.fori_loop(lo, hi, pass_two, jnp.zeros(gq_ref.shape, jnp.float32))
    gq_ref[...] = gq * scale

    @pl.when(i == pl.num_programs(1) - 1)
    def _():
        gk_ref[...] = gk_ref[...] * scale


def attn_backward(q, k, v, da, lse, segment_doc, scale, block=BLOCK):
    heads, seg_len, d = q.shape
    lo, hi = key_ranges(segment_doc, block)
    doc_col = segment_doc.reshape(seg_len, 1)
    doc_row = segment_doc.reshape(1, seg_len)
    grid = (heads, seg_len // block)
    spec_q = pl.BlockSpec((None, block, d), lambda h, i, lo, hi: (h, i, 0))
    spec_kv = pl.BlockSpec((None, seg_len, d), lambda h, i, lo, hi: (h, 0, 0))
    spec_dq = pl.BlockSpec((block, 1), lambda h, i, lo, hi: (i, 0))
    spec_dk = pl.BlockSpec((1, seg_len), lambda h, i, lo, hi: (0, 0))
    spec_lse = pl.BlockSpec((None, block, 1), lambda h, i, lo, hi: (h, i, 0))
    return pl.pallas_call(
        functools.partial(_bwd_kernel, scale=scale, block=block),
        grid_spec=pltpu.PrefetchScalarGridSpec(
            num_scalar_prefetch=2,
            grid=grid,
            in_specs=[spec_q, spec_kv, spec_kv, spec_q, spec_lse, spec_dq, spec_dk],
            out_specs=[spec_q, spec_kv, spec_kv],
        ),
        out_shape=[jax.ShapeDtypeStruct((heads, seg_len, d), jnp.float32)] * 3,
        compiler_params=pltpu.CompilerParams(dimension_semantics=("arbitrary", "arbitrary")),
    )(lo, hi, q, k, v, da, lse, doc_col, doc_row)


EPSILON = 1e-05
ROOT_HALF = 0.7071067811865476
INV_ROOT_TWO_PI = 0.3989422804014327


def norm_forward(values, norm_gain, norm_shift):
    row_mean = jnp.mean(values, axis=1, keepdims=True)
    centered = values - row_mean
    inverse = lax.rsqrt(jnp.mean(centered * centered, axis=1, keepdims=True) + EPSILON)
    scaled = centered * inverse
    return (scaled * norm_gain + norm_shift, scaled, inverse)


def norm_backward(gradient, scaled, inverse, norm_gain):
    grad_scaled = gradient * norm_gain
    grad_mean = jnp.mean(grad_scaled, axis=1, keepdims=True)
    grad_along = jnp.mean(grad_scaled * scaled, axis=1, keepdims=True)
    grad_rows = inverse * (grad_scaled - grad_mean - scaled * grad_along)
    return (grad_rows, jnp.sum(gradient * scaled, axis=0), jnp.sum(gradient, axis=0))


def gelu_slope(entries):
    return 0.5 * (1.0 + lax.erf(entries * ROOT_HALF)) + entries * INV_ROOT_TWO_PI * jnp.exp(
        -0.5 * entries * entries
    )


def ring_gather(rows, count, index):
    half = count // 2
    order = [2 * a for a in range(half)] + [2 * a + 1 for a in reversed(range(half))]
    place = [order.index(s) for s in range(count)]
    forward_pairs = [(order[i], order[(i + 1) % count]) for i in range(count)]
    backward_pairs = [(b, a) for a, b in forward_pairs]
    by_offset = [None] * count
    by_offset[0] = rows
    moving = rows
    for step in range(1, count - count // 2):
        moving = lax.ppermute(moving, "seq", forward_pairs)
        by_offset[count - step] = moving
    moving = rows
    for step in range(1, count // 2 + 1):
        moving = lax.ppermute(moving, "seq", backward_pairs)
        by_offset[step] = moving
    position = jnp.asarray(place, jnp.int32)[index]
    pick = (jnp.asarray(place, jnp.int32) - position) % count
    stacked = jnp.stack(by_offset)
    return jnp.take(stacked, pick, axis=0).reshape((count * rows.shape[0],) + rows.shape[1:])


def attn_sum(values):
    return lax.psum_scatter(values, "fsdp", scatter_dimension=0, tiled=True)[0]


def contract_rows(left, right):
    return lax.dot_general(
        left, right, (((0,), (0,)), ((), ())), preferred_element_type=jnp.float32
    )


def contract_cols(left, right):
    return lax.dot_general(
        left, right, (((1,), (1,)), ((), ())), preferred_element_type=jnp.float32
    )


def layer_body(layer_in, cotangent, doc_ids, valid_len, attn_weights, mlp_weights, param_vector):
    seq_count = lax.axis_size("seq")
    seq_index = lax.axis_index("seq")
    tokens, model_width = layer_in.shape
    head_size = model_width // H
    local_heads = H // seq_count
    score_scale = head_size ** (-0.5)
    attn_rows, vector_slot = attn_weights.shape[0], param_vector.shape[0]
    packed = jnp.concatenate(
        [attn_weights, jnp.pad(param_vector, (0, model_width - vector_slot))[None]], axis=0
    )
    packed_full = lax.all_gather(packed, ("fsdp", "seq"), axis=0, tiled=False)
    attn_full = packed_full[:, :attn_rows].reshape(-1, model_width)
    vector_full = packed_full[:, attn_rows, :vector_slot].reshape(-1)
    mlp_full = lax.all_gather(mlp_weights, ("fsdp", "seq"), axis=0, tiled=True)
    hidden = mlp_full.shape[0] // 2
    vector_wide = vector_full.astype(jnp.float32)
    pieces = [
        vector_wide[slot_index * model_width : (slot_index + 1) * model_width]
        for slot_index in range(8)
    ]
    bias_q, bias_v, bias_o, gain_one, shift_one, bias_two, gain_two, shift_two = pieces
    bias_up = vector_wide[8 * model_width :]
    qkv_weights = attn_full[: 3 * model_width].reshape(3, model_width, model_width)
    out_weights = attn_full[3 * model_width :]
    in_weights = mlp_full[:hidden]
    down_weights = mlp_full[hidden:]
    segment_in = ring_gather(layer_in, seq_count, seq_index)
    segment_doc = doc_ids[0]
    seg_len = segment_doc.shape[0]
    positions = seq_index * tokens + lax.iota(jnp.int32, tokens)
    valid_rows = (positions < valid_len[0]).astype(jnp.float32)[:, None]
    zero_row = jnp.zeros((1, model_width), jnp.float32)
    qkv_bias = jnp.concatenate([bias_q[None], zero_row, bias_v[None]], axis=0)
    head_width = local_heads * head_size
    own_columns = seq_index * head_width
    own_weights = lax.dynamic_slice_in_dim(qkv_weights, own_columns, head_width, axis=2)
    own_bias = lax.dynamic_slice_in_dim(qkv_bias, own_columns, head_width, axis=1)
    projected = (
        jnp.einsum("td,ide->tie", segment_in, own_weights, preferred_element_type=jnp.float32)
        + own_bias[None]
    )
    head_all = jnp.transpose(
        projected.astype(jnp.bfloat16).reshape(seg_len, 3, local_heads, head_size), (1, 2, 0, 3)
    )
    head_q, head_k, head_v = head_all[0], head_all[1], head_all[2]
    head_mixed, log_total = attn_forward(head_q, head_k, head_v, segment_doc, score_scale)
    mixed_rows = jnp.transpose(head_mixed, (1, 0, 2)).reshape(seq_count, tokens, head_width)
    token_mixed = lax.all_to_all(mixed_rows, "seq", split_axis=0, concat_axis=0, tiled=True)
    attn_mixed = jnp.transpose(token_mixed, (1, 0, 2)).reshape(tokens, model_width)
    branch = jnp.dot(attn_mixed, out_weights, preferred_element_type=jnp.float32) + bias_o
    resid_one = layer_in.astype(jnp.float32) + branch
    normed, scaled_one, inverse_one = norm_forward(resid_one, gain_one, shift_one)
    normed_low = normed.astype(jnp.bfloat16)
    normed_seg = lax.all_gather(normed_low, "seq", axis=0, tiled=True)
    upper = contract_cols(normed_low, in_weights) + bias_up
    active_low = jax.nn.gelu(upper, approximate=False).astype(jnp.bfloat16)
    mlp_branch = jnp.dot(active_low, down_weights, preferred_element_type=jnp.float32) + bias_two
    resid_two = normed + mlp_branch
    layer_values, scaled_two, inverse_two = norm_forward(resid_two, gain_two, shift_two)
    squares = jnp.stack(
        [
            jnp.sum(valid_rows * resid_one * resid_one),
            jnp.sum(valid_rows * branch * branch),
            jnp.sum(valid_rows * resid_two * resid_two),
            jnp.sum(valid_rows * mlp_branch * mlp_branch),
        ]
    )
    square_sums, valid_total = lax.psum((squares, jnp.sum(valid_rows)), ("fsdp", "seq"))
    square_sums, valid_total, cotangent = lax.optimization_barrier(
        (square_sums, valid_total, cotangent)
    )
    grad_out = cotangent.astype(jnp.float32)
    grad_resid_two, grad_gain_two, grad_shift_two = norm_backward(
        grad_out, scaled_two, inverse_two, gain_two
    )
    grad_mlp_low = grad_resid_two.astype(jnp.bfloat16)
    grad_bias_two = jnp.sum(grad_mlp_low.astype(jnp.float32), axis=0)
    grad_active = contract_cols(grad_mlp_low, down_weights)
    grad_upper_low = (grad_active * gelu_slope(upper)).astype(jnp.bfloat16)
    grad_bias_up = jnp.sum(grad_upper_low.astype(jnp.float32), axis=0)
    grad_normed = grad_resid_two + jnp.dot(
        grad_upper_low, in_weights, preferred_element_type=jnp.float32
    )
    fsdp_count = lax.axis_size("fsdp")
    mlp_height = 2 * hidden // (fsdp_count * seq_count)
    mlp_groups = hidden // (seq_count * mlp_height)

    def own_rows(rows):
        blocks = rows.reshape((mlp_groups, seq_count, mlp_height) + rows.shape[1:])
        picked = lax.dynamic_index_in_dim(blocks, seq_index, axis=1, keepdims=False)
        return picked.reshape((mlp_groups * mlp_height,) + rows.shape[1:])

    grad_mlp_seg = lax.all_gather(grad_mlp_low, "seq", axis=0, tiled=True)
    upper_own = contract_cols(normed_seg, own_rows(in_weights)) + own_rows(bias_up)
    active_own = jax.nn.gelu(upper_own, approximate=False).astype(jnp.bfloat16)
    grad_active_own = contract_cols(grad_mlp_seg, own_rows(down_weights))
    grad_upper_own = (grad_active_own * gelu_slope(upper_own)).astype(jnp.bfloat16)
    grad_in_own = contract_rows(grad_upper_own, normed_seg)
    grad_down_own = contract_rows(active_own, grad_mlp_seg)
    mlp_stack = jnp.concatenate(
        [
            grad_in_own.reshape(mlp_groups, mlp_height, model_width),
            grad_down_own.reshape(mlp_groups, mlp_height, model_width),
        ],
        axis=0,
    )
    mlp_shard = lax.psum_scatter(mlp_stack, "fsdp", scatter_dimension=0, tiled=True)[0]
    grad_resid_one, grad_gain_one, grad_shift_one = norm_backward(
        grad_normed, scaled_one, inverse_one, gain_one
    )
    grad_branch_low = grad_resid_one.astype(jnp.bfloat16)
    grad_bias_o = jnp.sum(grad_branch_low.astype(jnp.float32), axis=0)
    block_height = 4 * model_width // (fsdp_count * seq_count)
    out_blocks = model_width // (seq_count * block_height)
    if out_blocks == 1 and block_height == head_width:
        grad_branch_seg = ring_gather(grad_branch_low, seq_count, seq_index)
        head_rows = jnp.transpose(head_mixed, (1, 0, 2)).reshape(seg_len, head_width)
        out_rows = contract_rows(head_rows, grad_branch_seg)[None]
    else:
        out_rows = lax.psum_scatter(
            contract_rows(attn_mixed, grad_branch_low).reshape(
                out_blocks, seq_count, block_height, model_width
            ),
            "seq",
            scatter_dimension=1,
            tiled=True,
        )[:, 0]
    grad_mixed_low = contract_cols(grad_branch_low, out_weights).astype(jnp.bfloat16)
    grad_split = jnp.transpose(
        grad_mixed_low.reshape(tokens, seq_count, head_width), (1, 0, 2)
    )
    grad_heads = lax.all_to_all(grad_split, "seq", split_axis=0, concat_axis=0, tiled=True)
    head_grad = jnp.transpose(grad_heads.reshape(seg_len, local_heads, head_size), (1, 0, 2))

    grad_queries, grad_keys, grad_values = attn_backward(
        head_q, head_k, head_v, head_grad, log_total, segment_doc, score_scale
    )
    head_grads = jnp.transpose(
        jnp.stack([grad_queries, grad_keys, grad_values], axis=0), (2, 0, 1, 3)
    ).astype(jnp.bfloat16)
    head_weight_grads = jnp.einsum(
        "td,tihe->dihe", segment_in, head_grads, preferred_element_type=jnp.float32
    )
    qkv_blocks = 3 * out_blocks
    head_bias_sums = jnp.sum(head_grads.astype(jnp.float32), axis=0).reshape(3, head_width)
    bias_qv = lax.dynamic_update_slice(
        jnp.zeros((2, model_width), jnp.float32),
        head_bias_sums[::2],
        (0, seq_index * head_width),
    )
    grad_vector = jnp.concatenate(
        [
            bias_qv.reshape(-1),
            grad_bias_o,
            grad_gain_one,
            grad_shift_one,
            grad_bias_two,
            grad_gain_two,
            grad_shift_two,
            grad_bias_up,
        ]
    )
    slot = grad_vector.shape[0] // (fsdp_count * seq_count)
    vector_part = jnp.transpose(grad_vector.reshape(fsdp_count, seq_count, slot), (1, 0, 2))
    by_row = jnp.transpose(head_weight_grads.reshape(model_width, 3, head_width), (1, 0, 2))
    row_part = jnp.transpose(
        by_row.reshape(qkv_blocks, seq_count, block_height, head_width), (1, 0, 2, 3)
    )
    row_size = qkv_blocks * block_height * head_width
    exchanged = lax.all_to_all(
        jnp.concatenate(
            [row_part.reshape(seq_count, -1), vector_part.reshape(seq_count, -1)], axis=1
        ),
        "seq", split_axis=0, concat_axis=0, tiled=True,
    )
    row_blocks = exchanged[:, :row_size].reshape(seq_count, qkv_blocks, block_height, head_width)
    qkv_rows = jnp.transpose(row_blocks, (1, 2, 0, 3)).reshape(qkv_blocks, block_height, model_width)
    vector_rows = jnp.sum(exchanged[:, row_size:].reshape(seq_count, fsdp_count, slot), axis=0)
    vector_rows = jnp.pad(vector_rows, ((0, 0), (0, model_width - slot)))[:, None]
    token_grads = lax.all_to_all(
        head_grads.reshape(seq_count, tokens, 3 * head_width),
        "seq", split_axis=0, concat_axis=0, tiled=True,
    )
    grad_qkv = jnp.transpose(
        token_grads.reshape(seq_count, tokens, 3, head_width), (1, 2, 0, 3)
    ).reshape(tokens, 3, model_width)
    input_grad = grad_resid_one + jnp.einsum(
        "tie,ide->td", grad_qkv, qkv_weights, preferred_element_type=jnp.float32
    )
    grad_attn_rows = jnp.concatenate([qkv_rows, out_rows], axis=0)
    summed = attn_sum(jnp.concatenate([grad_attn_rows, vector_rows], axis=1))
    attn_shard = summed[:block_height]
    vector_shard = summed[block_height, :slot]
    rms_values = jnp.sqrt(square_sums / (valid_total * model_width))
    return (
        layer_values.astype(jnp.bfloat16),
        input_grad,
        attn_shard,
        mlp_shard,
        vector_shard,
        rms_values,
    )


def solution(mesh):
    in_specs = (
        P(("fsdp", "seq"), None),
        P(("fsdp", "seq"), None),
        P("fsdp", None),
        P("fsdp"),
        P(("fsdp", "seq"), None),
        P(("fsdp", "seq"), None),
        P(("fsdp", "seq")),
    )
    out_specs = (
        P(("fsdp", "seq"), None),
        P(("fsdp", "seq"), None),
        P(("fsdp", "seq"), None),
        P(("fsdp", "seq"), None),
        P(("fsdp", "seq")),
        P(),
    )
    return jax.shard_map(
        layer_body, mesh=mesh, in_specs=in_specs, out_specs=out_specs, check_vma=False
    )
```

```python
import functools
import jax
import jax.numpy as jnp
from jax import lax
from jax.sharding import PartitionSpec as P

from jax.experimental import pallas as pl
from jax.experimental.pallas import tpu as pltpu


H = 16

BLOCK = 512
NEG = -1e30


def key_ranges(segment_doc, block):
    firsts = segment_doc[::block]
    lasts = segment_doc[block - 1 :: block]
    starts = jnp.sum(segment_doc[None, :] < firsts[:, None], axis=1).astype(jnp.int32)
    ends = jnp.sum(segment_doc[None, :] <= lasts[:, None], axis=1).astype(jnp.int32)
    return starts // block, (ends + block - 1) // block


def _scores(q, k, doc_q, doc_k, scale):
    s = lax.dot_general(q, k, (((1,), (1,)), ((), ())), preferred_element_type=jnp.float32) * scale
    return jnp.where(doc_q == doc_k, s, NEG)


def _fwd_kernel(lo_ref, hi_ref, q_ref, k_ref, v_ref, dq_ref, dk_ref, out_ref, lse_ref, s_buf,
                *, scale, block):
    i = pl.program_id(1)
    lo = lo_ref[i]
    hi = hi_ref[i]
    q = q_ref[...]
    doc_q = dq_ref[...]
    rows = q.shape[0]

    def pass_one(kb, m):
        start = pl.multiple_of(kb * block, block)
        s = _scores(q, k_ref[pl.ds(start, block), :], doc_q, dk_ref[:, pl.ds(start, block)], scale)
        s_buf[kb - lo] = s
        return jnp.maximum(m, jnp.max(s, axis=1, keepdims=True))

    m = lax.fori_loop(lo, hi, pass_one, jnp.full((rows, 1), NEG, jnp.float32))

    def pass_two(kb, l):
        e = jnp.exp(s_buf[kb - lo] - m)
        s_buf[kb - lo] = e
        return l + jnp.sum(e, axis=1, keepdims=True)

    l = lax.fori_loop(lo, hi, pass_two, jnp.zeros((rows, 1), jnp.float32))

    def pass_three(kb, acc):
        start = pl.multiple_of(kb * block, block)
        p = (s_buf[kb - lo] / l).astype(jnp.bfloat16)
        return acc + jnp.dot(p, v_ref[pl.ds(start, block), :], preferred_element_type=jnp.float32)

    acc = lax.fori_loop(lo, hi, pass_three, jnp.zeros(out_ref.shape, jnp.float32))
    out_ref[...] = acc.astype(out_ref.dtype)
    lse_ref[...] = m + jnp.log(l)


def attn_forward(q, k, v, segment_doc, scale, block=BLOCK):
    heads, seg_len, d = q.shape
    lo, hi = key_ranges(segment_doc, block)
    doc_col = segment_doc.reshape(seg_len, 1)
    doc_row = segment_doc.reshape(1, seg_len)
    grid = (heads, seg_len // block)
    spec_q = pl.BlockSpec((None, block, d), lambda h, i, lo, hi: (h, i, 0))
    spec_kv = pl.BlockSpec((None, seg_len, d), lambda h, i, lo, hi: (h, 0, 0))
    spec_dq = pl.BlockSpec((block, 1), lambda h, i, lo, hi: (i, 0))
    spec_dk = pl.BlockSpec((1, seg_len), lambda h, i, lo, hi: (0, 0))
    spec_lse = pl.BlockSpec((None, block, 1), lambda h, i, lo, hi: (h, i, 0))
    return pl.pallas_call(
        functools.partial(_fwd_kernel, scale=scale, block=block),
        grid_spec=pltpu.PrefetchScalarGridSpec(
            num_scalar_prefetch=2,
            grid=grid,
            in_specs=[spec_q, spec_kv, spec_kv, spec_dq, spec_dk],
            out_specs=[spec_q, spec_lse],
            scratch_shapes=[pltpu.VMEM((seg_len // block, block, block), jnp.float32)],
        ),
        out_shape=[
            jax.ShapeDtypeStruct((heads, seg_len, d), jnp.bfloat16),
            jax.ShapeDtypeStruct((heads, seg_len, 1), jnp.float32),
        ],
        compiler_params=pltpu.CompilerParams(dimension_semantics=("arbitrary", "arbitrary")),
    )(lo, hi, q, k, v, doc_col, doc_row)


def _bwd_kernel(lo_ref, hi_ref, q_ref, k_ref, v_ref, da_ref, lse_ref, dq_ref, dk_ref,
                gq_ref, gk_ref, gv_ref, p_buf, dp_buf, *, scale, block):
    i = pl.program_id(1)
    lo = lo_ref[i]
    hi = hi_ref[i]

    @pl.when(i == 0)
    def _():
        gk_ref[...] = jnp.zeros(gk_ref.shape, gk_ref.dtype)
        gv_ref[...] = jnp.zeros(gv_ref.shape, gv_ref.dtype)

    q = q_ref[...]
    da = da_ref[...]
    lse = lse_ref[...]
    doc_q = dq_ref[...]
    rows = q.shape[0]

    def pass_one(kb, delta):
        start = pl.multiple_of(kb * block, block)
        s = _scores(q, k_ref[pl.ds(start, block), :], doc_q, dk_ref[:, pl.ds(start, block)], scale)
        p = jnp.exp(s - lse)
        dp = lax.dot_general(da, v_ref[pl.ds(start, block), :], (((1,), (1,)), ((), ())),
                             preferred_element_type=jnp.float32)
        p_buf[kb - lo] = p
        dp_buf[kb - lo] = dp
        return delta + jnp.sum(dp * p, axis=1, keepdims=True)

    delta = lax.fori_loop(lo, hi, pass_one, jnp.zeros((rows, 1), jnp.float32))

    def pass_two(kb, gq):
        start = pl.multiple_of(kb * block, block)
        p = p_buf[kb - lo]
        ds = (p * (dp_buf[kb - lo] - delta)).astype(jnp.bfloat16)
        pb = p.astype(jnp.bfloat16)
        gq = gq + jnp.dot(ds, k_ref[pl.ds(start, block), :], preferred_element_type=jnp.float32)
        gk_ref[pl.ds(start, block), :] += lax.dot_general(
            ds, q, (((0,), (0,)), ((), ())), preferred_element_type=jnp.float32)
        gv_ref[pl.ds(start, block), :] += lax.dot_general(
            pb, da, (((0,), (0,)), ((), ())), preferred_element_type=jnp.float32)
        return gq

    gq = lax.fori_loop(lo, hi, pass_two, jnp.zeros(gq_ref.shape, jnp.float32))
    gq_ref[...] = gq * scale

    @pl.when(i == pl.num_programs(1) - 1)
    def _():
        gk_ref[...] = gk_ref[...] * scale


def attn_backward(q, k, v, da, lse, segment_doc, scale, block=BLOCK):
    heads, seg_len, d = q.shape
    lo, hi = key_ranges(segment_doc, block)
    doc_col = segment_doc.reshape(seg_len, 1)
    doc_row = segment_doc.reshape(1, seg_len)
    grid = (heads, seg_len // block)
    spec_q = pl.BlockSpec((None, block, d), lambda h, i, lo, hi: (h, i, 0))
    spec_kv = pl.BlockSpec((None, seg_len, d), lambda h, i, lo, hi: (h, 0, 0))
    spec_dq = pl.BlockSpec((block, 1), lambda h, i, lo, hi: (i, 0))
    spec_dk = pl.BlockSpec((1, seg_len), lambda h, i, lo, hi: (0, 0))
    spec_lse = pl.BlockSpec((None, block, 1), lambda h, i, lo, hi: (h, i, 0))
    return pl.pallas_call(
        functools.partial(_bwd_kernel, scale=scale, block=block),
        grid_spec=pltpu.PrefetchScalarGridSpec(
            num_scalar_prefetch=2,
            grid=grid,
            in_specs=[spec_q, spec_kv, spec_kv, spec_q, spec_lse, spec_dq, spec_dk],
            out_specs=[spec_q, spec_kv, spec_kv],
            scratch_shapes=[pltpu.VMEM((seg_len // block, block, block), jnp.float32)] * 2,
        ),
        out_shape=[jax.ShapeDtypeStruct((heads, seg_len, d), jnp.float32)] * 3,
        compiler_params=pltpu.CompilerParams(dimension_semantics=("arbitrary", "arbitrary")),
    )(lo, hi, q, k, v, da, lse, doc_col, doc_row)


EPSILON = 1e-05
ROOT_HALF = 0.7071067811865476
INV_ROOT_TWO_PI = 0.3989422804014327


def norm_forward(values, norm_gain, norm_shift):
    row_mean = jnp.mean(values, axis=1, keepdims=True)
    centered = values - row_mean
    inverse = lax.rsqrt(jnp.mean(centered * centered, axis=1, keepdims=True) + EPSILON)
    scaled = centered * inverse
    return (scaled * norm_gain + norm_shift, scaled, inverse)


def norm_backward(gradient, scaled, inverse, norm_gain):
    grad_scaled = gradient * norm_gain
    grad_mean = jnp.mean(grad_scaled, axis=1, keepdims=True)
    grad_along = jnp.mean(grad_scaled * scaled, axis=1, keepdims=True)
    grad_rows = inverse * (grad_scaled - grad_mean - scaled * grad_along)
    return (grad_rows, jnp.sum(gradient * scaled, axis=0), jnp.sum(gradient, axis=0))


def gelu_slope(entries):
    return 0.5 * (1.0 + lax.erf(entries * ROOT_HALF)) + entries * INV_ROOT_TWO_PI * jnp.exp(
        -0.5 * entries * entries
    )


def ring_gather(rows, count, index):
    half = count // 2
    order = [2 * a for a in range(half)] + [2 * a + 1 for a in reversed(range(half))]
    place = [order.index(s) for s in range(count)]
    forward_pairs = [(order[i], order[(i + 1) % count]) for i in range(count)]
    backward_pairs = [(b, a) for a, b in forward_pairs]
    by_offset = [None] * count
    by_offset[0] = rows
    moving = rows
    for step in range(1, count - count // 2):
        moving = lax.ppermute(moving, "seq", forward_pairs)
        by_offset[count - step] = moving
    moving = rows
    for step in range(1, count // 2 + 1):
        moving = lax.ppermute(moving, "seq", backward_pairs)
        by_offset[step] = moving
    position = jnp.asarray(place, jnp.int32)[index]
    pick = (jnp.asarray(place, jnp.int32) - position) % count
    stacked = jnp.stack(by_offset)
    return jnp.take(stacked, pick, axis=0).reshape((count * rows.shape[0],) + rows.shape[1:])


def attn_sum(values):
    return lax.psum_scatter(values, "fsdp", scatter_dimension=0, tiled=True)[0]


def contract_rows(left, right):
    return lax.dot_general(
        left, right, (((0,), (0,)), ((), ())), preferred_element_type=jnp.float32
    )


def contract_cols(left, right):
    return lax.dot_general(
        left, right, (((1,), (1,)), ((), ())), preferred_element_type=jnp.float32
    )


def layer_body(layer_in, cotangent, doc_ids, valid_len, attn_weights, mlp_weights, param_vector):
    seq_count = lax.axis_size("seq")
    seq_index = lax.axis_index("seq")
    tokens, model_width = layer_in.shape
    head_size = model_width // H
    local_heads = H // seq_count
    score_scale = head_size ** (-0.5)
    attn_rows, vector_slot = attn_weights.shape[0], param_vector.shape[0]
    packed = jnp.concatenate(
        [attn_weights, jnp.pad(param_vector, (0, model_width - vector_slot))[None]], axis=0
    )
    packed_full = lax.all_gather(packed, ("fsdp", "seq"), axis=0, tiled=False)
    attn_full = packed_full[:, :attn_rows].reshape(-1, model_width)
    vector_full = packed_full[:, attn_rows, :vector_slot].reshape(-1)
    mlp_full = lax.all_gather(mlp_weights, ("fsdp", "seq"), axis=0, tiled=True)
    hidden = mlp_full.shape[0] // 2
    vector_wide = vector_full.astype(jnp.float32)
    pieces = [
        vector_wide[slot_index * model_width : (slot_index + 1) * model_width]
        for slot_index in range(8)
    ]
    bias_q, bias_v, bias_o, gain_one, shift_one, bias_two, gain_two, shift_two = pieces
    bias_up = vector_wide[8 * model_width :]
    qkv_weights = attn_full[: 3 * model_width].reshape(3, model_width, model_width)
    out_weights = attn_full[3 * model_width :]
    in_weights = mlp_full[:hidden]
    down_weights = mlp_full[hidden:]
    segment_in = ring_gather(layer_in, seq_count, seq_index)
    segment_doc = doc_ids[0]
    seg_len = segment_doc.shape[0]
    positions = seq_index * tokens + lax.iota(jnp.int32, tokens)
    valid_rows = (positions < valid_len[0]).astype(jnp.float32)[:, None]
    zero_row = jnp.zeros((1, model_width), jnp.float32)
    qkv_bias = jnp.concatenate([bias_q[None], zero_row, bias_v[None]], axis=0)
    head_width = local_heads * head_size
    own_columns = seq_index * head_width
    own_weights = lax.dynamic_slice_in_dim(qkv_weights, own_columns, head_width, axis=2)
    own_bias = lax.dynamic_slice_in_dim(qkv_bias, own_columns, head_width, axis=1)
    projected = (
        jnp.einsum("td,ide->tie", segment_in, own_weights, preferred_element_type=jnp.float32)
        + own_bias[None]
    )
    head_all = jnp.transpose(
        projected.astype(jnp.bfloat16).reshape(seg_len, 3, local_heads, head_size), (1, 2, 0, 3)
    )
    head_q, head_k, head_v = head_all[0], head_all[1], head_all[2]
    head_mixed, log_total = attn_forward(head_q, head_k, head_v, segment_doc, score_scale)
    mixed_rows = jnp.transpose(head_mixed, (1, 0, 2)).reshape(seq_count, tokens, head_width)
    token_mixed = lax.all_to_all(mixed_rows, "seq", split_axis=0, concat_axis=0, tiled=True)
    attn_mixed = jnp.transpose(token_mixed, (1, 0, 2)).reshape(tokens, model_width)
    branch = jnp.dot(attn_mixed, out_weights, preferred_element_type=jnp.float32) + bias_o
    resid_one = layer_in.astype(jnp.float32) + branch
    normed, scaled_one, inverse_one = norm_forward(resid_one, gain_one, shift_one)
    normed_low = normed.astype(jnp.bfloat16)
    normed_seg = lax.all_gather(normed_low, "seq", axis=0, tiled=True)
    upper = contract_cols(normed_low, in_weights) + bias_up
    active_low = jax.nn.gelu(upper, approximate=False).astype(jnp.bfloat16)
    mlp_branch = jnp.dot(active_low, down_weights, preferred_element_type=jnp.float32) + bias_two
    resid_two = normed + mlp_branch
    layer_values, scaled_two, inverse_two = norm_forward(resid_two, gain_two, shift_two)
    squares = jnp.stack(
        [
            jnp.sum(valid_rows * resid_one * resid_one),
            jnp.sum(valid_rows * branch * branch),
            jnp.sum(valid_rows * resid_two * resid_two),
            jnp.sum(valid_rows * mlp_branch * mlp_branch),
        ]
    )
    square_sums, valid_total = lax.psum((squares, jnp.sum(valid_rows)), ("fsdp", "seq"))
    square_sums, valid_total, cotangent = lax.optimization_barrier(
        (square_sums, valid_total, cotangent)
    )
    grad_out = cotangent.astype(jnp.float32)
    grad_resid_two, grad_gain_two, grad_shift_two = norm_backward(
        grad_out, scaled_two, inverse_two, gain_two
    )
    grad_mlp_low = grad_resid_two.astype(jnp.bfloat16)
    grad_bias_two = jnp.sum(grad_mlp_low.astype(jnp.float32), axis=0)
    grad_active = contract_cols(grad_mlp_low, down_weights)
    grad_upper_low = (grad_active * gelu_slope(upper)).astype(jnp.bfloat16)
    grad_bias_up = jnp.sum(grad_upper_low.astype(jnp.float32), axis=0)
    grad_normed = grad_resid_two + jnp.dot(
        grad_upper_low, in_weights, preferred_element_type=jnp.float32
    )
    fsdp_count = lax.axis_size("fsdp")
    mlp_height = 2 * hidden // (fsdp_count * seq_count)
    mlp_groups = hidden // (seq_count * mlp_height)

    def own_rows(rows):
        blocks = rows.reshape((mlp_groups, seq_count, mlp_height) + rows.shape[1:])
        picked = lax.dynamic_index_in_dim(blocks, seq_index, axis=1, keepdims=False)
        return picked.reshape((mlp_groups * mlp_height,) + rows.shape[1:])

    grad_mlp_seg = lax.all_gather(grad_mlp_low, "seq", axis=0, tiled=True)
    upper_own = contract_cols(normed_seg, own_rows(in_weights)) + own_rows(bias_up)
    active_own = jax.nn.gelu(upper_own, approximate=False).astype(jnp.bfloat16)
    grad_active_own = contract_cols(grad_mlp_seg, own_rows(down_weights))
    grad_upper_own = (grad_active_own * gelu_slope(upper_own)).astype(jnp.bfloat16)
    grad_in_own = contract_rows(grad_upper_own, normed_seg)
    grad_down_own = contract_rows(active_own, grad_mlp_seg)
    mlp_stack = jnp.concatenate(
        [
            grad_in_own.reshape(mlp_groups, mlp_height, model_width),
            grad_down_own.reshape(mlp_groups, mlp_height, model_width),
        ],
        axis=0,
    )
    mlp_shard = lax.psum_scatter(mlp_stack, "fsdp", scatter_dimension=0, tiled=True)[0]
    grad_resid_one, grad_gain_one, grad_shift_one = norm_backward(
        grad_normed, scaled_one, inverse_one, gain_one
    )
    grad_branch_low = grad_resid_one.astype(jnp.bfloat16)
    grad_bias_o = jnp.sum(grad_branch_low.astype(jnp.float32), axis=0)
    block_height = 4 * model_width // (fsdp_count * seq_count)
    out_blocks = model_width // (seq_count * block_height)
    out_rows = lax.psum_scatter(
        contract_rows(attn_mixed, grad_branch_low).reshape(
            out_blocks, seq_count, block_height, model_width
        ),
        "seq",
        scatter_dimension=1,
        tiled=True,
    )[:, 0]
    grad_mixed_low = contract_cols(grad_branch_low, out_weights).astype(jnp.bfloat16)
    grad_split = jnp.transpose(
        grad_mixed_low.reshape(tokens, seq_count, head_width), (1, 0, 2)
    )
    grad_heads = lax.all_to_all(grad_split, "seq", split_axis=0, concat_axis=0, tiled=True)
    head_grad = jnp.transpose(grad_heads.reshape(seg_len, local_heads, head_size), (1, 0, 2))

    grad_queries, grad_keys, grad_values = attn_backward(
        head_q, head_k, head_v, head_grad, log_total, segment_doc, score_scale
    )
    head_grads = jnp.transpose(
        jnp.stack([grad_queries, grad_keys, grad_values], axis=0), (2, 0, 1, 3)
    ).astype(jnp.bfloat16)
    head_weight_grads = jnp.einsum(
        "td,tihe->dihe", segment_in, head_grads, preferred_element_type=jnp.float32
    )
    qkv_blocks = 3 * out_blocks
    head_bias_sums = jnp.sum(head_grads.astype(jnp.float32), axis=0).reshape(3, head_width)
    bias_qv = lax.dynamic_update_slice(
        jnp.zeros((2, model_width), jnp.float32),
        head_bias_sums[::2],
        (0, seq_index * head_width),
    )
    grad_vector = jnp.concatenate(
        [
            bias_qv.reshape(-1),
            grad_bias_o,
            grad_gain_one,
            grad_shift_one,
            grad_bias_two,
            grad_gain_two,
            grad_shift_two,
            grad_bias_up,
        ]
    )
    slot = grad_vector.shape[0] // (fsdp_count * seq_count)
    vector_part = jnp.transpose(grad_vector.reshape(fsdp_count, seq_count, slot), (1, 0, 2))
    by_row = jnp.transpose(head_weight_grads.reshape(model_width, 3, head_width), (1, 0, 2))
    row_part = jnp.transpose(
        by_row.reshape(qkv_blocks, seq_count, block_height, head_width), (1, 0, 2, 3)
    )
    row_size = qkv_blocks * block_height * head_width
    exchanged = lax.all_to_all(
        jnp.concatenate(
            [row_part.reshape(seq_count, -1), vector_part.reshape(seq_count, -1)], axis=1
        ),
        "seq", split_axis=0, concat_axis=0, tiled=True,
    )
    row_blocks = exchanged[:, :row_size].reshape(seq_count, qkv_blocks, block_height, head_width)
    qkv_rows = jnp.transpose(row_blocks, (1, 2, 0, 3)).reshape(qkv_blocks, block_height, model_width)
    vector_rows = jnp.sum(exchanged[:, row_size:].reshape(seq_count, fsdp_count, slot), axis=0)
    vector_rows = jnp.pad(vector_rows, ((0, 0), (0, model_width - slot)))[:, None]
    token_grads = lax.all_to_all(
        head_grads.reshape(seq_count, tokens, 3 * head_width),
        "seq", split_axis=0, concat_axis=0, tiled=True,
    )
    grad_qkv = jnp.transpose(
        token_grads.reshape(seq_count, tokens, 3, head_width), (1, 2, 0, 3)
    ).reshape(tokens, 3, model_width)
    input_grad = grad_resid_one + jnp.einsum(
        "tie,ide->td", grad_qkv, qkv_weights, preferred_element_type=jnp.float32
    )
    grad_attn_rows = jnp.concatenate([qkv_rows, out_rows], axis=0)
    summed = attn_sum(jnp.concatenate([grad_attn_rows, vector_rows], axis=1))
    attn_shard = summed[:block_height]
    vector_shard = summed[block_height, :slot]
    rms_values = jnp.sqrt(square_sums / (valid_total * model_width))
    return (
        layer_values.astype(jnp.bfloat16),
        input_grad,
        attn_shard,
        mlp_shard,
        vector_shard,
        rms_values,
    )


def solution(mesh):
    in_specs = (
        P(("fsdp", "seq"), None),
        P(("fsdp", "seq"), None),
        P("fsdp", None),
        P("fsdp"),
        P(("fsdp", "seq"), None),
        P(("fsdp", "seq"), None),
        P(("fsdp", "seq")),
    )
    out_specs = (
        P(("fsdp", "seq"), None),
        P(("fsdp", "seq"), None),
        P(("fsdp", "seq"), None),
        P(("fsdp", "seq"), None),
        P(("fsdp", "seq")),
        P(),
    )
    return jax.shard_map(
        layer_body, mesh=mesh, in_specs=in_specs, out_specs=out_specs, check_vma=False
    )
```

```python
import functools
import jax
import jax.numpy as jnp
from jax import lax
from jax.sharding import PartitionSpec as P

from jax.experimental import pallas as pl
from jax.experimental.pallas import tpu as pltpu


H = 16

BLOCK = 512
NEG = -1e30


def key_ranges(segment_doc, block):
    firsts = segment_doc[::block]
    lasts = segment_doc[block - 1 :: block]
    starts = jnp.sum(segment_doc[None, :] < firsts[:, None], axis=1).astype(jnp.int32)
    ends = jnp.sum(segment_doc[None, :] <= lasts[:, None], axis=1).astype(jnp.int32)
    return starts // block, (ends + block - 1) // block


def _scores(q, k, doc_q, doc_k, scale):
    s = lax.dot_general(q, k, (((1,), (1,)), ((), ())), preferred_element_type=jnp.float32) * scale
    return jnp.where(doc_q == doc_k, s, NEG)


def _fwd_kernel(lo_ref, hi_ref, q_ref, k_ref, v_ref, dq_ref, dk_ref, out_ref, lse_ref, s_buf,
                *, scale, block):
    i = pl.program_id(1)
    lo = lo_ref[i]
    hi = hi_ref[i]
    q = q_ref[...]
    doc_q = dq_ref[...]
    rows = q.shape[0]

    def pass_one(kb, m):
        start = pl.multiple_of(kb * block, block)
        s = _scores(q, k_ref[pl.ds(start, block), :], doc_q, dk_ref[:, pl.ds(start, block)], scale)
        s_buf[kb - lo] = s
        return jnp.maximum(m, jnp.max(s, axis=1, keepdims=True))

    m = lax.fori_loop(lo, hi, pass_one, jnp.full((rows, 1), NEG, jnp.float32))

    def pass_two(kb, l):
        e = jnp.exp(s_buf[kb - lo] - m)
        s_buf[kb - lo] = e
        return l + jnp.sum(e, axis=1, keepdims=True)

    l = lax.fori_loop(lo, hi, pass_two, jnp.zeros((rows, 1), jnp.float32))

    def pass_three(kb, acc):
        start = pl.multiple_of(kb * block, block)
        p = (s_buf[kb - lo] / l).astype(jnp.bfloat16)
        return acc + jnp.dot(p, v_ref[pl.ds(start, block), :], preferred_element_type=jnp.float32)

    acc = lax.fori_loop(lo, hi, pass_three, jnp.zeros(out_ref.shape, jnp.float32))
    out_ref[...] = acc.astype(out_ref.dtype)
    lse_ref[...] = m + jnp.log(l)


def attn_forward(q, k, v, segment_doc, scale, block=BLOCK):
    heads, seg_len, d = q.shape
    lo, hi = key_ranges(segment_doc, block)
    doc_col = segment_doc.reshape(seg_len, 1)
    doc_row = segment_doc.reshape(1, seg_len)
    grid = (heads, seg_len // block)
    spec_q = pl.BlockSpec((None, block, d), lambda h, i, lo, hi: (h, i, 0))
    spec_kv = pl.BlockSpec((None, seg_len, d), lambda h, i, lo, hi: (h, 0, 0))
    spec_dq = pl.BlockSpec((block, 1), lambda h, i, lo, hi: (i, 0))
    spec_dk = pl.BlockSpec((1, seg_len), lambda h, i, lo, hi: (0, 0))
    spec_lse = pl.BlockSpec((None, block, 1), lambda h, i, lo, hi: (h, i, 0))
    return pl.pallas_call(
        functools.partial(_fwd_kernel, scale=scale, block=block),
        grid_spec=pltpu.PrefetchScalarGridSpec(
            num_scalar_prefetch=2,
            grid=grid,
            in_specs=[spec_q, spec_kv, spec_kv, spec_dq, spec_dk],
            out_specs=[spec_q, spec_lse],
            scratch_shapes=[pltpu.VMEM((seg_len // block, block, block), jnp.float32)],
        ),
        out_shape=[
            jax.ShapeDtypeStruct((heads, seg_len, d), jnp.bfloat16),
            jax.ShapeDtypeStruct((heads, seg_len, 1), jnp.float32),
        ],
        compiler_params=pltpu.CompilerParams(dimension_semantics=("arbitrary", "arbitrary")),
    )(lo, hi, q, k, v, doc_col, doc_row)


def _bwd_kernel(lo_ref, hi_ref, q_ref, k_ref, v_ref, da_ref, lse_ref, dq_ref, dk_ref,
                gq_ref, gk_ref, gv_ref, p_buf, dp_buf, *, scale, block):
    i = pl.program_id(1)
    lo = lo_ref[i]
    hi = hi_ref[i]

    @pl.when(i == 0)
    def _():
        gk_ref[...] = jnp.zeros(gk_ref.shape, gk_ref.dtype)
        gv_ref[...] = jnp.zeros(gv_ref.shape, gv_ref.dtype)

    q = q_ref[...]
    da = da_ref[...]
    lse = lse_ref[...]
    doc_q = dq_ref[...]
    rows = q.shape[0]

    def pass_one(kb, delta):
        start = pl.multiple_of(kb * block, block)
        s = _scores(q, k_ref[pl.ds(start, block), :], doc_q, dk_ref[:, pl.ds(start, block)], scale)
        p = jnp.exp(s - lse)
        dp = lax.dot_general(da, v_ref[pl.ds(start, block), :], (((1,), (1,)), ((), ())),
                             preferred_element_type=jnp.float32)
        p_buf[kb - lo] = p
        dp_buf[kb - lo] = dp
        return delta + jnp.sum(dp * p, axis=1, keepdims=True)

    delta = lax.fori_loop(lo, hi, pass_one, jnp.zeros((rows, 1), jnp.float32))

    def pass_two(kb, gq):
        start = pl.multiple_of(kb * block, block)
        p = p_buf[kb - lo]
        ds = (p * (dp_buf[kb - lo] - delta)).astype(jnp.bfloat16)
        pb = p.astype(jnp.bfloat16)
        gq = gq + jnp.dot(ds, k_ref[pl.ds(start, block), :], preferred_element_type=jnp.float32)
        gk_ref[pl.ds(start, block), :] += lax.dot_general(
            ds, q, (((0,), (0,)), ((), ())), preferred_element_type=jnp.float32)
        gv_ref[pl.ds(start, block), :] += lax.dot_general(
            pb, da, (((0,), (0,)), ((), ())), preferred_element_type=jnp.float32)
        return gq

    gq = lax.fori_loop(lo, hi, pass_two, jnp.zeros(gq_ref.shape, jnp.float32))
    gq_ref[...] = gq * scale

    @pl.when(i == pl.num_programs(1) - 1)
    def _():
        gk_ref[...] = gk_ref[...] * scale


def attn_backward(q, k, v, da, lse, segment_doc, scale, block=BLOCK):
    heads, seg_len, d = q.shape
    lo, hi = key_ranges(segment_doc, block)
    doc_col = segment_doc.reshape(seg_len, 1)
    doc_row = segment_doc.reshape(1, seg_len)
    grid = (heads, seg_len // block)
    spec_q = pl.BlockSpec((None, block, d), lambda h, i, lo, hi: (h, i, 0))
    spec_kv = pl.BlockSpec((None, seg_len, d), lambda h, i, lo, hi: (h, 0, 0))
    spec_dq = pl.BlockSpec((block, 1), lambda h, i, lo, hi: (i, 0))
    spec_dk = pl.BlockSpec((1, seg_len), lambda h, i, lo, hi: (0, 0))
    spec_lse = pl.BlockSpec((None, block, 1), lambda h, i, lo, hi: (h, i, 0))
    return pl.pallas_call(
        functools.partial(_bwd_kernel, scale=scale, block=block),
        grid_spec=pltpu.PrefetchScalarGridSpec(
            num_scalar_prefetch=2,
            grid=grid,
            in_specs=[spec_q, spec_kv, spec_kv, spec_q, spec_lse, spec_dq, spec_dk],
            out_specs=[spec_q, spec_kv, spec_kv],
            scratch_shapes=[pltpu.VMEM((seg_len // block, block, block), jnp.float32)] * 2,
        ),
        out_shape=[jax.ShapeDtypeStruct((heads, seg_len, d), jnp.float32)] * 3,
        compiler_params=pltpu.CompilerParams(dimension_semantics=("arbitrary", "arbitrary")),
    )(lo, hi, q, k, v, da, lse, doc_col, doc_row)


EPSILON = 1e-05
ROOT_HALF = 0.7071067811865476
INV_ROOT_TWO_PI = 0.3989422804014327


def norm_forward(values, norm_gain, norm_shift):
    row_mean = jnp.mean(values, axis=1, keepdims=True)
    centered = values - row_mean
    inverse = lax.rsqrt(jnp.mean(centered * centered, axis=1, keepdims=True) + EPSILON)
    scaled = centered * inverse
    return (scaled * norm_gain + norm_shift, scaled, inverse)


def norm_backward(gradient, scaled, inverse, norm_gain):
    grad_scaled = gradient * norm_gain
    grad_mean = jnp.mean(grad_scaled, axis=1, keepdims=True)
    grad_along = jnp.mean(grad_scaled * scaled, axis=1, keepdims=True)
    grad_rows = inverse * (grad_scaled - grad_mean - scaled * grad_along)
    return (grad_rows, jnp.sum(gradient * scaled, axis=0), jnp.sum(gradient, axis=0))


def gelu_slope(entries):
    return 0.5 * (1.0 + lax.erf(entries * ROOT_HALF)) + entries * INV_ROOT_TWO_PI * jnp.exp(
        -0.5 * entries * entries
    )


def ring_gather(rows, count, index):
    half = count // 2
    order = [2 * a for a in range(half)] + [2 * a + 1 for a in reversed(range(half))]
    place = [order.index(s) for s in range(count)]
    forward_pairs = [(order[i], order[(i + 1) % count]) for i in range(count)]
    backward_pairs = [(b, a) for a, b in forward_pairs]
    by_offset = [None] * count
    by_offset[0] = rows
    moving = rows
    for step in range(1, count - count // 2):
        moving = lax.ppermute(moving, "seq", forward_pairs)
        by_offset[count - step] = moving
    moving = rows
    for step in range(1, count // 2 + 1):
        moving = lax.ppermute(moving, "seq", backward_pairs)
        by_offset[step] = moving
    position = jnp.asarray(place, jnp.int32)[index]
    pick = (jnp.asarray(place, jnp.int32) - position) % count
    stacked = jnp.stack(by_offset)
    return jnp.take(stacked, pick, axis=0).reshape((count * rows.shape[0],) + rows.shape[1:])


def attn_sum(values):
    return lax.psum_scatter(values, "fsdp", scatter_dimension=0, tiled=True)[0]


def contract_rows(left, right):
    return lax.dot_general(
        left, right, (((0,), (0,)), ((), ())), preferred_element_type=jnp.float32
    )


def contract_cols(left, right):
    return lax.dot_general(
        left, right, (((1,), (1,)), ((), ())), preferred_element_type=jnp.float32
    )


def layer_body(layer_in, cotangent, doc_ids, valid_len, attn_weights, mlp_weights, param_vector):
    seq_count = lax.axis_size("seq")
    seq_index = lax.axis_index("seq")
    tokens, model_width = layer_in.shape
    head_size = model_width // H
    local_heads = H // seq_count
    score_scale = head_size ** (-0.5)
    attn_rows, vector_slot = attn_weights.shape[0], param_vector.shape[0]
    packed = jnp.concatenate(
        [attn_weights, jnp.pad(param_vector, (0, model_width - vector_slot))[None]], axis=0
    )
    packed_full = lax.all_gather(packed, ("fsdp", "seq"), axis=0, tiled=False)
    attn_full = packed_full[:, :attn_rows].reshape(-1, model_width)
    vector_full = packed_full[:, attn_rows, :vector_slot].reshape(-1)
    mlp_full = lax.all_gather(mlp_weights, ("fsdp", "seq"), axis=0, tiled=True)
    hidden = mlp_full.shape[0] // 2
    vector_wide = vector_full.astype(jnp.float32)
    pieces = [
        vector_wide[slot_index * model_width : (slot_index + 1) * model_width]
        for slot_index in range(8)
    ]
    bias_q, bias_v, bias_o, gain_one, shift_one, bias_two, gain_two, shift_two = pieces
    bias_up = vector_wide[8 * model_width :]
    qkv_weights = attn_full[: 3 * model_width].reshape(3, model_width, model_width)
    out_weights = attn_full[3 * model_width :]
    in_weights = mlp_full[:hidden]
    down_weights = mlp_full[hidden:]
    segment_in = ring_gather(layer_in, seq_count, seq_index)
    segment_doc = doc_ids[0]
    seg_len = segment_doc.shape[0]
    positions = seq_index * tokens + lax.iota(jnp.int32, tokens)
    valid_rows = (positions < valid_len[0]).astype(jnp.float32)[:, None]
    zero_row = jnp.zeros((1, model_width), jnp.float32)
    qkv_bias = jnp.concatenate([bias_q[None], zero_row, bias_v[None]], axis=0)
    head_width = local_heads * head_size
    own_columns = seq_index * head_width
    own_weights = lax.dynamic_slice_in_dim(qkv_weights, own_columns, head_width, axis=2)
    own_bias = lax.dynamic_slice_in_dim(qkv_bias, own_columns, head_width, axis=1)
    projected = (
        jnp.einsum("td,ide->tie", segment_in, own_weights, preferred_element_type=jnp.float32)
        + own_bias[None]
    )
    head_all = jnp.transpose(
        projected.astype(jnp.bfloat16).reshape(seg_len, 3, local_heads, head_size), (1, 2, 0, 3)
    )
    head_q, head_k, head_v = head_all[0], head_all[1], head_all[2]
    head_mixed, log_total = attn_forward(head_q, head_k, head_v, segment_doc, score_scale)
    mixed_rows = jnp.transpose(head_mixed, (1, 0, 2)).reshape(seq_count, tokens, head_width)
    token_mixed = lax.all_to_all(mixed_rows, "seq", split_axis=0, concat_axis=0, tiled=True)
    attn_mixed = jnp.transpose(token_mixed, (1, 0, 2)).reshape(tokens, model_width)
    branch = jnp.dot(attn_mixed, out_weights, preferred_element_type=jnp.float32) + bias_o
    resid_one = layer_in.astype(jnp.float32) + branch
    normed, scaled_one, inverse_one = norm_forward(resid_one, gain_one, shift_one)
    normed_low = normed.astype(jnp.bfloat16)
    normed_seg = lax.all_gather(normed_low, "seq", axis=0, tiled=True)
    upper = contract_cols(normed_low, in_weights) + bias_up
    active_low = jax.nn.gelu(upper, approximate=False).astype(jnp.bfloat16)
    mlp_branch = jnp.dot(active_low, down_weights, preferred_element_type=jnp.float32) + bias_two
    resid_two = normed + mlp_branch
    layer_values, scaled_two, inverse_two = norm_forward(resid_two, gain_two, shift_two)
    squares = jnp.stack(
        [
            jnp.sum(valid_rows * resid_one * resid_one),
            jnp.sum(valid_rows * branch * branch),
            jnp.sum(valid_rows * resid_two * resid_two),
            jnp.sum(valid_rows * mlp_branch * mlp_branch),
        ]
    )
    square_sums, valid_total = lax.psum((squares, jnp.sum(valid_rows)), ("fsdp", "seq"))
    square_sums, valid_total, cotangent = lax.optimization_barrier(
        (square_sums, valid_total, cotangent)
    )
    grad_out = cotangent.astype(jnp.float32)
    grad_resid_two, grad_gain_two, grad_shift_two = norm_backward(
        grad_out, scaled_two, inverse_two, gain_two
    )
    grad_mlp_low = grad_resid_two.astype(jnp.bfloat16)
    grad_bias_two = jnp.sum(grad_mlp_low.astype(jnp.float32), axis=0)
    grad_active = contract_cols(grad_mlp_low, down_weights)
    grad_upper_low = (grad_active * gelu_slope(upper)).astype(jnp.bfloat16)
    grad_bias_up = jnp.sum(grad_upper_low.astype(jnp.float32), axis=0)
    grad_normed = grad_resid_two + jnp.dot(
        grad_upper_low, in_weights, preferred_element_type=jnp.float32
    )
    fsdp_count = lax.axis_size("fsdp")
    mlp_height = 2 * hidden // (fsdp_count * seq_count)
    mlp_groups = hidden // (seq_count * mlp_height)

    def own_rows(rows):
        blocks = rows.reshape((mlp_groups, seq_count, mlp_height) + rows.shape[1:])
        picked = lax.dynamic_index_in_dim(blocks, seq_index, axis=1, keepdims=False)
        return picked.reshape((mlp_groups * mlp_height,) + rows.shape[1:])

    grad_mlp_seg = lax.all_gather(grad_mlp_low, "seq", axis=0, tiled=True)
    upper_own = contract_cols(normed_seg, own_rows(in_weights)) + own_rows(bias_up)
    active_own = jax.nn.gelu(upper_own, approximate=False).astype(jnp.bfloat16)
    grad_active_own = contract_cols(grad_mlp_seg, own_rows(down_weights))
    grad_upper_own = (grad_active_own * gelu_slope(upper_own)).astype(jnp.bfloat16)
    grad_in_own = contract_rows(grad_upper_own, normed_seg)
    grad_down_own = contract_rows(active_own, grad_mlp_seg)
    mlp_stack = jnp.concatenate(
        [
            grad_in_own.reshape(mlp_groups, mlp_height, model_width),
            grad_down_own.reshape(mlp_groups, mlp_height, model_width),
        ],
        axis=0,
    )
    mlp_shard = lax.psum_scatter(mlp_stack, "fsdp", scatter_dimension=0, tiled=True)[0]
    grad_resid_one, grad_gain_one, grad_shift_one = norm_backward(
        grad_normed, scaled_one, inverse_one, gain_one
    )
    grad_branch_low = grad_resid_one.astype(jnp.bfloat16)
    grad_bias_o = jnp.sum(grad_branch_low.astype(jnp.float32), axis=0)
    block_height = 4 * model_width // (fsdp_count * seq_count)
    out_blocks = model_width // (seq_count * block_height)
    out_partial = jnp.transpose(
        contract_rows(attn_mixed, grad_branch_low).reshape(
            out_blocks, seq_count, block_height, model_width
        ),
        (1, 0, 2, 3),
    )
    out_parts = lax.all_to_all(out_partial, "seq", split_axis=0, concat_axis=0, tiled=True)
    out_rows = jnp.sum(out_parts, axis=0)
    grad_mixed_low = contract_cols(grad_branch_low, out_weights).astype(jnp.bfloat16)
    grad_split = jnp.transpose(
        grad_mixed_low.reshape(tokens, seq_count, head_width), (1, 0, 2)
    )
    grad_heads = lax.all_to_all(grad_split, "seq", split_axis=0, concat_axis=0, tiled=True)
    head_grad = jnp.transpose(grad_heads.reshape(seg_len, local_heads, head_size), (1, 0, 2))

    grad_queries, grad_keys, grad_values = attn_backward(
        head_q, head_k, head_v, head_grad, log_total, segment_doc, score_scale
    )
    head_grads = jnp.transpose(
        jnp.stack([grad_queries, grad_keys, grad_values], axis=0), (2, 0, 1, 3)
    ).astype(jnp.bfloat16)
    head_weight_grads = jnp.einsum(
        "td,tihe->dihe", segment_in, head_grads, preferred_element_type=jnp.float32
    )
    qkv_blocks = 3 * out_blocks
    head_bias_sums = jnp.sum(head_grads.astype(jnp.float32), axis=0).reshape(3, head_width)
    bias_qv = lax.dynamic_update_slice(
        jnp.zeros((2, model_width), jnp.float32),
        head_bias_sums[::2],
        (0, seq_index * head_width),
    )
    grad_vector = jnp.concatenate(
        [
            bias_qv.reshape(-1),
            grad_bias_o,
            grad_gain_one,
            grad_shift_one,
            grad_bias_two,
            grad_gain_two,
            grad_shift_two,
            grad_bias_up,
        ]
    )
    slot = grad_vector.shape[0] // (fsdp_count * seq_count)
    vector_part = jnp.transpose(grad_vector.reshape(fsdp_count, seq_count, slot), (1, 0, 2))
    by_row = jnp.transpose(head_weight_grads.reshape(model_width, 3, head_width), (1, 0, 2))
    row_part = jnp.transpose(
        by_row.reshape(qkv_blocks, seq_count, block_height, head_width), (1, 0, 2, 3)
    )
    row_size = qkv_blocks * block_height * head_width
    exchanged = lax.all_to_all(
        jnp.concatenate(
            [row_part.reshape(seq_count, -1), vector_part.reshape(seq_count, -1)], axis=1
        ),
        "seq", split_axis=0, concat_axis=0, tiled=True,
    )
    row_blocks = exchanged[:, :row_size].reshape(seq_count, qkv_blocks, block_height, head_width)
    qkv_rows = jnp.transpose(row_blocks, (1, 2, 0, 3)).reshape(qkv_blocks, block_height, model_width)
    vector_rows = jnp.sum(exchanged[:, row_size:].reshape(seq_count, fsdp_count, slot), axis=0)
    vector_rows = jnp.pad(vector_rows, ((0, 0), (0, model_width - slot)))[:, None]
    token_grads = lax.all_to_all(
        head_grads.reshape(seq_count, tokens, 3 * head_width),
        "seq", split_axis=0, concat_axis=0, tiled=True,
    )
    grad_qkv = jnp.transpose(
        token_grads.reshape(seq_count, tokens, 3, head_width), (1, 2, 0, 3)
    ).reshape(tokens, 3, model_width)
    input_grad = grad_resid_one + jnp.einsum(
        "tie,ide->td", grad_qkv, qkv_weights, preferred_element_type=jnp.float32
    )
    grad_attn_rows = jnp.concatenate([qkv_rows, out_rows], axis=0)
    summed = attn_sum(jnp.concatenate([grad_attn_rows, vector_rows], axis=1))
    attn_shard = summed[:block_height]
    vector_shard = summed[block_height, :slot]
    rms_values = jnp.sqrt(square_sums / (valid_total * model_width))
    return (
        layer_values.astype(jnp.bfloat16),
        input_grad,
        attn_shard,
        mlp_shard,
        vector_shard,
        rms_values,
    )


def solution(mesh):
    in_specs = (
        P(("fsdp", "seq"), None),
        P(("fsdp", "seq"), None),
        P("fsdp", None),
        P("fsdp"),
        P(("fsdp", "seq"), None),
        P(("fsdp", "seq"), None),
        P(("fsdp", "seq")),
    )
    out_specs = (
        P(("fsdp", "seq"), None),
        P(("fsdp", "seq"), None),
        P(("fsdp", "seq"), None),
        P(("fsdp", "seq"), None),
        P(("fsdp", "seq")),
        P(),
    )
    return jax.shard_map(
        layer_body, mesh=mesh, in_specs=in_specs, out_specs=out_specs, check_vma=False
    )
```

```python
import functools
import jax
import jax.numpy as jnp
from jax import lax
from jax.sharding import PartitionSpec as P

from jax.experimental import pallas as pl
from jax.experimental.pallas import tpu as pltpu


H = 16

BLOCK = 768
NEG = -1e30


def key_ranges(segment_doc, block):
    firsts = segment_doc[::block]
    lasts = segment_doc[block - 1 :: block]
    starts = jnp.sum(segment_doc[None, :] < firsts[:, None], axis=1).astype(jnp.int32)
    ends = jnp.sum(segment_doc[None, :] <= lasts[:, None], axis=1).astype(jnp.int32)
    return starts // block, (ends + block - 1) // block


def _scores(q, k, doc_q, doc_k, scale):
    s = lax.dot_general(q, k, (((1,), (1,)), ((), ())), preferred_element_type=jnp.float32) * scale
    return jnp.where(doc_q == doc_k, s, NEG)


def _fwd_kernel(lo_ref, hi_ref, q_ref, k_ref, v_ref, dq_ref, dk_ref, out_ref, lse_ref, s_buf,
                *, scale, block):
    i = pl.program_id(1)
    lo = lo_ref[i]
    hi = hi_ref[i]
    q = q_ref[...]
    doc_q = dq_ref[...]
    rows = q.shape[0]

    def pass_one(kb, m):
        start = pl.multiple_of(kb * block, block)
        s = _scores(q, k_ref[pl.ds(start, block), :], doc_q, dk_ref[:, pl.ds(start, block)], scale)
        s_buf[kb - lo] = s
        return jnp.maximum(m, jnp.max(s, axis=1, keepdims=True))

    m = lax.fori_loop(lo, hi, pass_one, jnp.full((rows, 1), NEG, jnp.float32))

    def pass_two(kb, l):
        e = jnp.exp(s_buf[kb - lo] - m)
        s_buf[kb - lo] = e
        return l + jnp.sum(e, axis=1, keepdims=True)

    l = lax.fori_loop(lo, hi, pass_two, jnp.zeros((rows, 1), jnp.float32))

    def pass_three(kb, acc):
        start = pl.multiple_of(kb * block, block)
        p = (s_buf[kb - lo] / l).astype(jnp.bfloat16)
        return acc + jnp.dot(p, v_ref[pl.ds(start, block), :], preferred_element_type=jnp.float32)

    acc = lax.fori_loop(lo, hi, pass_three, jnp.zeros(out_ref.shape, jnp.float32))
    out_ref[...] = acc.astype(out_ref.dtype)
    lse_ref[...] = m + jnp.log(l)


def attn_forward(q, k, v, segment_doc, scale, block=BLOCK):
    heads, seg_len, d = q.shape
    lo, hi = key_ranges(segment_doc, block)
    doc_col = segment_doc.reshape(seg_len, 1)
    doc_row = segment_doc.reshape(1, seg_len)
    grid = (heads, seg_len // block)
    spec_q = pl.BlockSpec((None, block, d), lambda h, i, lo, hi: (h, i, 0))
    spec_kv = pl.BlockSpec((None, seg_len, d), lambda h, i, lo, hi: (h, 0, 0))
    spec_dq = pl.BlockSpec((block, 1), lambda h, i, lo, hi: (i, 0))
    spec_dk = pl.BlockSpec((1, seg_len), lambda h, i, lo, hi: (0, 0))
    spec_lse = pl.BlockSpec((None, block, 1), lambda h, i, lo, hi: (h, i, 0))
    return pl.pallas_call(
        functools.partial(_fwd_kernel, scale=scale, block=block),
        grid_spec=pltpu.PrefetchScalarGridSpec(
            num_scalar_prefetch=2,
            grid=grid,
            in_specs=[spec_q, spec_kv, spec_kv, spec_dq, spec_dk],
            out_specs=[spec_q, spec_lse],
            scratch_shapes=[pltpu.VMEM((seg_len // block, block, block), jnp.float32)],
        ),
        out_shape=[
            jax.ShapeDtypeStruct((heads, seg_len, d), jnp.bfloat16),
            jax.ShapeDtypeStruct((heads, seg_len, 1), jnp.float32),
        ],
        compiler_params=pltpu.CompilerParams(dimension_semantics=("arbitrary", "arbitrary")),
    )(lo, hi, q, k, v, doc_col, doc_row)


def _bwd_kernel(lo_ref, hi_ref, q_ref, k_ref, v_ref, da_ref, lse_ref, dq_ref, dk_ref,
                gq_ref, gk_ref, gv_ref, p_buf, dp_buf, *, scale, block):
    i = pl.program_id(1)
    lo = lo_ref[i]
    hi = hi_ref[i]

    @pl.when(i == 0)
    def _():
        gk_ref[...] = jnp.zeros(gk_ref.shape, gk_ref.dtype)
        gv_ref[...] = jnp.zeros(gv_ref.shape, gv_ref.dtype)

    q = q_ref[...]
    da = da_ref[...]
    lse = lse_ref[...]
    doc_q = dq_ref[...]
    rows = q.shape[0]

    def pass_one(kb, delta):
        start = pl.multiple_of(kb * block, block)
        s = _scores(q, k_ref[pl.ds(start, block), :], doc_q, dk_ref[:, pl.ds(start, block)], scale)
        p = jnp.exp(s - lse)
        dp = lax.dot_general(da, v_ref[pl.ds(start, block), :], (((1,), (1,)), ((), ())),
                             preferred_element_type=jnp.float32)
        p_buf[kb - lo] = p
        dp_buf[kb - lo] = dp
        return delta + jnp.sum(dp * p, axis=1, keepdims=True)

    delta = lax.fori_loop(lo, hi, pass_one, jnp.zeros((rows, 1), jnp.float32))

    def pass_two(kb, gq):
        start = pl.multiple_of(kb * block, block)
        p = p_buf[kb - lo]
        ds = (p * (dp_buf[kb - lo] - delta)).astype(jnp.bfloat16)
        pb = p.astype(jnp.bfloat16)
        gq = gq + jnp.dot(ds, k_ref[pl.ds(start, block), :], preferred_element_type=jnp.float32)
        gk_ref[pl.ds(start, block), :] += lax.dot_general(
            ds, q, (((0,), (0,)), ((), ())), preferred_element_type=jnp.float32)
        gv_ref[pl.ds(start, block), :] += lax.dot_general(
            pb, da, (((0,), (0,)), ((), ())), preferred_element_type=jnp.float32)
        return gq

    gq = lax.fori_loop(lo, hi, pass_two, jnp.zeros(gq_ref.shape, jnp.float32))
    gq_ref[...] = gq * scale

    @pl.when(i == pl.num_programs(1) - 1)
    def _():
        gk_ref[...] = gk_ref[...] * scale


def attn_backward(q, k, v, da, lse, segment_doc, scale, block=BLOCK):
    heads, seg_len, d = q.shape
    lo, hi = key_ranges(segment_doc, block)
    doc_col = segment_doc.reshape(seg_len, 1)
    doc_row = segment_doc.reshape(1, seg_len)
    grid = (heads, seg_len // block)
    spec_q = pl.BlockSpec((None, block, d), lambda h, i, lo, hi: (h, i, 0))
    spec_kv = pl.BlockSpec((None, seg_len, d), lambda h, i, lo, hi: (h, 0, 0))
    spec_dq = pl.BlockSpec((block, 1), lambda h, i, lo, hi: (i, 0))
    spec_dk = pl.BlockSpec((1, seg_len), lambda h, i, lo, hi: (0, 0))
    spec_lse = pl.BlockSpec((None, block, 1), lambda h, i, lo, hi: (h, i, 0))
    return pl.pallas_call(
        functools.partial(_bwd_kernel, scale=scale, block=block),
        grid_spec=pltpu.PrefetchScalarGridSpec(
            num_scalar_prefetch=2,
            grid=grid,
            in_specs=[spec_q, spec_kv, spec_kv, spec_q, spec_lse, spec_dq, spec_dk],
            out_specs=[spec_q, spec_kv, spec_kv],
            scratch_shapes=[pltpu.VMEM((seg_len // block, block, block), jnp.float32)] * 2,
        ),
        out_shape=[jax.ShapeDtypeStruct((heads, seg_len, d), jnp.float32)] * 3,
        compiler_params=pltpu.CompilerParams(dimension_semantics=("arbitrary", "arbitrary")),
    )(lo, hi, q, k, v, da, lse, doc_col, doc_row)


EPSILON = 1e-05
ROOT_HALF = 0.7071067811865476
INV_ROOT_TWO_PI = 0.3989422804014327


def norm_forward(values, norm_gain, norm_shift):
    row_mean = jnp.mean(values, axis=1, keepdims=True)
    centered = values - row_mean
    inverse = lax.rsqrt(jnp.mean(centered * centered, axis=1, keepdims=True) + EPSILON)
    scaled = centered * inverse
    return (scaled * norm_gain + norm_shift, scaled, inverse)


def norm_backward(gradient, scaled, inverse, norm_gain):
    grad_scaled = gradient * norm_gain
    grad_mean = jnp.mean(grad_scaled, axis=1, keepdims=True)
    grad_along = jnp.mean(grad_scaled * scaled, axis=1, keepdims=True)
    grad_rows = inverse * (grad_scaled - grad_mean - scaled * grad_along)
    return (grad_rows, jnp.sum(gradient * scaled, axis=0), jnp.sum(gradient, axis=0))


def gelu_slope(entries):
    return 0.5 * (1.0 + lax.erf(entries * ROOT_HALF)) + entries * INV_ROOT_TWO_PI * jnp.exp(
        -0.5 * entries * entries
    )


def ring_gather(rows, count, index):
    half = count // 2
    order = [2 * a for a in range(half)] + [2 * a + 1 for a in reversed(range(half))]
    place = [order.index(s) for s in range(count)]
    forward_pairs = [(order[i], order[(i + 1) % count]) for i in range(count)]
    backward_pairs = [(b, a) for a, b in forward_pairs]
    by_offset = [None] * count
    by_offset[0] = rows
    moving = rows
    for step in range(1, count - count // 2):
        moving = lax.ppermute(moving, "seq", forward_pairs)
        by_offset[count - step] = moving
    moving = rows
    for step in range(1, count // 2 + 1):
        moving = lax.ppermute(moving, "seq", backward_pairs)
        by_offset[step] = moving
    position = jnp.asarray(place, jnp.int32)[index]
    pick = (jnp.asarray(place, jnp.int32) - position) % count
    stacked = jnp.stack(by_offset)
    return jnp.take(stacked, pick, axis=0).reshape((count * rows.shape[0],) + rows.shape[1:])


def attn_sum(values):
    return lax.psum_scatter(values, "fsdp", scatter_dimension=0, tiled=True)[0]


def contract_rows(left, right):
    return lax.dot_general(
        left, right, (((0,), (0,)), ((), ())), preferred_element_type=jnp.float32
    )


def contract_cols(left, right):
    return lax.dot_general(
        left, right, (((1,), (1,)), ((), ())), preferred_element_type=jnp.float32
    )


def layer_body(layer_in, cotangent, doc_ids, valid_len, attn_weights, mlp_weights, param_vector):
    seq_count = lax.axis_size("seq")
    seq_index = lax.axis_index("seq")
    tokens, model_width = layer_in.shape
    head_size = model_width // H
    local_heads = H // seq_count
    score_scale = head_size ** (-0.5)
    attn_rows, vector_slot = attn_weights.shape[0], param_vector.shape[0]
    packed = jnp.concatenate(
        [attn_weights, jnp.pad(param_vector, (0, model_width - vector_slot))[None]], axis=0
    )
    packed_full = lax.all_gather(packed, ("fsdp", "seq"), axis=0, tiled=False)
    attn_full = packed_full[:, :attn_rows].reshape(-1, model_width)
    vector_full = packed_full[:, attn_rows, :vector_slot].reshape(-1)
    mlp_full = lax.all_gather(mlp_weights, ("fsdp", "seq"), axis=0, tiled=True)
    hidden = mlp_full.shape[0] // 2
    vector_wide = vector_full.astype(jnp.float32)
    pieces = [
        vector_wide[slot_index * model_width : (slot_index + 1) * model_width]
        for slot_index in range(8)
    ]
    bias_q, bias_v, bias_o, gain_one, shift_one, bias_two, gain_two, shift_two = pieces
    bias_up = vector_wide[8 * model_width :]
    qkv_weights = attn_full[: 3 * model_width].reshape(3, model_width, model_width)
    out_weights = attn_full[3 * model_width :]
    in_weights = mlp_full[:hidden]
    down_weights = mlp_full[hidden:]
    segment_in = ring_gather(layer_in, seq_count, seq_index)
    segment_doc = doc_ids[0]
    seg_len = segment_doc.shape[0]
    positions = seq_index * tokens + lax.iota(jnp.int32, tokens)
    valid_rows = (positions < valid_len[0]).astype(jnp.float32)[:, None]
    zero_row = jnp.zeros((1, model_width), jnp.float32)
    qkv_bias = jnp.concatenate([bias_q[None], zero_row, bias_v[None]], axis=0)
    head_width = local_heads * head_size
    own_columns = seq_index * head_width
    own_weights = lax.dynamic_slice_in_dim(qkv_weights, own_columns, head_width, axis=2)
    own_bias = lax.dynamic_slice_in_dim(qkv_bias, own_columns, head_width, axis=1)
    projected = (
        jnp.einsum("td,ide->tie", segment_in, own_weights, preferred_element_type=jnp.float32)
        + own_bias[None]
    )
    head_all = jnp.transpose(
        projected.astype(jnp.bfloat16).reshape(seg_len, 3, local_heads, head_size), (1, 2, 0, 3)
    )
    head_q, head_k, head_v = head_all[0], head_all[1], head_all[2]
    head_mixed, log_total = attn_forward(head_q, head_k, head_v, segment_doc, score_scale)
    mixed_rows = jnp.transpose(head_mixed, (1, 0, 2)).reshape(seq_count, tokens, head_width)
    token_mixed = lax.all_to_all(mixed_rows, "seq", split_axis=0, concat_axis=0, tiled=True)
    attn_mixed = jnp.transpose(token_mixed, (1, 0, 2)).reshape(tokens, model_width)
    branch = jnp.dot(attn_mixed, out_weights, preferred_element_type=jnp.float32) + bias_o
    resid_one = layer_in.astype(jnp.float32) + branch
    normed, scaled_one, inverse_one = norm_forward(resid_one, gain_one, shift_one)
    normed_low = normed.astype(jnp.bfloat16)
    normed_seg = lax.all_gather(normed_low, "seq", axis=0, tiled=True)
    upper = contract_cols(normed_low, in_weights) + bias_up
    active_low = jax.nn.gelu(upper, approximate=False).astype(jnp.bfloat16)
    mlp_branch = jnp.dot(active_low, down_weights, preferred_element_type=jnp.float32) + bias_two
    resid_two = normed + mlp_branch
    layer_values, scaled_two, inverse_two = norm_forward(resid_two, gain_two, shift_two)
    squares = jnp.stack(
        [
            jnp.sum(valid_rows * resid_one * resid_one),
            jnp.sum(valid_rows * branch * branch),
            jnp.sum(valid_rows * resid_two * resid_two),
            jnp.sum(valid_rows * mlp_branch * mlp_branch),
        ]
    )
    own_sums = jnp.pad(jnp.concatenate([squares, jnp.sum(valid_rows)[None]]), (0, 3))
    grad_out = cotangent.astype(jnp.float32)
    grad_resid_two, grad_gain_two, grad_shift_two = norm_backward(
        grad_out, scaled_two, inverse_two, gain_two
    )
    grad_mlp_low = grad_resid_two.astype(jnp.bfloat16)
    grad_bias_two = jnp.sum(grad_mlp_low.astype(jnp.float32), axis=0)
    grad_active = contract_cols(grad_mlp_low, down_weights)
    grad_upper_low = (grad_active * gelu_slope(upper)).astype(jnp.bfloat16)
    grad_bias_up = jnp.sum(grad_upper_low.astype(jnp.float32), axis=0)
    grad_normed = grad_resid_two + jnp.dot(
        grad_upper_low, in_weights, preferred_element_type=jnp.float32
    )
    fsdp_count = lax.axis_size("fsdp")
    mlp_height = 2 * hidden // (fsdp_count * seq_count)
    mlp_groups = hidden // (seq_count * mlp_height)

    def own_rows(rows):
        blocks = rows.reshape((mlp_groups, seq_count, mlp_height) + rows.shape[1:])
        picked = lax.dynamic_index_in_dim(blocks, seq_index, axis=1, keepdims=False)
        return picked.reshape((mlp_groups * mlp_height,) + rows.shape[1:])

    grad_mlp_seg = lax.all_gather(grad_mlp_low, "seq", axis=0, tiled=True)
    upper_own = contract_cols(normed_seg, own_rows(in_weights)) + own_rows(bias_up)
    active_own = jax.nn.gelu(upper_own, approximate=False).astype(jnp.bfloat16)
    grad_active_own = contract_cols(grad_mlp_seg, own_rows(down_weights))
    grad_upper_own = (grad_active_own * gelu_slope(upper_own)).astype(jnp.bfloat16)
    grad_in_own = contract_rows(grad_upper_own, normed_seg)
    grad_down_own = contract_rows(active_own, grad_mlp_seg)
    mlp_stack = jnp.concatenate(
        [
            grad_in_own.reshape(mlp_groups, mlp_height, model_width),
            grad_down_own.reshape(mlp_groups, mlp_height, model_width),
        ],
        axis=0,
    )
    mlp_shard = lax.psum_scatter(mlp_stack, "fsdp", scatter_dimension=0, tiled=True)[0]
    grad_resid_one, grad_gain_one, grad_shift_one = norm_backward(
        grad_normed, scaled_one, inverse_one, gain_one
    )
    grad_branch_low = grad_resid_one.astype(jnp.bfloat16)
    grad_bias_o = jnp.sum(grad_branch_low.astype(jnp.float32), axis=0)
    block_height = 4 * model_width // (fsdp_count * seq_count)
    out_blocks = model_width // (seq_count * block_height)
    out_partial = jnp.transpose(
        contract_rows(attn_mixed, grad_branch_low).reshape(
            out_blocks, seq_count, block_height, model_width
        ),
        (1, 0, 2, 3),
    )
    out_parts = lax.all_to_all(out_partial, "seq", split_axis=0, concat_axis=0, tiled=True)
    out_rows = jnp.sum(out_parts, axis=0)
    grad_mixed_low = contract_cols(grad_branch_low, out_weights).astype(jnp.bfloat16)
    grad_split = jnp.transpose(
        grad_mixed_low.reshape(tokens, seq_count, head_width), (1, 0, 2)
    )
    grad_heads = lax.all_to_all(grad_split, "seq", split_axis=0, concat_axis=0, tiled=True)
    head_grad = jnp.transpose(grad_heads.reshape(seg_len, local_heads, head_size), (1, 0, 2))

    grad_queries, grad_keys, grad_values = attn_backward(
        head_q, head_k, head_v, head_grad, log_total, segment_doc, score_scale
    )
    head_grads = jnp.transpose(
        jnp.stack([grad_queries, grad_keys, grad_values], axis=0), (2, 0, 1, 3)
    ).astype(jnp.bfloat16)
    head_weight_grads = jnp.einsum(
        "td,tihe->dihe", segment_in, head_grads, preferred_element_type=jnp.float32
    )
    qkv_blocks = 3 * out_blocks
    head_bias_sums = jnp.sum(head_grads.astype(jnp.float32), axis=0).reshape(3, head_width)
    bias_qv = lax.dynamic_update_slice(
        jnp.zeros((2, model_width), jnp.float32),
        head_bias_sums[::2],
        (0, seq_index * head_width),
    )
    grad_vector = jnp.concatenate(
        [
            bias_qv.reshape(-1),
            grad_bias_o,
            grad_gain_one,
            grad_shift_one,
            grad_bias_two,
            grad_gain_two,
            grad_shift_two,
            grad_bias_up,
        ]
    )
    slot = grad_vector.shape[0] // (fsdp_count * seq_count)
    vector_part = jnp.transpose(grad_vector.reshape(fsdp_count, seq_count, slot), (1, 0, 2))
    sums_part = jnp.broadcast_to(own_sums, (seq_count, fsdp_count, own_sums.shape[0]))
    vector_part = jnp.concatenate([vector_part, sums_part], axis=2)
    wide_slot = slot + own_sums.shape[0]
    by_row = jnp.transpose(head_weight_grads.reshape(model_width, 3, head_width), (1, 0, 2))
    row_part = jnp.transpose(
        by_row.reshape(qkv_blocks, seq_count, block_height, head_width), (1, 0, 2, 3)
    )
    row_size = qkv_blocks * block_height * head_width
    exchanged = lax.all_to_all(
        jnp.concatenate(
            [row_part.reshape(seq_count, -1), vector_part.reshape(seq_count, -1)], axis=1
        ),
        "seq", split_axis=0, concat_axis=0, tiled=True,
    )
    row_blocks = exchanged[:, :row_size].reshape(seq_count, qkv_blocks, block_height, head_width)
    qkv_rows = jnp.transpose(row_blocks, (1, 2, 0, 3)).reshape(qkv_blocks, block_height, model_width)
    vector_rows = jnp.sum(
        exchanged[:, row_size:].reshape(seq_count, fsdp_count, wide_slot), axis=0
    )
    sums_width = own_sums.shape[0]
    segment_sums = vector_rows[0, slot:]
    sums_groups = lax.dynamic_update_slice(
        jnp.zeros((fsdp_count * sums_width,), jnp.float32),
        segment_sums,
        (lax.axis_index("fsdp") * sums_width,),
    )
    vector_rows = jnp.concatenate(
        [
            vector_rows[:, :slot],
            jnp.broadcast_to(sums_groups, (fsdp_count, fsdp_count * sums_width)),
        ],
        axis=1,
    )
    vector_rows = jnp.pad(
        vector_rows, ((0, 0), (0, model_width - vector_rows.shape[1]))
    )[:, None]
    token_grads = lax.all_to_all(
        head_grads.reshape(seq_count, tokens, 3 * head_width),
        "seq", split_axis=0, concat_axis=0, tiled=True,
    )
    grad_qkv = jnp.transpose(
        token_grads.reshape(seq_count, tokens, 3, head_width), (1, 2, 0, 3)
    ).reshape(tokens, 3, model_width)
    input_grad = grad_resid_one + jnp.einsum(
        "tie,ide->td", grad_qkv, qkv_weights, preferred_element_type=jnp.float32
    )
    grad_attn_rows = jnp.concatenate([qkv_rows, out_rows], axis=0)
    summed = attn_sum(jnp.concatenate([grad_attn_rows, vector_rows], axis=1))
    attn_shard = summed[:block_height]
    vector_shard = summed[block_height, :slot]
    total_sums = jnp.sum(
        summed[block_height, slot : slot + fsdp_count * sums_width].reshape(fsdp_count, sums_width),
        axis=0,
    )
    square_sums, valid_total = total_sums[:4], total_sums[4]
    rms_values = jnp.sqrt(square_sums / (valid_total * model_width))
    return (
        layer_values.astype(jnp.bfloat16),
        input_grad,
        attn_shard,
        mlp_shard,
        vector_shard,
        rms_values,
    )


def solution(mesh):
    in_specs = (
        P(("fsdp", "seq"), None),
        P(("fsdp", "seq"), None),
        P("fsdp", None),
        P("fsdp"),
        P(("fsdp", "seq"), None),
        P(("fsdp", "seq"), None),
        P(("fsdp", "seq")),
    )
    out_specs = (
        P(("fsdp", "seq"), None),
        P(("fsdp", "seq"), None),
        P(("fsdp", "seq"), None),
        P(("fsdp", "seq"), None),
        P(("fsdp", "seq")),
        P(),
    )
    return jax.shard_map(
        layer_body, mesh=mesh, in_specs=in_specs, out_specs=out_specs, check_vma=False
    )
```

```python
import functools
import jax
import jax.numpy as jnp
from jax import lax
from jax.sharding import PartitionSpec as P

from jax.experimental import pallas as pl
from jax.experimental.pallas import tpu as pltpu


H = 16

BLOCK = 512
NEG = -1e30


def key_ranges(segment_doc, block):
    firsts = segment_doc[::block]
    lasts = segment_doc[block - 1 :: block]
    starts = jnp.sum(segment_doc[None, :] < firsts[:, None], axis=1).astype(jnp.int32)
    ends = jnp.sum(segment_doc[None, :] <= lasts[:, None], axis=1).astype(jnp.int32)
    return starts // block, (ends + block - 1) // block


def _scores(q, k, doc_q, doc_k, scale):
    s = lax.dot_general(q, k, (((1,), (1,)), ((), ())), preferred_element_type=jnp.float32) * scale
    return jnp.where(doc_q == doc_k, s, NEG)


def _fwd_kernel(lo_ref, hi_ref, q_ref, k_ref, v_ref, dq_ref, dk_ref, out_ref, lse_ref, s_buf,
                *, scale, block):
    i = pl.program_id(1)
    lo = lo_ref[i]
    hi = hi_ref[i]
    q = q_ref[...]
    doc_q = dq_ref[...]
    rows = q.shape[0]

    def pass_one(kb, m):
        start = pl.multiple_of(kb * block, block)
        s = _scores(q, k_ref[pl.ds(start, block), :], doc_q, dk_ref[:, pl.ds(start, block)], scale)
        s_buf[kb - lo] = s
        return jnp.maximum(m, jnp.max(s, axis=1, keepdims=True))

    m = lax.fori_loop(lo, hi, pass_one, jnp.full((rows, 1), NEG, jnp.float32))

    def pass_two(kb, l):
        e = jnp.exp(s_buf[kb - lo] - m)
        s_buf[kb - lo] = e
        return l + jnp.sum(e, axis=1, keepdims=True)

    l = lax.fori_loop(lo, hi, pass_two, jnp.zeros((rows, 1), jnp.float32))

    def pass_three(kb, acc):
        start = pl.multiple_of(kb * block, block)
        p = (s_buf[kb - lo] / l).astype(jnp.bfloat16)
        return acc + jnp.dot(p, v_ref[pl.ds(start, block), :], preferred_element_type=jnp.float32)

    acc = lax.fori_loop(lo, hi, pass_three, jnp.zeros(out_ref.shape, jnp.float32))
    out_ref[...] = acc.astype(out_ref.dtype)
    lse_ref[...] = m + jnp.log(l)


def attn_forward(q, k, v, segment_doc, scale, block=BLOCK):
    heads, seg_len, d = q.shape
    lo, hi = key_ranges(segment_doc, block)
    doc_col = segment_doc.reshape(seg_len, 1)
    doc_row = segment_doc.reshape(1, seg_len)
    grid = (heads, seg_len // block)
    spec_q = pl.BlockSpec((None, block, d), lambda h, i, lo, hi: (h, i, 0))
    spec_kv = pl.BlockSpec((None, seg_len, d), lambda h, i, lo, hi: (h, 0, 0))
    spec_dq = pl.BlockSpec((block, 1), lambda h, i, lo, hi: (i, 0))
    spec_dk = pl.BlockSpec((1, seg_len), lambda h, i, lo, hi: (0, 0))
    spec_lse = pl.BlockSpec((None, block, 1), lambda h, i, lo, hi: (h, i, 0))
    return pl.pallas_call(
        functools.partial(_fwd_kernel, scale=scale, block=block),
        grid_spec=pltpu.PrefetchScalarGridSpec(
            num_scalar_prefetch=2,
            grid=grid,
            in_specs=[spec_q, spec_kv, spec_kv, spec_dq, spec_dk],
            out_specs=[spec_q, spec_lse],
            scratch_shapes=[pltpu.VMEM((seg_len // block, block, block), jnp.float32)],
        ),
        out_shape=[
            jax.ShapeDtypeStruct((heads, seg_len, d), jnp.bfloat16),
            jax.ShapeDtypeStruct((heads, seg_len, 1), jnp.float32),
        ],
        compiler_params=pltpu.CompilerParams(dimension_semantics=("arbitrary", "arbitrary")),
    )(lo, hi, q, k, v, doc_col, doc_row)


def _bwd_kernel(lo_ref, hi_ref, q_ref, k_ref, v_ref, da_ref, lse_ref, dq_ref, dk_ref,
                gq_ref, gk_ref, gv_ref, p_buf, dp_buf, *, scale, block):
    i = pl.program_id(1)
    lo = lo_ref[i]
    hi = hi_ref[i]

    @pl.when(i == 0)
    def _():
        gk_ref[...] = jnp.zeros(gk_ref.shape, gk_ref.dtype)
        gv_ref[...] = jnp.zeros(gv_ref.shape, gv_ref.dtype)

    q = q_ref[...]
    da = da_ref[...]
    lse = lse_ref[...]
    doc_q = dq_ref[...]
    rows = q.shape[0]

    def pass_one(kb, delta):
        start = pl.multiple_of(kb * block, block)
        s = _scores(q, k_ref[pl.ds(start, block), :], doc_q, dk_ref[:, pl.ds(start, block)], scale)
        p = jnp.exp(s - lse)
        dp = lax.dot_general(da, v_ref[pl.ds(start, block), :], (((1,), (1,)), ((), ())),
                             preferred_element_type=jnp.float32)
        p_buf[kb - lo] = p
        dp_buf[kb - lo] = dp
        return delta + jnp.sum(dp * p, axis=1, keepdims=True)

    delta = lax.fori_loop(lo, hi, pass_one, jnp.zeros((rows, 1), jnp.float32))

    def pass_two(kb, gq):
        start = pl.multiple_of(kb * block, block)
        p = p_buf[kb - lo]
        ds = (p * (dp_buf[kb - lo] - delta)).astype(jnp.bfloat16)
        pb = p.astype(jnp.bfloat16)
        gq = gq + jnp.dot(ds, k_ref[pl.ds(start, block), :], preferred_element_type=jnp.float32)
        gk_ref[pl.ds(start, block), :] += lax.dot_general(
            ds, q, (((0,), (0,)), ((), ())), preferred_element_type=jnp.float32)
        gv_ref[pl.ds(start, block), :] += lax.dot_general(
            pb, da, (((0,), (0,)), ((), ())), preferred_element_type=jnp.float32)
        return gq

    gq = lax.fori_loop(lo, hi, pass_two, jnp.zeros(gq_ref.shape, jnp.float32))
    gq_ref[...] = gq * scale

    @pl.when(i == pl.num_programs(1) - 1)
    def _():
        gk_ref[...] = gk_ref[...] * scale


def attn_backward(q, k, v, da, lse, segment_doc, scale, block=BLOCK):
    heads, seg_len, d = q.shape
    lo, hi = key_ranges(segment_doc, block)
    doc_col = segment_doc.reshape(seg_len, 1)
    doc_row = segment_doc.reshape(1, seg_len)
    grid = (heads, seg_len // block)
    spec_q = pl.BlockSpec((None, block, d), lambda h, i, lo, hi: (h, i, 0))
    spec_kv = pl.BlockSpec((None, seg_len, d), lambda h, i, lo, hi: (h, 0, 0))
    spec_dq = pl.BlockSpec((block, 1), lambda h, i, lo, hi: (i, 0))
    spec_dk = pl.BlockSpec((1, seg_len), lambda h, i, lo, hi: (0, 0))
    spec_lse = pl.BlockSpec((None, block, 1), lambda h, i, lo, hi: (h, i, 0))
    return pl.pallas_call(
        functools.partial(_bwd_kernel, scale=scale, block=block),
        grid_spec=pltpu.PrefetchScalarGridSpec(
            num_scalar_prefetch=2,
            grid=grid,
            in_specs=[spec_q, spec_kv, spec_kv, spec_q, spec_lse, spec_dq, spec_dk],
            out_specs=[spec_q, spec_kv, spec_kv],
            scratch_shapes=[pltpu.VMEM((seg_len // block, block, block), jnp.float32)] * 2,
        ),
        out_shape=[jax.ShapeDtypeStruct((heads, seg_len, d), jnp.float32)] * 3,
        compiler_params=pltpu.CompilerParams(dimension_semantics=("arbitrary", "arbitrary")),
    )(lo, hi, q, k, v, da, lse, doc_col, doc_row)


EPSILON = 1e-05
ROOT_HALF = 0.7071067811865476
INV_ROOT_TWO_PI = 0.3989422804014327


def norm_forward(values, norm_gain, norm_shift):
    row_mean = jnp.mean(values, axis=1, keepdims=True)
    centered = values - row_mean
    inverse = lax.rsqrt(jnp.mean(centered * centered, axis=1, keepdims=True) + EPSILON)
    scaled = centered * inverse
    return (scaled * norm_gain + norm_shift, scaled, inverse)


def norm_backward(gradient, scaled, inverse, norm_gain):
    grad_scaled = gradient * norm_gain
    grad_mean = jnp.mean(grad_scaled, axis=1, keepdims=True)
    grad_along = jnp.mean(grad_scaled * scaled, axis=1, keepdims=True)
    grad_rows = inverse * (grad_scaled - grad_mean - scaled * grad_along)
    return (grad_rows, jnp.sum(gradient * scaled, axis=0), jnp.sum(gradient, axis=0))


def gelu_slope(entries):
    return 0.5 * (1.0 + lax.erf(entries * ROOT_HALF)) + entries * INV_ROOT_TWO_PI * jnp.exp(
        -0.5 * entries * entries
    )


def ring_gather(rows, count, index):
    half = count // 2
    order = [2 * a for a in range(half)] + [2 * a + 1 for a in reversed(range(half))]
    place = [order.index(s) for s in range(count)]
    forward_pairs = [(order[i], order[(i + 1) % count]) for i in range(count)]
    backward_pairs = [(b, a) for a, b in forward_pairs]
    by_offset = [None] * count
    by_offset[0] = rows
    moving = rows
    for step in range(1, count - count // 2):
        moving = lax.ppermute(moving, "seq", forward_pairs)
        by_offset[count - step] = moving
    moving = rows
    for step in range(1, count // 2 + 1):
        moving = lax.ppermute(moving, "seq", backward_pairs)
        by_offset[step] = moving
    position = jnp.asarray(place, jnp.int32)[index]
    pick = (jnp.asarray(place, jnp.int32) - position) % count
    stacked = jnp.stack(by_offset)
    return jnp.take(stacked, pick, axis=0).reshape((count * rows.shape[0],) + rows.shape[1:])


def attn_sum(values):
    return lax.psum_scatter(values, "fsdp", scatter_dimension=0, tiled=True)[0]


def contract_rows(left, right):
    return lax.dot_general(
        left, right, (((0,), (0,)), ((), ())), preferred_element_type=jnp.float32
    )


def contract_cols(left, right):
    return lax.dot_general(
        left, right, (((1,), (1,)), ((), ())), preferred_element_type=jnp.float32
    )


def layer_body(layer_in, cotangent, doc_ids, valid_len, attn_weights, mlp_weights, param_vector):
    seq_count = lax.axis_size("seq")
    seq_index = lax.axis_index("seq")
    tokens, model_width = layer_in.shape
    head_size = model_width // H
    local_heads = H // seq_count
    score_scale = head_size ** (-0.5)
    attn_rows, vector_slot = attn_weights.shape[0], param_vector.shape[0]
    packed = jnp.concatenate(
        [attn_weights, jnp.pad(param_vector, (0, model_width - vector_slot))[None]], axis=0
    )
    packed_full = lax.all_gather(packed, ("fsdp", "seq"), axis=0, tiled=False)
    attn_full = packed_full[:, :attn_rows].reshape(-1, model_width)
    vector_full = packed_full[:, attn_rows, :vector_slot].reshape(-1)
    mlp_full = lax.all_gather(mlp_weights, ("fsdp", "seq"), axis=0, tiled=True)
    hidden = mlp_full.shape[0] // 2
    vector_wide = vector_full.astype(jnp.float32)
    pieces = [
        vector_wide[slot_index * model_width : (slot_index + 1) * model_width]
        for slot_index in range(8)
    ]
    bias_q, bias_v, bias_o, gain_one, shift_one, bias_two, gain_two, shift_two = pieces
    bias_up = vector_wide[8 * model_width :]
    qkv_weights = attn_full[: 3 * model_width].reshape(3, model_width, model_width)
    out_weights = attn_full[3 * model_width :]
    in_weights = mlp_full[:hidden]
    down_weights = mlp_full[hidden:]
    segment_in = ring_gather(layer_in, seq_count, seq_index)
    segment_doc = doc_ids[0]
    seg_len = segment_doc.shape[0]
    positions = seq_index * tokens + lax.iota(jnp.int32, tokens)
    valid_rows = (positions < valid_len[0]).astype(jnp.float32)[:, None]
    zero_row = jnp.zeros((1, model_width), jnp.float32)
    qkv_bias = jnp.concatenate([bias_q[None], zero_row, bias_v[None]], axis=0)
    head_width = local_heads * head_size
    own_columns = seq_index * head_width
    own_weights = lax.dynamic_slice_in_dim(qkv_weights, own_columns, head_width, axis=2)
    own_bias = lax.dynamic_slice_in_dim(qkv_bias, own_columns, head_width, axis=1)
    projected = (
        jnp.einsum("td,ide->tie", segment_in, own_weights, preferred_element_type=jnp.float32)
        + own_bias[None]
    )
    head_all = jnp.transpose(
        projected.astype(jnp.bfloat16).reshape(seg_len, 3, local_heads, head_size), (1, 2, 0, 3)
    )
    head_q, head_k, head_v = head_all[0], head_all[1], head_all[2]
    head_mixed, log_total = attn_forward(head_q, head_k, head_v, segment_doc, score_scale)
    mixed_rows = jnp.transpose(head_mixed, (1, 0, 2)).reshape(seq_count, tokens, head_width)
    token_mixed = lax.all_to_all(mixed_rows, "seq", split_axis=0, concat_axis=0, tiled=True)
    attn_mixed = jnp.transpose(token_mixed, (1, 0, 2)).reshape(tokens, model_width)
    branch = jnp.dot(attn_mixed, out_weights, preferred_element_type=jnp.float32) + bias_o
    resid_one = layer_in.astype(jnp.float32) + branch
    normed, scaled_one, inverse_one = norm_forward(resid_one, gain_one, shift_one)
    normed_low = normed.astype(jnp.bfloat16)
    normed_seg = lax.all_gather(normed_low, "seq", axis=0, tiled=True)
    upper = contract_cols(normed_low, in_weights) + bias_up
    active_low = jax.nn.gelu(upper, approximate=False).astype(jnp.bfloat16)
    mlp_branch = jnp.dot(active_low, down_weights, preferred_element_type=jnp.float32) + bias_two
    resid_two = normed + mlp_branch
    layer_values, scaled_two, inverse_two = norm_forward(resid_two, gain_two, shift_two)
    squares = jnp.stack(
        [
            jnp.sum(valid_rows * resid_one * resid_one),
            jnp.sum(valid_rows * branch * branch),
            jnp.sum(valid_rows * resid_two * resid_two),
            jnp.sum(valid_rows * mlp_branch * mlp_branch),
        ]
    )
    own_sums = jnp.pad(jnp.concatenate([squares, jnp.sum(valid_rows)[None]]), (0, 3))
    grad_out = cotangent.astype(jnp.float32)
    grad_resid_two, grad_gain_two, grad_shift_two = norm_backward(
        grad_out, scaled_two, inverse_two, gain_two
    )
    grad_mlp_low = grad_resid_two.astype(jnp.bfloat16)
    grad_bias_two = jnp.sum(grad_mlp_low.astype(jnp.float32), axis=0)
    grad_active = contract_cols(grad_mlp_low, down_weights)
    grad_upper_low = (grad_active * gelu_slope(upper)).astype(jnp.bfloat16)
    grad_bias_up = jnp.sum(grad_upper_low.astype(jnp.float32), axis=0)
    grad_normed = grad_resid_two + jnp.dot(
        grad_upper_low, in_weights, preferred_element_type=jnp.float32
    )
    fsdp_count = lax.axis_size("fsdp")
    mlp_height = 2 * hidden // (fsdp_count * seq_count)
    mlp_groups = hidden // (seq_count * mlp_height)

    def own_rows(rows):
        blocks = rows.reshape((mlp_groups, seq_count, mlp_height) + rows.shape[1:])
        picked = lax.dynamic_index_in_dim(blocks, seq_index, axis=1, keepdims=False)
        return picked.reshape((mlp_groups * mlp_height,) + rows.shape[1:])

    grad_mlp_seg = lax.all_gather(grad_mlp_low, "seq", axis=0, tiled=True)
    upper_own = contract_cols(normed_seg, own_rows(in_weights)) + own_rows(bias_up)
    active_own = jax.nn.gelu(upper_own, approximate=False).astype(jnp.bfloat16)
    grad_down_own = contract_rows(active_own, grad_mlp_seg)
    grad_active_own = contract_cols(grad_mlp_seg, own_rows(down_weights))
    grad_upper_own = (grad_active_own * gelu_slope(upper_own)).astype(jnp.bfloat16)
    grad_in_own = contract_rows(grad_upper_own, normed_seg)
    mlp_stack = jnp.concatenate(
        [
            grad_in_own.reshape(mlp_groups, mlp_height, model_width),
            grad_down_own.reshape(mlp_groups, mlp_height, model_width),
        ],
        axis=0,
    )
    mlp_shard = lax.psum_scatter(mlp_stack, "fsdp", scatter_dimension=0, tiled=True)[0]
    grad_resid_one, grad_gain_one, grad_shift_one = norm_backward(
        grad_normed, scaled_one, inverse_one, gain_one
    )
    grad_branch_low = grad_resid_one.astype(jnp.bfloat16)
    grad_bias_o = jnp.sum(grad_branch_low.astype(jnp.float32), axis=0)
    block_height = 4 * model_width // (fsdp_count * seq_count)
    out_blocks = model_width // (seq_count * block_height)
    quarter = block_height // fsdp_count
    out_partial = jnp.transpose(
        contract_rows(attn_mixed, grad_branch_low).reshape(
            out_blocks, seq_count, fsdp_count, quarter, model_width
        ),
        (2, 0, 1, 3, 4),
    )
    out_parts = lax.all_to_all(out_partial, "fsdp", split_axis=0, concat_axis=0, tiled=True)
    out_quarters = jnp.transpose(jnp.sum(out_parts, axis=0), (1, 0, 2, 3))
    grad_mixed_low = contract_cols(grad_branch_low, out_weights).astype(jnp.bfloat16)
    grad_split = jnp.transpose(
        grad_mixed_low.reshape(tokens, seq_count, head_width), (1, 0, 2)
    )
    grad_heads = lax.all_to_all(grad_split, "seq", split_axis=0, concat_axis=0, tiled=True)
    head_grad = jnp.transpose(grad_heads.reshape(seg_len, local_heads, head_size), (1, 0, 2))

    grad_queries, grad_keys, grad_values = attn_backward(
        head_q, head_k, head_v, head_grad, log_total, segment_doc, score_scale
    )
    head_grads = jnp.transpose(
        jnp.stack([grad_queries, grad_keys, grad_values], axis=0), (2, 0, 1, 3)
    ).astype(jnp.bfloat16)
    head_weight_grads = jnp.einsum(
        "td,tihe->dihe", segment_in, head_grads, preferred_element_type=jnp.float32
    )
    qkv_blocks = 3 * out_blocks
    head_bias_sums = jnp.sum(head_grads.astype(jnp.float32), axis=0).reshape(3, head_width)
    bias_qv = lax.dynamic_update_slice(
        jnp.zeros((2, model_width), jnp.float32),
        head_bias_sums[::2],
        (0, seq_index * head_width),
    )
    grad_vector = jnp.concatenate(
        [
            bias_qv.reshape(-1),
            grad_bias_o,
            grad_gain_one,
            grad_shift_one,
            grad_bias_two,
            grad_gain_two,
            grad_shift_two,
            grad_bias_up,
        ]
    )
    slot = grad_vector.shape[0] // (fsdp_count * seq_count)
    vector_part = jnp.transpose(grad_vector.reshape(fsdp_count, seq_count, slot), (1, 0, 2))
    sums_part = jnp.broadcast_to(own_sums, (seq_count, fsdp_count, own_sums.shape[0]))
    vector_part = jnp.concatenate([vector_part, sums_part], axis=2)
    wide_slot = slot + own_sums.shape[0]
    by_row = jnp.transpose(head_weight_grads.reshape(model_width, 3, head_width), (1, 0, 2))
    row_part = jnp.transpose(
        by_row.reshape(qkv_blocks, seq_count, block_height, head_width), (1, 0, 2, 3)
    )
    row_size = qkv_blocks * block_height * head_width
    out_size = out_blocks * quarter * model_width
    exchanged = lax.all_to_all(
        jnp.concatenate(
            [
                row_part.reshape(seq_count, -1),
                out_quarters.reshape(seq_count, -1),
                vector_part.reshape(seq_count, -1),
            ],
            axis=1,
        ),
        "seq", split_axis=0, concat_axis=0, tiled=True,
    )
    own_quarters = jnp.sum(
        exchanged[:, row_size : row_size + out_size].reshape(
            seq_count, out_blocks, quarter, model_width
        ),
        axis=0,
    )
    out_rows = lax.dynamic_update_slice(
        jnp.zeros((out_blocks, block_height, model_width), jnp.float32),
        own_quarters,
        (0, lax.axis_index("fsdp") * quarter, 0),
    )
    exchanged = jnp.concatenate(
        [exchanged[:, :row_size], exchanged[:, row_size + out_size :]], axis=1
    )
    row_blocks = exchanged[:, :row_size].reshape(seq_count, qkv_blocks, block_height, head_width)
    qkv_rows = jnp.transpose(row_blocks, (1, 2, 0, 3)).reshape(qkv_blocks, block_height, model_width)
    vector_rows = jnp.sum(
        exchanged[:, row_size:].reshape(seq_count, fsdp_count, wide_slot), axis=0
    )
    sums_width = own_sums.shape[0]
    segment_sums = vector_rows[0, slot:]
    sums_groups = lax.dynamic_update_slice(
        jnp.zeros((fsdp_count * sums_width,), jnp.float32),
        segment_sums,
        (lax.axis_index("fsdp") * sums_width,),
    )
    vector_rows = jnp.concatenate(
        [
            vector_rows[:, :slot],
            jnp.broadcast_to(sums_groups, (fsdp_count, fsdp_count * sums_width)),
        ],
        axis=1,
    )
    vector_rows = jnp.pad(
        vector_rows, ((0, 0), (0, model_width - vector_rows.shape[1]))
    )[:, None]
    token_grads = lax.all_to_all(
        head_grads.reshape(seq_count, tokens, 3 * head_width),
        "seq", split_axis=0, concat_axis=0, tiled=True,
    )
    grad_qkv = jnp.transpose(
        token_grads.reshape(seq_count, tokens, 3, head_width), (1, 2, 0, 3)
    ).reshape(tokens, 3, model_width)
    input_grad = grad_resid_one + jnp.einsum(
        "tie,ide->td", grad_qkv, qkv_weights, preferred_element_type=jnp.float32
    )
    grad_attn_rows = jnp.concatenate([qkv_rows, out_rows], axis=0)
    summed = attn_sum(jnp.concatenate([grad_attn_rows, vector_rows], axis=1))
    attn_shard = summed[:block_height]
    vector_shard = summed[block_height, :slot]
    total_sums = jnp.sum(
        summed[block_height, slot : slot + fsdp_count * sums_width].reshape(fsdp_count, sums_width),
        axis=0,
    )
    square_sums, valid_total = total_sums[:4], total_sums[4]
    rms_values = jnp.sqrt(square_sums / (valid_total * model_width))
    return (
        layer_values.astype(jnp.bfloat16),
        input_grad,
        attn_shard,
        mlp_shard,
        vector_shard,
        rms_values,
    )


def solution(mesh):
    in_specs = (
        P(("fsdp", "seq"), None),
        P(("fsdp", "seq"), None),
        P("fsdp", None),
        P("fsdp"),
        P(("fsdp", "seq"), None),
        P(("fsdp", "seq"), None),
        P(("fsdp", "seq")),
    )
    out_specs = (
        P(("fsdp", "seq"), None),
        P(("fsdp", "seq"), None),
        P(("fsdp", "seq"), None),
        P(("fsdp", "seq"), None),
        P(("fsdp", "seq")),
        P(),
    )
    return jax.shard_map(
        layer_body, mesh=mesh, in_specs=in_specs, out_specs=out_specs, check_vma=False
    )
```
